256 devices in a mesh: row: 32 (over z_lo, y, core), col: 8 (over x, z_hi).
Axes of the slice: x: 4, y: 4, z: 8 (z_hi: 2, z_lo: 4; z = z_hi * 4 + z_lo), core: 2. Of those that a mesh axis runs over, the one named last changes fastest.
Arguments:
- spectral_field: float32 [2, 256, 256, 256], P(None, 'row', 'col'), may hold values from -4.5 to 4.5
Outputs:
- updated_field: float32 [2, 256, 256, 256], P(None, 'row', 'col')
- shell_spectrum: float32 [256], replicated
The draws below stay inside these ranges and needn't reach their ends.
All inputs are finite; a program needn't handle non-finite values.
Results may differ from the reference program's by a relative error of at most 0.0031.
Values may be sent and summed in bfloat16 or wider, within the bound.
No kernel may reach another device: no remote copies, remote signals or barrier semaphores. Data moves between devices by JAX's collectives and lax.ppermute only.
A program may use at most 64 MiB of HBM per device.

```python
import math
import jax
import jax.numpy as jnp
from jax import lax

K = 256


def block_levels(key, dims, shards, smallest, top_value):
    factor_of = 1.0
    for axis_at, blocks in shards:
        draws = jax.random.uniform(jax.random.fold_in(jax.random.fold_in(key, 6), axis_at), (blocks,), jnp.float32, smallest / len(shards), top_value / len(shards))
        factor_of = factor_of * jnp.repeat(jnp.exp(draws), dims[axis_at] // blocks).reshape((-1,) + (1,) * (len(dims) - 1 - axis_at))
    return factor_of


def bell_draw(rng, shape, deviation, reach, cuts=(), kind=jnp.bfloat16):
    loudness = block_levels(rng, shape, cuts, -0.22, 0.18) if cuts else 1.0
    entries = jax.random.normal(rng, shape, jnp.float32) * deviation * loudness
    return jnp.minimum(jnp.maximum(entries, -reach), reach).astype(kind)


def setup_inputs(seed: int = 0) -> dict:
    splits = jax.random.split(jax.random.key(seed), 2)
    spectral_field = bell_draw(splits[0], (2, K, K, K), 0.7, 4.5, ((1, 32), (2, 8)), jnp.float32)
    return {"spectral_field": spectral_field}


phase_rate = 0.0002
coupling = 0.2

def wave_table(inputs, outputs, length, sine_sign, live_mask):
    phase_turns = jnp.mod(inputs[:, None] * outputs[None, :], length)
    phase_angle = phase_turns.astype(jnp.float32) * (2.0 * math.pi / length)
    live_rows = live_mask.astype(jnp.float32)[:, None]
    cosine_part = (jnp.cos(phase_angle) * live_rows).astype(jnp.bfloat16)
    sine_part = (sine_sign * jnp.sin(phase_angle) * live_rows).astype(jnp.bfloat16)
    return (cosine_part, sine_part)

def rotate(values_in, cosine_part, sine_part, einsum_form, factor):
    precise = lax.Precision.HIGHEST
    real_part = values_in[0].astype(jnp.float32)
    imag_part = values_in[1].astype(jnp.float32)
    cos_wide = cosine_part.astype(jnp.float32)
    sin_wide = sine_part.astype(jnp.float32)
    out_real = jnp.einsum(einsum_form, real_part, cos_wide, precision=precise) - jnp.einsum(einsum_form, imag_part, sin_wide, precision=precise)
    out_imag = jnp.einsum(einsum_form, real_part, sin_wide, precision=precise) + jnp.einsum(einsum_form, imag_part, cos_wide, precision=precise)
    return jnp.stack([out_real, out_imag]) * factor

def reference(spectral_field):
    mode_count = spectral_field.shape[1]
    grid_count = 2 * mode_count
    wavenumbers = jnp.arange(mode_count, dtype=jnp.int32) - mode_count // 2
    grid_points = jnp.arange(grid_count, dtype=jnp.int32)
    inv_cos, inv_sin = wave_table(wavenumbers, grid_points, grid_count, 1.0, jnp.ones((mode_count,), bool))
    fwd_cos, fwd_sin = wave_table(grid_points, wavenumbers, grid_count, -1.0, jnp.ones((grid_count,), bool))
    scale_in = 1.0 / math.sqrt(mode_count)
    scale_out = math.sqrt(mode_count) / grid_count
    coeffs = spectral_field.astype(jnp.bfloat16)
    along_z = rotate(coeffs, inv_cos, inv_sin, 'abc,cd->abd', scale_in).astype(jnp.bfloat16)
    along_y = rotate(along_z, inv_cos, inv_sin, 'abc,bd->adc', scale_in).astype(jnp.bfloat16)
    block_size = grid_count // 8
    pieces = []
    for number in range(8):
        z_block = lax.slice_in_dim(along_y, number * block_size, (number + 1) * block_size, axis=3)
        physical = rotate(z_block, inv_cos, inv_sin, 'abc,ad->dbc', scale_in)
        cubic_term = (coupling * (physical[0] * physical[0] + physical[1] * physical[1]) * physical).astype(jnp.bfloat16)
        pieces.append(rotate(cubic_term, fwd_cos, fwd_sin, 'abc,ad->dbc', scale_out).astype(jnp.bfloat16))
    back_x = jnp.concatenate(pieces, axis=3)
    back_y = rotate(back_x, fwd_cos, fwd_sin, 'abc,bd->adc', scale_out).astype(jnp.bfloat16)
    nonlinear = rotate(back_y, fwd_cos, fwd_sin, 'abc,cd->abd', scale_out)
    wave_first = wavenumbers[:, None, None]
    wave_second = wavenumbers[None, :, None]
    wave_third = wavenumbers[None, None, :]
    squared = wave_first * wave_first + wave_second * wave_second + wave_third * wave_third
    phase_angle = phase_rate * squared.astype(jnp.float32)
    cosine_part = jnp.cos(phase_angle)
    sine_part = jnp.sin(phase_angle)
    shifted_real = spectral_field[0] - nonlinear[1]
    shifted_imag = spectral_field[1] + nonlinear[0]
    new_real = shifted_real * cosine_part + shifted_imag * sine_part
    new_imag = shifted_imag * cosine_part - shifted_real * sine_part
    updated_field = jnp.stack([new_real, new_imag])
    energy = new_real * new_real + new_imag * new_imag
    shell_index = jnp.floor(jnp.sqrt(squared.astype(jnp.float32)) + 0.5).astype(jnp.int32)
    totals = jax.ops.segment_sum(energy.reshape(-1), shell_index.reshape(-1), num_segments=mode_count)
    counts = jax.ops.segment_sum(jnp.ones_like(energy).reshape(-1), shell_index.reshape(-1), num_segments=mode_count)
    shell_spectrum = totals / jnp.maximum(counts, 1.0)
    return (updated_field, shell_spectrum)
```

```python
import math

import jax
import jax.numpy as jnp
import numpy as np
from jax import lax
from jax.experimental import pallas as pl
from jax.experimental.pallas import tpu as pltpu
from jax.sharding import Mesh
from jax.sharding import PartitionSpec as P

ROW = ("z_lo", "y", "core")
COL = ("x", "z_hi")
RING = ("z_hi", "z_lo", "y", "x", "core")

phase_rate = 0.0002
coupling = 0.2

F32 = jnp.float32
BF16 = jnp.bfloat16


def trig(waves, points, length):
    turns = np.mod(np.asarray(waves)[:, None] * np.asarray(points)[None, :], length)
    angle = turns.astype(np.float32) * np.float32(2.0 * math.pi / length)
    return np.cos(angle).astype(np.float32), np.sin(angle).astype(np.float32)


def to_slabs(field_ref, table_ref, out_ref, wide_ref, *, scale):
    modes = field_ref.shape[3]
    width = field_ref.shape[2]
    lane = lax.broadcasted_iota(jnp.int32, (width, modes), 1)
    sign = jnp.where(lane % 2 == 0, 1.0, -1.0)
    table = table_ref[...]
    width_x = field_ref.shape[1]
    for pair in range(0, width_x, 2):
        rows = []
        for at in (pair, pair + 1):
            real, imag = field_ref[0, at], field_ref[1, at]
            for factor in (None, sign):
                if factor is not None:
                    real, imag = real * factor, imag * factor
                rows.append(jnp.concatenate([real, -imag], axis=1).astype(BF16))
                rows.append(jnp.concatenate([imag, real], axis=1).astype(BF16))
        block = jnp.concatenate(rows, axis=0)
        product = lax.dot_general(
            table, block, (((1,), (1,)), ((), ())), preferred_element_type=F32
        ) * scale
        for k in range(2):
            wide_ref[pl.ds(pair + k, modes, stride=width_x), :] = product[:, 128 * k : 128 * (k + 1)]
    out_ref[...] = wide_ref[...].astype(BF16).reshape(out_ref.shape)


def planes(in_ref, ty_ref, tx_ref, fx_ref, fy_ref, out_ref, back_ref, done_ref, *, scale_in, scale_out, chunk):
    modes = 256
    grid = 512
    half = 64
    for plane in range(2):
        parts = []
        for x in range(4):
            for z in range(2):
                block = in_ref[z, :, x].reshape(modes, 128)
                parts.append(block[:, half * plane : half * (plane + 1)])
        lines = jnp.concatenate(parts, axis=1)
        along_y = (jnp.dot(lines, ty_ref[...], preferred_element_type=F32) * scale_in).astype(BF16)
        first = lax.broadcasted_iota(jnp.int32, (modes, chunk), 0) == 0
        for start in range(0, grid, chunk):
            rhs = jnp.concatenate(
                [along_y[:, start : start + chunk], along_y[:, grid + start : grid + start + chunk]], axis=1
            )
            even_odd = jnp.dot(tx_ref[...], rhs, preferred_element_type=F32) * scale_in
            pr, pi = even_odd[:modes, :chunk], even_odd[:modes, chunk:]
            qr, qi = even_odd[modes:, :chunk], even_odd[modes:, chunk:]
            ar = jnp.where(first, pr, pr - qi)
            ai = jnp.where(first, pi, pi + qr)
            br = jnp.where(first, qr, pr + qi)
            bi = jnp.where(first, qi, pi - qr)
            ma = coupling * (ar * ar + ai * ai)
            mb = coupling * (br * br + bi * bi)
            ar, ai, br, bi = ma * ar, ma * ai, mb * br, mb * bi
            even_r = jnp.where(first, ar, ar + br)
            even_i = jnp.where(first, ai, ai + bi)
            odd_i = jnp.where(first, br, ai - bi)
            odd_r = jnp.where(first, bi, br - ar)
            folded = jnp.concatenate(
                [
                    jnp.concatenate([even_r.astype(BF16), even_i.astype(BF16)], axis=1),
                    jnp.concatenate([odd_i.astype(BF16), odd_r.astype(BF16)], axis=1),
                ],
                axis=0,
            )
            back_x = (jnp.dot(fx_ref[...], folded, preferred_element_type=F32) * scale_out).astype(BF16)
            back_ref[:, start : start + chunk] = back_x[:, :chunk]
            back_ref[:, grid + start : grid + start + chunk] = back_x[:, chunk:]
        done_ref[plane] = (
            jnp.dot(back_ref[...], fy_ref[...], preferred_element_type=F32) * scale_out
        ).astype(BF16)
    for x in range(4):
        for z in range(2):
            at = 128 * x + half * z
            message = jnp.concatenate([done_ref[0, :, at : at + half], done_ref[1, :, at : at + half]], axis=1)
            out_ref[z, :, x] = message.reshape(16, 16, 128)


def finish(in_ref, field_ref, table_ref, out_ref, sums_ref, wide_ref, energy_ref, *, scale, bins):
    _, width_x, width_y, modes = field_ref.shape
    half_modes = modes // 2
    row = (lax.axis_index("z_lo") * 4 + lax.axis_index("y")) * 2 + lax.axis_index("core")
    col = lax.axis_index("x") * 2 + lax.axis_index("z_hi")
    base_x = row * width_x - half_modes
    base_y = col * width_y - half_modes
    wave_y = base_y + lax.broadcasted_iota(jnp.int32, (width_y, modes), 0)
    wave_z = lax.broadcasted_iota(jnp.int32, (width_y, modes), 1) - half_modes
    square_yz = wave_y * wave_y + wave_z * wave_z
    angle_yz = phase_rate * square_yz.astype(F32)
    cos_yz, sin_yz = jnp.cos(angle_yz), jnp.sin(angle_yz)
    wave_x8 = base_x + lax.broadcasted_iota(jnp.int32, (width_x, modes), 0)
    angle_x = phase_rate * (wave_x8 * wave_x8).astype(F32)
    cos_x, sin_x = jnp.cos(angle_x), jnp.sin(angle_x)
    near_x = jnp.maximum(base_x, -(base_x + width_x - 1))
    near_y = jnp.maximum(base_y, -(base_y + width_y - 1))
    near = near_x * near_x + near_y * near_y

    def shell_of(squared):
        return jnp.floor(jnp.sqrt(squared.astype(F32)) + 0.5).astype(jnp.int32)

    lowest = shell_of(near + wave_z * wave_z)
    sign = jnp.where(wave_z % 2 == 0, 1.0, -1.0)
    wide_ref[...] = in_ref[...].reshape(wide_ref.shape).astype(F32)
    table = table_ref[...]
    for at in range(width_x):
        slab = wide_ref[pl.ds(at, modes, stride=width_x), :].astype(BF16)
        got = lax.dot_general(slab, table, (((0,), (0,)), ((), ())), preferred_element_type=F32)
        r0, i0, r1, i1 = (got[width_y * k : width_y * (k + 1)] for k in range(4))
        non_r = (r0[:, :modes] + i0[:, modes:] + sign * (r1[:, :modes] + i1[:, modes:])) * scale
        non_i = (i0[:, :modes] - r0[:, modes:] + sign * (i1[:, :modes] - r1[:, modes:])) * scale
        u = field_ref[0, at] - non_i
        v = field_ref[1, at] + non_r
        cx, sx = cos_x[at : at + 1], sin_x[at : at + 1]
        cos = cos_yz * cx - sin_yz * sx
        sin = sin_yz * cx + cos_yz * sx
        new_r = u * cos + v * sin
        new_i = v * cos - u * sin
        out_ref[0, at] = new_r
        out_ref[1, at] = new_i
        energy_ref[0, at] = new_r * new_r + new_i * new_i
        wx = base_x + at
        energy_ref[1, at] = (shell_of(square_yz + wx * wx) - lowest).astype(F32)
    rows = []
    for k in range(bins):
        total = jnp.zeros((8, modes), F32)
        for at in range(width_x):
            hit = jnp.where(energy_ref[1, at] == float(k), energy_ref[0, at], 0.0)
            for j in range(0, width_y, 8):
                total = total + hit[j : j + 8]
        rows.append(jnp.sum(total, axis=0, keepdims=True))
    stacked = jnp.concatenate(rows, axis=0)
    wave_col = lax.broadcasted_iota(jnp.int32, (modes, modes), 0) - half_modes
    shell_col = shell_of(near + wave_col * wave_col)
    one_hot = (shell_col == lax.broadcasted_iota(jnp.int32, (modes, modes), 1)).astype(F32)
    placed = jnp.dot(stacked, one_hot, preferred_element_type=F32, precision=lax.Precision.HIGHEST)
    shifted = pltpu.roll(placed, 0, 1, stride=1, stride_axis=0)
    sums_ref[...] = jnp.sum(shifted, axis=0, keepdims=True)


def tables(modes):
    grid = 2 * modes
    waves = np.arange(modes) - modes // 2
    cos, sin = trig(waves, np.arange(grid), grid)
    low_cos, low_sin = cos[:, :modes].T, sin[:, :modes].T
    z_table = np.concatenate([low_cos, low_sin], axis=1)
    blocks = modes // 32
    c, s = cos.reshape(blocks, 32, grid), sin.reshape(blocks, 32, grid)
    ty = np.stack([np.concatenate([c, s], 2), np.concatenate([-s, c], 2)], 1).reshape(2 * modes, 2 * grid)
    ct, st = c.transpose(2, 0, 1), s.transpose(2, 0, 1)
    fy = np.stack([np.stack([ct, -st], 2), np.stack([st, ct], 2)], 0).reshape(2 * grid, 2 * modes)
    odd = low_sin.copy()
    odd[0] = cos[:, modes]
    tx = np.concatenate([low_cos, odd], axis=0)
    fx = tx.T
    return [jnp.asarray(np.ascontiguousarray(t), BF16) for t in (z_table, ty, tx, fx, fy)]


def shell_counts(modes):
    wave = np.arange(modes) - modes // 2
    square = wave * wave
    total = square[:, None, None] + square[None, :, None] + square[None, None, :]
    shell = np.floor(np.sqrt(total.astype(np.float32)) + np.float32(0.5)).astype(np.int64)
    return np.bincount(shell.reshape(-1), minlength=modes)[:modes].astype(np.float32)


def params():
    return pltpu.CompilerParams(vmem_limit_bytes=48 * 1024 * 1024)


def body(field):
    _, width_x, width_y, modes = field.shape
    devices = lax.axis_size(RING)
    scale_in = 1.0 / math.sqrt(modes)
    scale_out = math.sqrt(modes) / (2 * modes)
    z_table, ty, tx, fx, fy = tables(modes)
    import functools

    messages = pl.pallas_call(
        functools.partial(to_slabs, scale=scale_in),
        out_shape=jax.ShapeDtypeStruct((devices, width_x, 128), BF16),
        scratch_shapes=[pltpu.VMEM((devices * width_x, 128), F32)],
        compiler_params=params(),
        name="to_slabs",
    )(field, z_table)
    slabs = lax.all_to_all(messages, RING, 0, 0, tiled=True)
    back = pl.pallas_call(
        functools.partial(planes, scale_in=scale_in, scale_out=scale_out, chunk=256),
        out_shape=jax.ShapeDtypeStruct((2, 16, 4, 16, 128), BF16),
        scratch_shapes=[pltpu.VMEM((modes, 4 * modes), BF16), pltpu.VMEM((2, modes, 2 * modes), BF16)],
        compiler_params=params(),
        name="planes",
    )(slabs.reshape(2, 16, 4, 16, 128), ty, tx, fx, fy)
    home = lax.all_to_all(back.reshape(devices, width_x, 128), RING, 0, 0, tiled=True)
    bins = 8 * math.ceil((math.sqrt((width_x - 1) ** 2 + (width_y - 1) ** 2) + 2) / 8)
    updated, sums = pl.pallas_call(
        functools.partial(finish, scale=scale_out, bins=bins),
        out_shape=[jax.ShapeDtypeStruct(field.shape, F32), jax.ShapeDtypeStruct((1, modes), F32)],
        scratch_shapes=[
            pltpu.VMEM((devices * width_x, 128), F32),
            pltpu.VMEM((2, width_x, width_y, modes), F32),
        ],
        compiler_params=params(),
        name="finish",
    )(home, field, z_table)
    copies = jnp.broadcast_to(sums.reshape(1, modes // 128, 128), (devices, modes // 128, 128))
    everyone = lax.all_to_all(copies, RING, 0, 0, tiled=True)
    spectrum = jnp.sum(everyone, axis=0).reshape(modes) / jnp.asarray(np.maximum(shell_counts(modes), 1.0))
    return updated, spectrum


def solution(mesh):
    split = Mesh(mesh.devices.reshape(4, 4, 2, 4, 2), ROW + COL)
    placed = (P(None, ROW, COL, None),)
    return jax.shard_map(
        body, mesh=split, in_specs=placed, out_specs=(P(None, ROW, COL, None), P()), check_vma=False
    )
```

```python
import functools
import math

import jax
import jax.numpy as jnp
import numpy as np
from jax import lax
from jax.experimental import pallas as pl
from jax.experimental.pallas import tpu as pltpu
from jax.sharding import Mesh
from jax.sharding import PartitionSpec as P

ROW = ("z_lo", "y", "core")
COL = ("x", "z_hi")
RING = ("z_hi", "z_lo", "y", "x", "core")

phase_rate = 0.0002
coupling = 0.2

F32 = jnp.float32
BF16 = jnp.bfloat16


def trig(waves, points, length):
    turns = np.mod(np.asarray(waves)[:, None] * np.asarray(points)[None, :], length)
    angle = turns.astype(np.float32) * np.float32(2.0 * math.pi / length)
    return np.cos(angle).astype(np.float32), np.sin(angle).astype(np.float32)


def to_slabs(field_ref, table_hbm, out_ref, wide_ref, field, table, field_sems, table_sem, *, scale):
    _, width_x, width, modes = field_ref.shape
    table_copy = pltpu.make_async_copy(table_hbm, table, table_sem)
    copies = [
        pltpu.make_async_copy(field_ref.at[:, pl.ds(at, 2)], field.at[:, pl.ds(at, 2)], field_sems.at[at // 2])
        for at in range(0, width_x, 2)
    ]
    table_copy.start()
    for copy in copies:
        copy.start()
    lane = lax.broadcasted_iota(jnp.int32, (width, modes), 1)
    sign = jnp.where(lane % 2 == 0, 1.0, -1.0)
    table_copy.wait()
    for pair in range(0, width_x, 2):
        copies[pair // 2].wait()
        rows = []
        for at in (pair, pair + 1):
            real, imag = field[0, at], field[1, at]
            for factor in (None, sign):
                if factor is not None:
                    real, imag = real * factor, imag * factor
                rows.append(jnp.concatenate([real, -imag], axis=1).astype(BF16))
                rows.append(jnp.concatenate([imag, real], axis=1).astype(BF16))
        block = jnp.concatenate(rows, axis=0)
        product = lax.dot_general(
            table[...], block, (((1,), (1,)), ((), ())), preferred_element_type=F32
        ) * scale
        for k in range(2):
            wide_ref[pl.ds(pair + k, modes, stride=width_x), :] = product[:, 128 * k : 128 * (k + 1)]
    out_ref[...] = wide_ref[...].astype(BF16).reshape(out_ref.shape)


def planes(in_ref, ty_ref, tx_ref, fy_ref, out_ref, back_ref, done_ref, *, scale_in, scale_out, chunk):
    modes = 256
    grid = 512
    half = 64
    fx = tx_ref[...]
    tx = fx.T
    for plane in range(2):
        parts = []
        for x in range(4):
            for z in range(2):
                block = in_ref[z, :, x].reshape(modes, 128)
                parts.append(block[:, half * plane : half * (plane + 1)])
        lines = jnp.concatenate(parts, axis=1)
        along_y = (jnp.dot(lines, ty_ref[...], preferred_element_type=F32) * scale_in).astype(BF16)
        first = lax.broadcasted_iota(jnp.int32, (modes, chunk), 0) == 0
        for start in range(0, grid, chunk):
            rhs = jnp.concatenate(
                [along_y[:, start : start + chunk], along_y[:, grid + start : grid + start + chunk]], axis=1
            )
            even_odd = jnp.dot(tx, rhs, preferred_element_type=F32) * scale_in
            pr, pi = even_odd[:modes, :chunk], even_odd[:modes, chunk:]
            qr, qi = even_odd[modes:, :chunk], even_odd[modes:, chunk:]
            ar = jnp.where(first, pr, pr - qi)
            ai = jnp.where(first, pi, pi + qr)
            br = jnp.where(first, qr, pr + qi)
            bi = jnp.where(first, qi, pi - qr)
            ma = coupling * (ar * ar + ai * ai)
            mb = coupling * (br * br + bi * bi)
            ar, ai, br, bi = ma * ar, ma * ai, mb * br, mb * bi
            even_r = jnp.where(first, ar, ar + br)
            even_i = jnp.where(first, ai, ai + bi)
            odd_i = jnp.where(first, br, ai - bi)
            odd_r = jnp.where(first, bi, br - ar)
            folded = jnp.concatenate(
                [
                    jnp.concatenate([even_r.astype(BF16), even_i.astype(BF16)], axis=1),
                    jnp.concatenate([odd_i.astype(BF16), odd_r.astype(BF16)], axis=1),
                ],
                axis=0,
            )
            back_x = (jnp.dot(fx, folded, preferred_element_type=F32) * scale_out).astype(BF16)
            back_ref[:, start : start + chunk] = back_x[:, :chunk]
            back_ref[:, grid + start : grid + start + chunk] = back_x[:, chunk:]
        done_ref[plane] = (
            jnp.dot(back_ref[...], fy_ref[...], preferred_element_type=F32) * scale_out
        ).astype(BF16)
    for x in range(4):
        for z in range(2):
            at = 128 * x + half * z
            message = jnp.concatenate([done_ref[0, :, at : at + half], done_ref[1, :, at : at + half]], axis=1)
            out_ref[z, :, x] = message.reshape(16, 16, 128)


def place(width_x, width_y, modes):
    row = (lax.axis_index("z_lo") * 4 + lax.axis_index("y")) * 2 + lax.axis_index("core")
    col = lax.axis_index("x") * 2 + lax.axis_index("z_hi")
    return row * width_x - modes // 2, col * width_y - modes // 2


def waves_yz(base_y, width_y, modes):
    wave_y = base_y + lax.broadcasted_iota(jnp.int32, (width_y, modes), 0)
    wave_z = lax.broadcasted_iota(jnp.int32, (width_y, modes), 1) - modes // 2
    return wave_y, wave_z


def finish(in_ref, field_ref, table_ref, out_hbm, sums_ref, wide_ref, out_ref, energy_ref, shell_ref, sems, *, scale, bins):
    _, width_x, width_y, modes = field_ref.shape
    base_x, base_y = place(width_x, width_y, modes)
    wave_y, wave_z = waves_yz(base_y, width_y, modes)
    square_yz = wave_y * wave_y + wave_z * wave_z
    near_x = jnp.maximum(base_x, -(base_x + width_x - 1))
    near_y = jnp.maximum(base_y, -(base_y + width_y - 1))
    near = near_x * near_x + near_y * near_y

    def shell_of(squared):
        return jnp.floor(jnp.sqrt(squared.astype(F32)) + 0.5)

    lowest = shell_of(near + wave_z * wave_z)
    angle_yz = phase_rate * square_yz.astype(F32)
    cos_yz, sin_yz = jnp.cos(angle_yz), jnp.sin(angle_yz)
    wave_x = base_x + lax.broadcasted_iota(jnp.int32, (width_x, modes), 0)
    angle_x = phase_rate * (wave_x * wave_x).astype(F32)
    cos_x, sin_x = jnp.cos(angle_x), jnp.sin(angle_x)
    sign = jnp.where(wave_z % 2 == 0, 1.0, -1.0)
    wide_ref[...] = in_ref[...].reshape(wide_ref.shape).astype(F32)
    table = table_ref[...]
    copies = [
        pltpu.make_async_copy(out_ref.at[:, pl.ds(at, 1)], out_hbm.at[:, pl.ds(at, 1)], sems.at[at])
        for at in range(width_x)
    ]
    for at in range(width_x):
        slab = wide_ref[pl.ds(at, modes, stride=width_x), :].astype(BF16)
        got = lax.dot_general(slab, table, (((0,), (0,)), ((), ())), preferred_element_type=F32)
        r0, i0, r1, i1 = (got[width_y * k : width_y * (k + 1)] for k in range(4))
        non_r = (r0[:, :modes] + i0[:, modes:] + sign * (r1[:, :modes] + i1[:, modes:])) * scale
        non_i = (i0[:, :modes] - r0[:, modes:] + sign * (i1[:, :modes] - r1[:, modes:])) * scale
        u = field_ref[0, at] - non_i
        v = field_ref[1, at] + non_r
        cx, sx = cos_x[at : at + 1], sin_x[at : at + 1]
        cos = cos_yz * cx - sin_yz * sx
        sin = sin_yz * cx + cos_yz * sx
        new_r = u * cos + v * sin
        new_i = v * cos - u * sin
        out_ref[0, at] = new_r
        out_ref[1, at] = new_i
        copies[at].start()
        energy_ref[at] = new_r * new_r + new_i * new_i
        wx = base_x + at
        shell_ref[at] = shell_of(square_yz + wx * wx) - lowest
    rows = []
    for k in range(bins):
        total = jnp.zeros((8, modes), F32)
        for at in range(width_x):
            hit = jnp.where(shell_ref[at] == float(k), energy_ref[at], 0.0)
            for j in range(0, width_y, 8):
                total = total + hit[j : j + 8]
        rows.append(jnp.sum(total, axis=0, keepdims=True))
    rows.extend([jnp.zeros((1, modes), F32)] * (-bins % 8))
    stacked = jnp.concatenate(rows, axis=0)
    wave_col = lax.broadcasted_iota(jnp.int32, (modes, modes), 0) - modes // 2
    shell_col = shell_of(near + wave_col * wave_col).astype(jnp.int32)
    one_hot = (shell_col == lax.broadcasted_iota(jnp.int32, (modes, modes), 1)).astype(F32)
    placed = jnp.dot(stacked, one_hot, preferred_element_type=F32, precision=lax.Precision.HIGHEST)
    shifted = pltpu.roll(placed, 0, 1, stride=1, stride_axis=0)
    sums_ref[...] = jnp.sum(shifted, axis=0, keepdims=True)
    for copy in copies:
        copy.wait()


def mean_up(copies_ref, weight_ref, out_ref):
    out_ref[...] = jnp.sum(copies_ref[...].astype(F32), axis=0) * weight_ref[...]


def tables(modes):
    grid = 2 * modes
    waves = np.arange(modes) - modes // 2
    cos, sin = trig(waves, np.arange(grid), grid)
    low_cos, low_sin = cos[:, :modes].T, sin[:, :modes].T
    z_table = np.concatenate([low_cos, low_sin], axis=1)
    blocks = modes // 32
    c, s = cos.reshape(blocks, 32, grid), sin.reshape(blocks, 32, grid)
    ty = np.stack([np.concatenate([c, s], 2), np.concatenate([-s, c], 2)], 1).reshape(2 * modes, 2 * grid)
    ct, st = c.transpose(2, 0, 1), s.transpose(2, 0, 1)
    fy = np.stack([np.stack([ct, -st], 2), np.stack([st, ct], 2)], 0).reshape(2 * grid, 2 * modes)
    odd = low_sin.copy()
    odd[0] = cos[:, modes]
    tx = np.concatenate([low_cos, odd], axis=0)
    return [jnp.asarray(np.ascontiguousarray(t), BF16) for t in (z_table, ty, tx.T, fy)]


def shell_counts(modes):
    wave = np.arange(modes) - modes // 2
    square = wave * wave
    total = square[:, None, None] + square[None, :, None] + square[None, None, :]
    shell = np.floor(np.sqrt(total.astype(np.float32)) + np.float32(0.5)).astype(np.int64)
    return np.bincount(shell.reshape(-1), minlength=modes)[:modes].astype(np.float32)


def params():
    return pltpu.CompilerParams(vmem_limit_bytes=48 * 1024 * 1024)


def body(field):
    _, width_x, width_y, modes = field.shape
    devices = lax.axis_size(RING)
    scale_in = 1.0 / math.sqrt(modes)
    scale_out = math.sqrt(modes) / (2 * modes)
    z_table, ty, fx, fy = tables(modes)
    messages = pl.pallas_call(
        functools.partial(to_slabs, scale=scale_in),
        in_specs=[pl.BlockSpec(memory_space=pltpu.HBM)] * 2,
        out_shape=jax.ShapeDtypeStruct((devices, width_x, 128), BF16),
        scratch_shapes=[
            pltpu.VMEM((devices * width_x, 128), F32),
            pltpu.VMEM(field.shape, F32),
            pltpu.VMEM(z_table.shape, BF16),
            pltpu.SemaphoreType.DMA((width_x // 2,)),
            pltpu.SemaphoreType.DMA(()),
        ],
        compiler_params=params(),
        name="to_slabs",
    )(pltpu.with_memory_space_constraint(field, pltpu.HBM), pltpu.with_memory_space_constraint(z_table, pltpu.HBM))
    slabs = lax.all_to_all(messages, RING, 0, 0, tiled=True)
    back = pl.pallas_call(
        functools.partial(planes, scale_in=scale_in, scale_out=scale_out, chunk=256),
        out_shape=jax.ShapeDtypeStruct((2, 16, 4, 16, 128), BF16),
        scratch_shapes=[pltpu.VMEM((modes, 4 * modes), BF16), pltpu.VMEM((2, modes, 2 * modes), BF16)],
        compiler_params=params(),
        name="planes",
    )(slabs.reshape(2, 16, 4, 16, 128), ty, fx, fy)
    home = lax.all_to_all(back.reshape(devices, width_x, 128), RING, 0, 0, tiled=True)
    bins = math.ceil(math.sqrt((width_x - 1) ** 2 + (width_y - 1) ** 2)) + 2
    updated, sums = pl.pallas_call(
        functools.partial(finish, scale=scale_out, bins=bins),
        out_shape=[jax.ShapeDtypeStruct(field.shape, F32), jax.ShapeDtypeStruct((1, modes), F32)],
        out_specs=[pl.BlockSpec(memory_space=pltpu.HBM), pl.BlockSpec(memory_space=pltpu.VMEM)],
        scratch_shapes=[
            pltpu.VMEM((devices * width_x, 128), F32),
            pltpu.VMEM(field.shape, F32),
            pltpu.VMEM((width_x, width_y, modes), F32),
            pltpu.VMEM((width_x, width_y, modes), F32),
            pltpu.SemaphoreType.DMA((width_x,)),
        ],
        compiler_params=params(),
        name="finish",
    )(home, field, z_table)
    lanes = modes // 128
    copies = jnp.broadcast_to(sums.reshape(1, lanes, 128).astype(BF16), (devices, lanes, 128))
    everyone = lax.all_to_all(copies, RING, 0, 0, tiled=True)
    weights = jnp.asarray((1.0 / np.maximum(shell_counts(modes), 1.0)).reshape(lanes, 128))
    spectrum = pl.pallas_call(
        mean_up, out_shape=jax.ShapeDtypeStruct((lanes, 128), F32), compiler_params=params(), name="mean_up"
    )(everyone, weights)
    return updated, spectrum.reshape(modes)


def solution(mesh):
    split = Mesh(mesh.devices.reshape(4, 4, 2, 4, 2), ROW + COL)
    placed = (P(None, ROW, COL, None),)
    return jax.shard_map(
        body, mesh=split, in_specs=placed, out_specs=(P(None, ROW, COL, None), P()), check_vma=False
    )
```

```python
import functools
import math

import jax
import jax.numpy as jnp
import numpy as np
from jax import lax
from jax.experimental import pallas as pl
from jax.experimental.pallas import tpu as pltpu
from jax.sharding import Mesh
from jax.sharding import PartitionSpec as P

ROW = ("z_lo1", "z_lo0", "y1", "y0", "core")
COL = ("x1", "x0", "z_hi")
RING = ("z_lo1", "y1", "x1", "z_hi", "z_lo0", "y0", "x0", "core")

phase_rate = 0.0002
coupling = 0.2

F32 = jnp.float32
BF16 = jnp.bfloat16


def trig(waves, points, length):
    turns = np.mod(np.asarray(waves)[:, None] * np.asarray(points)[None, :], length)
    angle = turns.astype(np.float32) * np.float32(2.0 * math.pi / length)
    return np.cos(angle).astype(np.float32), np.sin(angle).astype(np.float32)


def place(width_x, width_y, modes):
    row = functools.reduce(lambda at, axis: 2 * at + lax.axis_index(axis), ROW, 0)
    col = functools.reduce(lambda at, axis: 2 * at + lax.axis_index(axis), COL, 0)
    return row * width_x - modes // 2, col * width_y - modes // 2


def nearest(base, width):
    return jnp.maximum(base, -(base + width - 1))


def shell_of(squared):
    return jnp.floor(jnp.sqrt(squared.astype(F32)) + 0.5)


def phases(angle):
    return jnp.cos(angle), jnp.sin(angle)


def geometry(turn_ref, shell_ref, spot_ref):
    _, width_x, width_y, modes = turn_ref.shape
    base_x, base_y = place(width_x, width_y, modes)

    def square(shape, axis, base):
        wave = base + lax.broadcasted_iota(jnp.int32, shape, axis)
        return wave * wave

    square_x = square((width_x, modes), 0, base_x)
    square_y = square((width_y, modes), 0, base_y)
    square_z = square((8, modes), 1, -(modes // 2))
    cos_x, sin_x = phases(phase_rate * square_x[:, :128].astype(F32))
    cos_y, sin_y = phases(phase_rate * square_y[:, :128].astype(F32))
    cos_z, sin_z = phases(phase_rate * square_z.astype(F32))
    cos_x, sin_x, cos_y, sin_y = (jnp.concatenate([t] * (modes // 128), axis=1) for t in (cos_x, sin_x, cos_y, sin_y))
    column = square((modes, modes), 0, -(modes // 2))
    shells = lax.broadcasted_iota(jnp.int32, (modes, modes), 1).astype(F32)
    near_x = nearest(base_x, width_x)
    for block in range(width_y // 8):
        rows = slice(8 * block, 8 * block + 8)
        near_y = nearest(base_y + 8 * block, 8)
        near = near_x * near_x + near_y * near_y
        lowest = shell_of(near + square_z)
        spot_ref[block] = jnp.where(shell_of(near + column) == shells, 1.0, 0.0).astype(BF16)
        cos_yz = cos_y[rows] * cos_z - sin_y[rows] * sin_z
        sin_yz = sin_y[rows] * cos_z + cos_y[rows] * sin_z
        square_yz = square_y[rows] + square_z
        for at in range(width_x):
            cx, sx = cos_x[at : at + 1], sin_x[at : at + 1]
            turn_ref[0, at, rows] = cos_yz * cx - sin_yz * sx
            turn_ref[1, at, rows] = sin_yz * cx + cos_yz * sx
            shell_ref[at, rows] = shell_of(square_yz + square_x[at : at + 1]) - lowest


def to_slabs(
    field_hbm, table_hbm, out_ref, turn_ref, shell_ref, spot_ref, wide_ref, field, table, field_sems, table_sem, *, scale
):
    _, width_x, width, modes = field_hbm.shape
    table_copy = pltpu.make_async_copy(table_hbm, table, table_sem)
    copies = [
        pltpu.make_async_copy(field_hbm.at[:, pl.ds(at, 2)], field.at[:, pl.ds(at, 2)], field_sems.at[at // 2])
        for at in range(0, width_x, 2)
    ]
    table_copy.start()
    for copy in copies:
        copy.start()
    geometry(turn_ref, shell_ref, spot_ref)
    lane = lax.broadcasted_iota(jnp.int32, (width, modes), 1)
    sign = jnp.where(lane % 2 == 0, 1.0, -1.0)
    table_copy.wait()
    for pair in range(0, width_x, 2):
        copies[pair // 2].wait()
        rows = []
        for at in (pair, pair + 1):
            real, imag = field[0, at], field[1, at]
            for factor in (None, sign):
                if factor is not None:
                    real, imag = real * factor, imag * factor
                rows.append(jnp.concatenate([real, -imag], axis=1).astype(BF16))
                rows.append(jnp.concatenate([imag, real], axis=1).astype(BF16))
        block = jnp.concatenate(rows, axis=0)
        product = lax.dot_general(
            table[...], block, (((1,), (1,)), ((), ())), preferred_element_type=F32
        ) * scale
        for k in range(2):
            wide_ref[pl.ds(pair + k, modes, stride=width_x), :] = product[:, 128 * k : 128 * (k + 1)]
    out_ref[...] = wide_ref[...].astype(BF16).reshape(out_ref.shape)


def dot(left, right):
    return jnp.dot(left, right, preferred_element_type=F32)


def cube(parts, head):
    pr, pi, qr, qi = parts
    if head:
        first = lax.broadcasted_iota(jnp.int32, pr.shape, 0) == 0
        pick = functools.partial(jnp.where, first)
    else:
        pick = lambda special, general: general
    ar, ai = pick(pr, pr - qi), pick(pi, pi + qr)
    br, bi = pick(qr, pr + qi), pick(qi, pi - qr)
    ma = coupling * (ar * ar + ai * ai)
    mb = coupling * (br * br + bi * bi)
    ar, ai, br, bi = ma * ar, ma * ai, mb * br, mb * bi
    folded = pick(ar, ar + br), pick(ai, ai + bi), pick(br, ai - bi), pick(bi, br - ar)
    return [part.astype(BF16) for part in folded]


def planes(in_ref, ty_ref, fx_ref, fy_hbm, out_ref, back_ref, fy_ref, fy_sem, *, chunk):
    modes = fx_ref.shape[0]
    grid = 2 * modes
    half = 64
    fy_copy = pltpu.make_async_copy(fy_hbm, fy_ref, fy_sem)
    fy_copy.start()
    fx = fx_ref[...]
    tx = fx.T
    spots = [(x1, x0, z) for x1 in range(2) for x0 in range(2) for z in range(2)]
    blocks = [in_ref[:, x1, z, :, x0].reshape(modes, 128) for x1, x0, z in spots]
    lines = jnp.concatenate(
        [jnp.concatenate([b[:, half * plane : half * (plane + 1)] for b in blocks], axis=1) for plane in range(2)], axis=0
    )
    along_y = dot(lines, ty_ref[...]).astype(BF16)
    for plane in range(2):
        mine = slice(plane * modes, (plane + 1) * modes)
        for start in range(0, grid, chunk):
            real, imag = slice(start, start + chunk), slice(grid + start, grid + start + chunk)
            even_odd = dot(tx, jnp.concatenate([along_y[mine, real], along_y[mine, imag]], axis=1))
            even, odd = even_odd[:modes], even_odd[modes:]
            parts = even[:, :chunk], even[:, chunk:], odd[:, :chunk], odd[:, chunk:]
            top, rest = cube([p[:16] for p in parts], True), cube([p[16:] for p in parts], False)
            even_r, even_i, odd_i, odd_r = (jnp.concatenate(pair, axis=0) for pair in zip(top, rest))
            folded = jnp.concatenate(
                [jnp.concatenate([even_r, even_i], axis=1), jnp.concatenate([odd_i, odd_r], axis=1)], axis=0
            )
            back_x = dot(fx, folded).astype(BF16)
            back_ref[mine, real] = back_x[:, :chunk]
            back_ref[mine, imag] = back_x[:, chunk:]
    fy_copy.wait()
    done = dot(back_ref[...], fy_ref[...]).astype(BF16)
    for k, (x1, x0, z) in enumerate(spots):
        at = slice(half * k, half * (k + 1))
        message = jnp.concatenate([done[:modes, at], done[modes:, at]], axis=1)
        out_ref[:, x1, z, :, x0] = message.reshape(4, 4, 16, 128)


def finish(
    in_ref, field_ref, table_ref, turn_ref, shell_ref, spot_ref, out_hbm, sums_ref, wide_ref, out_ref, energy_ref, sems, *, scale, bins
):
    _, width_x, width_y, modes = field_ref.shape
    lane = lax.broadcasted_iota(jnp.int32, (width_y, modes), 1)
    sign = jnp.where(lane % 2 == 0, 1.0, -1.0)
    wide_ref[...] = in_ref[...].reshape(wide_ref.shape).astype(F32)
    table = table_ref[...]
    copies = [
        pltpu.make_async_copy(out_ref.at[:, pl.ds(at, 1)], out_hbm.at[:, pl.ds(at, 1)], sems.at[at])
        for at in range(width_x)
    ]
    for at in range(width_x):
        slab = wide_ref[pl.ds(at, modes, stride=width_x), :].astype(BF16)
        got = lax.dot_general(slab, table, (((0,), (0,)), ((), ())), preferred_element_type=F32)
        r0, i0, r1, i1 = (got[width_y * k : width_y * (k + 1)] for k in range(4))
        non_r = (r0[:, :modes] + i0[:, modes:] + sign * (r1[:, :modes] + i1[:, modes:])) * scale
        non_i = (i0[:, :modes] - r0[:, modes:] + sign * (i1[:, :modes] - r1[:, modes:])) * scale
        u = field_ref[0, at] - non_i
        v = field_ref[1, at] + non_r
        cos, sin = turn_ref[0, at], turn_ref[1, at]
        new_r = u * cos + v * sin
        new_i = v * cos - u * sin
        out_ref[0, at] = new_r
        out_ref[1, at] = new_i
        copies[at].start()
        energy_ref[at] = new_r * new_r + new_i * new_i
    result = jnp.zeros((1, modes), F32)
    for block in range(width_y // 8):
        rows = slice(8 * block, 8 * block + 8)
        totals = []
        for k in range(bins):
            total = jnp.zeros((8, modes), F32)
            for at in range(width_x):
                total = total + jnp.where(shell_ref[at, rows] == float(k), energy_ref[at, rows], 0.0)
            totals.append(jnp.sum(total, axis=0, keepdims=True))
        totals.extend([jnp.zeros((1, modes), F32)] * (-bins % 16))
        stacked = jnp.concatenate(totals, axis=0)
        high = stacked.astype(BF16)
        left = stacked - high.astype(F32)
        middle = left.astype(BF16)
        low = (left - middle.astype(F32)).astype(BF16)
        placed = dot(jnp.concatenate([high, middle, low], axis=0), spot_ref[block])
        count = stacked.shape[0]
        placed = placed[:count] + placed[count : 2 * count] + placed[2 * count :]
        shifted = pltpu.roll(placed, 0, 1, stride=1, stride_axis=0)
        result = result + jnp.sum(shifted, axis=0, keepdims=True)
    sums_ref[...] = result
    for copy in copies:
        copy.wait()


def mean_up(copies_ref, weight_ref, out_ref):
    out_ref[...] = jnp.sum(copies_ref[...].astype(F32), axis=0) * weight_ref[...]


def tables(modes, scale_in, scale_out):
    grid = 2 * modes
    waves = np.arange(modes) - modes // 2
    cos, sin = trig(waves, np.arange(grid), grid)
    low_cos, low_sin = cos[:, :modes].T, sin[:, :modes].T
    z_table = np.concatenate([low_cos, low_sin], axis=1)
    blocks = modes // 32
    c, s = cos.reshape(blocks, 32, grid), sin.reshape(blocks, 32, grid)
    ty = np.stack([np.concatenate([c, s], 2), np.concatenate([-s, c], 2)], 1).reshape(2 * modes, 2 * grid)
    ct, st = c.transpose(2, 0, 1), s.transpose(2, 0, 1)
    fy = np.stack([np.stack([ct, -st], 2), np.stack([st, ct], 2)], 0).reshape(2 * grid, 2 * modes)
    odd = low_sin.copy()
    odd[0] = cos[:, modes]
    tx = np.concatenate([low_cos, odd], axis=0)
    bits = np.arange(modes).reshape(2, 2, 2, 2, 2, modes // 32)
    fx = tx.T[bits.transpose(0, 2, 1, 3, 4, 5).reshape(-1)]
    scaled = (z_table, ty * scale_in, fx * scale_in, fy * (scale_out * scale_out / scale_in))
    return [jnp.asarray(np.ascontiguousarray(t), BF16) for t in scaled]


def shell_counts(modes):
    wave = np.arange(modes) - modes // 2
    square = wave * wave
    total = square[:, None, None] + square[None, :, None] + square[None, None, :]
    shell = np.floor(np.sqrt(total.astype(np.float32)) + np.float32(0.5)).astype(np.int64)
    return np.bincount(shell.reshape(-1), minlength=modes)[:modes].astype(np.float32)


def in_hbm(array):
    return pltpu.with_memory_space_constraint(array, pltpu.HBM)


def params():
    return pltpu.CompilerParams(vmem_limit_bytes=48 * 1024 * 1024)


def body(field):
    _, width_x, width_y, modes = field.shape
    devices = math.prod(lax.axis_size(axis) for axis in RING)
    scale_in = 1.0 / math.sqrt(modes)
    scale_out = math.sqrt(modes) / (2 * modes)
    z_table, ty, fx, fy = tables(modes, scale_in, scale_out)
    messages, turn, shell, spot = pl.pallas_call(
        functools.partial(to_slabs, scale=scale_in),
        in_specs=[pl.BlockSpec(memory_space=pltpu.HBM)] * 2,
        out_shape=[
            jax.ShapeDtypeStruct((devices, width_x, 128), BF16),
            jax.ShapeDtypeStruct(field.shape, F32),
            jax.ShapeDtypeStruct(field.shape[1:], F32),
            jax.ShapeDtypeStruct((width_y // 8, modes, modes), BF16),
        ],
        scratch_shapes=[
            pltpu.VMEM((devices * width_x, 128), F32),
            pltpu.VMEM(field.shape, F32),
            pltpu.VMEM(z_table.shape, BF16),
            pltpu.SemaphoreType.DMA((width_x // 2,)),
            pltpu.SemaphoreType.DMA(()),
        ],
        compiler_params=params(),
        name="to_slabs",
    )(in_hbm(field), in_hbm(z_table))
    slabs = lax.all_to_all(messages, RING, 0, 0, tiled=True)
    shape = (4, 2, 2, 4, 2, 2 * width_x, 128)
    back = pl.pallas_call(
        functools.partial(planes, chunk=128),
        in_specs=[pl.BlockSpec(memory_space=pltpu.VMEM)] * 3 + [pl.BlockSpec(memory_space=pltpu.HBM)],
        out_shape=jax.ShapeDtypeStruct(shape, BF16),
        scratch_shapes=[
            pltpu.VMEM((2 * modes, 4 * modes), BF16),
            pltpu.VMEM(fy.shape, BF16),
            pltpu.SemaphoreType.DMA(()),
        ],
        compiler_params=params(),
        name="planes",
    )(slabs.reshape(shape), ty, fx, in_hbm(fy))
    home = lax.all_to_all(back.reshape(devices, width_x, 128), RING, 0, 0, tiled=True)
    bins = math.ceil(math.sqrt((width_x - 1) ** 2 + 49)) + 2
    updated, sums = pl.pallas_call(
        functools.partial(finish, scale=scale_out, bins=bins),
        out_shape=[jax.ShapeDtypeStruct(field.shape, F32), jax.ShapeDtypeStruct((1, modes), F32)],
        out_specs=[pl.BlockSpec(memory_space=pltpu.HBM), pl.BlockSpec(memory_space=pltpu.VMEM)],
        scratch_shapes=[
            pltpu.VMEM((devices * width_x, 128), F32),
            pltpu.VMEM(field.shape, F32),
            pltpu.VMEM((width_x, width_y, modes), F32),
            pltpu.SemaphoreType.DMA((width_x,)),
        ],
        compiler_params=params(),
        name="finish",
    )(home, field, z_table, turn, shell, spot)
    lanes = modes // 128
    copies = jnp.broadcast_to(sums.reshape(1, lanes, 128).astype(BF16), (devices, lanes, 128))
    everyone = lax.all_to_all(copies, RING, 0, 0, tiled=True)
    weights = jnp.asarray((1.0 / np.maximum(shell_counts(modes), 1.0)).reshape(lanes, 128))
    spectrum = pl.pallas_call(
        mean_up, out_shape=jax.ShapeDtypeStruct((lanes, 128), F32), compiler_params=params(), name="mean_up"
    )(everyone, weights)
    return updated, spectrum.reshape(modes)


def solution(mesh):
    split = Mesh(mesh.devices.reshape((2,) * 8), ROW + COL)
    placed = (P(None, ROW, COL, None),)
    return jax.shard_map(
        body, mesh=split, in_specs=placed, out_specs=(P(None, ROW, COL, None), P()), check_vma=False
    )
```

```python
import functools
import math

import jax
import jax.numpy as jnp
import numpy as np
from jax import lax
from jax.experimental import pallas as pl
from jax.experimental.pallas import tpu as pltpu
from jax.sharding import Mesh
from jax.sharding import PartitionSpec as P

ROW = ("z_lo1", "z_lo0", "y1", "y0", "core")
COL = ("x1", "x0", "z_hi")
RING = ("z_lo1", "y1", "x1", "z_hi", "z_lo0", "y0", "x0", "core")

phase_rate = 0.0002
coupling = 0.2

F32 = jnp.float32
BF16 = jnp.bfloat16


def trig(waves, points, length):
    turns = np.mod(np.asarray(waves)[:, None] * np.asarray(points)[None, :], length)
    angle = turns.astype(np.float32) * np.float32(2.0 * math.pi / length)
    return np.cos(angle).astype(np.float32), np.sin(angle).astype(np.float32)


def place(width_x, width_y, modes):
    row = functools.reduce(lambda at, axis: 2 * at + lax.axis_index(axis), ROW, 0)
    col = functools.reduce(lambda at, axis: 2 * at + lax.axis_index(axis), COL, 0)
    return row * width_x - modes // 2, col * width_y - modes // 2


def nearest(base, width):
    return jnp.maximum(base, -(base + width - 1))


def shell_of(squared):
    return jnp.floor(jnp.sqrt(squared.astype(F32)) + 0.5)


def phases(angle):
    return jnp.cos(angle), jnp.sin(angle)


def geometry(turn_ref, shell_ref, spot_ref):
    _, width_x, width_y, modes = turn_ref.shape
    base_x, base_y = place(width_x, width_y, modes)

    def square(shape, axis, base):
        wave = base + lax.broadcasted_iota(jnp.int32, shape, axis)
        return wave * wave

    square_x = square((width_x, modes), 0, base_x)
    square_y = square((width_y, modes), 0, base_y)
    square_z = square((8, modes), 1, -(modes // 2))
    cos_x, sin_x = phases(phase_rate * square_x[:, :128].astype(F32))
    cos_y, sin_y = phases(phase_rate * square_y[:, :128].astype(F32))
    cos_z, sin_z = phases(phase_rate * square_z.astype(F32))
    cos_x, sin_x, cos_y, sin_y = (jnp.concatenate([t] * (modes // 128), axis=1) for t in (cos_x, sin_x, cos_y, sin_y))
    column = square((modes, modes), 0, -(modes // 2))
    shells = lax.broadcasted_iota(jnp.int32, (modes, modes), 1).astype(F32)
    near_x = nearest(base_x, width_x)
    for block in range(width_y // 8):
        rows = slice(8 * block, 8 * block + 8)
        near_y = nearest(base_y + 8 * block, 8)
        near = near_x * near_x + near_y * near_y
        lowest = shell_of(near + square_z)
        spot_ref[block] = jnp.where(shell_of(near + column) == shells, 1.0, 0.0).astype(BF16)
        cos_yz = cos_y[rows] * cos_z - sin_y[rows] * sin_z
        sin_yz = sin_y[rows] * cos_z + cos_y[rows] * sin_z
        square_yz = square_y[rows] + square_z
        for at in range(width_x):
            cx, sx = cos_x[at : at + 1], sin_x[at : at + 1]
            turn_ref[0, at, rows] = cos_yz * cx - sin_yz * sx
            turn_ref[1, at, rows] = sin_yz * cx + cos_yz * sx
            shell_ref[at, rows] = shell_of(square_yz + square_x[at : at + 1]) - lowest


def to_slabs(
    field_hbm, table_hbm, ty_hbm, fy_hbm, out_ref, turn_ref, shell_ref, spot_ref, ty_ref, fy_ref, wide_ref, field, table, sems, *, scale
):
    _, width_x, width, modes = field_hbm.shape
    pairs = (table_hbm, table), (field_hbm, field), (ty_hbm, ty_ref), (fy_hbm, fy_ref)
    copies = [pltpu.make_async_copy(source, target, sems.at[k]) for k, (source, target) in enumerate(pairs)]
    for copy in copies:
        copy.start()
    geometry(turn_ref, shell_ref, spot_ref)
    lane = lax.broadcasted_iota(jnp.int32, (width, modes), 1)
    sign = jnp.where(lane % 2 == 0, 1.0, -1.0)
    copies[0].wait()
    copies[1].wait()
    for pair in range(0, width_x, 2):
        rows = []
        for at in (pair, pair + 1):
            real, imag = field[0, at], field[1, at]
            for factor in (None, sign):
                if factor is not None:
                    real, imag = real * factor, imag * factor
                rows.append(jnp.concatenate([real, -imag], axis=1).astype(BF16))
                rows.append(jnp.concatenate([imag, real], axis=1).astype(BF16))
        block = jnp.concatenate(rows, axis=0)
        product = lax.dot_general(
            table[...], block, (((1,), (1,)), ((), ())), preferred_element_type=F32
        ) * scale
        for k in range(2):
            wide_ref[pl.ds(pair + k, modes, stride=width_x), :] = product[:, 128 * k : 128 * (k + 1)]
    out_ref[...] = wide_ref[...].astype(BF16).reshape(out_ref.shape)
    copies[2].wait()
    copies[3].wait()


def dot(left, right):
    return jnp.dot(left, right, preferred_element_type=F32)


def cube(parts, head):
    pr, pi, qr, qi = parts
    if head:
        first = lax.broadcasted_iota(jnp.int32, pr.shape, 0) == 0
        pick = functools.partial(jnp.where, first)
    else:
        pick = lambda special, general: general
    ar, ai = pick(pr, pr - qi), pick(pi, pi + qr)
    br, bi = pick(qr, pr + qi), pick(qi, pi - qr)
    ma = coupling * (ar * ar + ai * ai)
    mb = coupling * (br * br + bi * bi)
    ar, ai, br, bi = ma * ar, ma * ai, mb * br, mb * bi
    folded = pick(ar, ar + br), pick(ai, ai + bi), pick(br, ai - bi), pick(bi, br - ar)
    return [part.astype(BF16) for part in folded]


def planes(in_ref, ty_ref, fx_ref, fy_ref, out_ref, back_ref, *, chunk):
    modes = fx_ref.shape[0]
    grid = 2 * modes
    half = 64
    fx = fx_ref[...]
    tx = fx.T
    spots = [(x1, x0, z) for x1 in range(2) for x0 in range(2) for z in range(2)]
    blocks = [in_ref[:, x1, z, :, x0].reshape(modes, 128) for x1, x0, z in spots]
    lines = jnp.concatenate(
        [jnp.concatenate([b[:, half * plane : half * (plane + 1)] for b in blocks], axis=1) for plane in range(2)], axis=0
    )
    along_y = dot(lines, ty_ref[...]).astype(BF16)
    for plane in range(2):
        mine = slice(plane * modes, (plane + 1) * modes)
        for start in range(0, grid, chunk):
            real, imag = slice(start, start + chunk), slice(grid + start, grid + start + chunk)
            even_odd = dot(tx, jnp.concatenate([along_y[mine, real], along_y[mine, imag]], axis=1))
            even, odd = even_odd[:modes], even_odd[modes:]
            parts = even[:, :chunk], even[:, chunk:], odd[:, :chunk], odd[:, chunk:]
            top, rest = cube([p[:16] for p in parts], True), cube([p[16:] for p in parts], False)
            even_r, even_i, odd_i, odd_r = (jnp.concatenate(pair, axis=0) for pair in zip(top, rest))
            folded = jnp.concatenate(
                [jnp.concatenate([even_r, even_i], axis=1), jnp.concatenate([odd_i, odd_r], axis=1)], axis=0
            )
            back_x = dot(fx, folded).astype(BF16)
            back_ref[mine, real] = back_x[:, :chunk]
            back_ref[mine, imag] = back_x[:, chunk:]
    done = dot(back_ref[...], fy_ref[...]).astype(BF16)
    for k, (x1, x0, z) in enumerate(spots):
        at = slice(half * k, half * (k + 1))
        message = jnp.concatenate([done[:modes, at], done[modes:, at]], axis=1)
        out_ref[:, x1, z, :, x0] = message.reshape(4, 4, 16, 128)


def finish(
    in_ref, field_ref, table_ref, turn_ref, shell_ref, spot_ref, out_hbm, sums_ref, wide_ref, out_ref, energy_ref, sems, *, scale, bins
):
    _, width_x, width_y, modes = field_ref.shape
    lane = lax.broadcasted_iota(jnp.int32, (width_y, modes), 1)
    sign = jnp.where(lane % 2 == 0, 1.0, -1.0)
    wide_ref[...] = in_ref[...].reshape(wide_ref.shape).astype(F32)
    table = table_ref[...]
    copies = [
        pltpu.make_async_copy(out_ref.at[:, pl.ds(at, 1)], out_hbm.at[:, pl.ds(at, 1)], sems.at[at])
        for at in range(width_x)
    ]
    for at in range(width_x):
        slab = wide_ref[pl.ds(at, modes, stride=width_x), :].astype(BF16)
        got = lax.dot_general(slab, table, (((0,), (0,)), ((), ())), preferred_element_type=F32)
        r0, i0, r1, i1 = (got[width_y * k : width_y * (k + 1)] for k in range(4))
        non_r = (r0[:, :modes] + i0[:, modes:] + sign * (r1[:, :modes] + i1[:, modes:])) * scale
        non_i = (i0[:, :modes] - r0[:, modes:] + sign * (i1[:, :modes] - r1[:, modes:])) * scale
        u = field_ref[0, at] - non_i
        v = field_ref[1, at] + non_r
        cos, sin = turn_ref[0, at], turn_ref[1, at]
        new_r = u * cos + v * sin
        new_i = v * cos - u * sin
        out_ref[0, at] = new_r
        out_ref[1, at] = new_i
        copies[at].start()
        energy_ref[at] = new_r * new_r + new_i * new_i
    result = jnp.zeros((1, modes), F32)
    for block in range(width_y // 8):
        rows = slice(8 * block, 8 * block + 8)
        totals = []
        for k in range(bins):
            total = jnp.zeros((8, modes), F32)
            for at in range(width_x):
                total = total + jnp.where(shell_ref[at, rows] == float(k), energy_ref[at, rows], 0.0)
            totals.append(jnp.sum(total, axis=0, keepdims=True))
        totals.extend([jnp.zeros((1, modes), F32)] * (-bins % 16))
        stacked = jnp.concatenate(totals, axis=0)
        high = stacked.astype(BF16)
        left = stacked - high.astype(F32)
        middle = left.astype(BF16)
        low = (left - middle.astype(F32)).astype(BF16)
        placed = dot(jnp.concatenate([high, middle, low], axis=0), spot_ref[block])
        count = stacked.shape[0]
        placed = placed[:count] + placed[count : 2 * count] + placed[2 * count :]
        shifted = pltpu.roll(placed, 0, 1, stride=1, stride_axis=0)
        result = result + jnp.sum(shifted, axis=0, keepdims=True)
    sums_ref[...] = result
    for copy in copies:
        copy.wait()


def mean_up(copies_ref, weight_ref, out_ref):
    out_ref[...] = jnp.sum(copies_ref[...].astype(F32), axis=0) * weight_ref[...]


def tables(modes, scale_in, scale_out):
    grid = 2 * modes
    waves = np.arange(modes) - modes // 2
    cos, sin = trig(waves, np.arange(grid), grid)
    low_cos, low_sin = cos[:, :modes].T, sin[:, :modes].T
    z_table = np.concatenate([low_cos, low_sin], axis=1)
    blocks = modes // 32
    c, s = cos.reshape(blocks, 32, grid), sin.reshape(blocks, 32, grid)
    ty = np.stack([np.concatenate([c, s], 2), np.concatenate([-s, c], 2)], 1).reshape(2 * modes, 2 * grid)
    ct, st = c.transpose(2, 0, 1), s.transpose(2, 0, 1)
    fy = np.stack([np.stack([ct, -st], 2), np.stack([st, ct], 2)], 0).reshape(2 * grid, 2 * modes)
    odd = low_sin.copy()
    odd[0] = cos[:, modes]
    tx = np.concatenate([low_cos, odd], axis=0)
    bits = np.arange(modes).reshape(2, 2, 2, 2, 2, modes // 32)
    fx = tx.T[bits.transpose(0, 2, 1, 3, 4, 5).reshape(-1)]
    scaled = (z_table, ty * scale_in, fx * scale_in, fy * (scale_out * scale_out / scale_in))
    return [jnp.asarray(np.ascontiguousarray(t), BF16) for t in scaled]


def shell_counts(modes):
    wave = np.arange(modes) - modes // 2
    square = wave * wave
    total = square[:, None, None] + square[None, :, None] + square[None, None, :]
    shell = np.floor(np.sqrt(total.astype(np.float32)) + np.float32(0.5)).astype(np.int64)
    return np.bincount(shell.reshape(-1), minlength=modes)[:modes].astype(np.float32)


def in_hbm(array):
    return pltpu.with_memory_space_constraint(array, pltpu.HBM)


def params():
    return pltpu.CompilerParams(vmem_limit_bytes=48 * 1024 * 1024)


def body(field):
    _, width_x, width_y, modes = field.shape
    devices = math.prod(lax.axis_size(axis) for axis in RING)
    scale_in = 1.0 / math.sqrt(modes)
    scale_out = math.sqrt(modes) / (2 * modes)
    z_table, ty, fx, fy = tables(modes, scale_in, scale_out)
    messages, turn, shell, spot, near_ty, near_fy = pl.pallas_call(
        functools.partial(to_slabs, scale=scale_in),
        in_specs=[pl.BlockSpec(memory_space=pltpu.HBM)] * 4,
        out_shape=[
            jax.ShapeDtypeStruct((devices, width_x, 128), BF16),
            jax.ShapeDtypeStruct(field.shape, F32),
            jax.ShapeDtypeStruct(field.shape[1:], F32),
            jax.ShapeDtypeStruct((width_y // 8, modes, modes), BF16),
            jax.ShapeDtypeStruct(ty.shape, BF16),
            jax.ShapeDtypeStruct(fy.shape, BF16),
        ],
        scratch_shapes=[
            pltpu.VMEM((devices * width_x, 128), F32),
            pltpu.VMEM(field.shape, F32),
            pltpu.VMEM(z_table.shape, BF16),
            pltpu.SemaphoreType.DMA((4,)),
        ],
        compiler_params=params(),
        name="to_slabs",
    )(in_hbm(field), in_hbm(z_table), in_hbm(ty), in_hbm(fy))
    slabs = lax.all_to_all(messages, RING, 0, 0, tiled=True)
    shape = (4, 2, 2, 4, 2, 2 * width_x, 128)
    back = pl.pallas_call(
        functools.partial(planes, chunk=128),
        out_shape=jax.ShapeDtypeStruct(shape, BF16),
        scratch_shapes=[pltpu.VMEM((2 * modes, 4 * modes), BF16)],
        compiler_params=params(),
        name="planes",
    )(slabs.reshape(shape), near_ty, fx, near_fy)
    home = lax.all_to_all(back.reshape(devices, width_x, 128), RING, 0, 0, tiled=True)
    bins = math.ceil(math.sqrt((width_x - 1) ** 2 + 49)) + 2
    updated, sums = pl.pallas_call(
        functools.partial(finish, scale=scale_out, bins=bins),
        out_shape=[jax.ShapeDtypeStruct(field.shape, F32), jax.ShapeDtypeStruct((1, modes), F32)],
        out_specs=[pl.BlockSpec(memory_space=pltpu.HBM), pl.BlockSpec(memory_space=pltpu.VMEM)],
        scratch_shapes=[
            pltpu.VMEM((devices * width_x, 128), F32),
            pltpu.VMEM(field.shape, F32),
            pltpu.VMEM((width_x, width_y, modes), F32),
            pltpu.SemaphoreType.DMA((width_x,)),
        ],
        compiler_params=params(),
        name="finish",
    )(home, field, z_table, turn, shell, spot)
    lanes = modes // 128
    copies = jnp.broadcast_to(sums.reshape(1, lanes, 128).astype(BF16), (devices, lanes, 128))
    everyone = lax.all_to_all(copies, RING, 0, 0, tiled=True)
    weights = jnp.asarray((1.0 / np.maximum(shell_counts(modes), 1.0)).reshape(lanes, 128))
    spectrum = pl.pallas_call(
        mean_up, out_shape=jax.ShapeDtypeStruct((lanes, 128), F32), compiler_params=params(), name="mean_up"
    )(everyone, weights)
    return updated, spectrum.reshape(modes)


def solution(mesh):
    split = Mesh(mesh.devices.reshape((2,) * 8), ROW + COL)
    placed = (P(None, ROW, COL, None),)
    return jax.shard_map(
        body, mesh=split, in_specs=placed, out_specs=(P(None, ROW, COL, None), P()), check_vma=False
    )
```

```python
import functools
import math

import jax
import jax.numpy as jnp
import numpy as np
from jax import lax
from jax.experimental import pallas as pl
from jax.experimental.pallas import tpu as pltpu
from jax.sharding import Mesh
from jax.sharding import PartitionSpec as P

ROW = ("z_lo1", "z_lo0", "y1", "y0", "core")
COL = ("x1", "x0", "z_hi")
RING = ("z_lo1", "y1", "x1", "z_hi", "z_lo0", "y0", "x0", "core")

phase_rate = 0.0002
coupling = 0.2

F32 = jnp.float32
BF16 = jnp.bfloat16


def trig(waves, points, length):
    turns = np.mod(np.asarray(waves)[:, None] * np.asarray(points)[None, :], length)
    angle = turns.astype(np.float32) * np.float32(2.0 * math.pi / length)
    return np.cos(angle).astype(np.float32), np.sin(angle).astype(np.float32)


def place(width_x, width_y, modes):
    row = functools.reduce(lambda at, axis: 2 * at + lax.axis_index(axis), ROW, 0)
    col = functools.reduce(lambda at, axis: 2 * at + lax.axis_index(axis), COL, 0)
    return row * width_x - modes // 2, col * width_y - modes // 2


def nearest(base, width):
    return jnp.maximum(base, -(base + width - 1))


def shell_of(squared):
    return jnp.floor(jnp.sqrt(squared.astype(F32)) + 0.5)


def phases(angle):
    return jnp.cos(angle), jnp.sin(angle)


def geometry(turn_ref, shell_ref, spot_ref):
    _, width_x, width_y, modes = turn_ref.shape
    base_x, base_y = place(width_x, width_y, modes)

    def square(shape, axis, base):
        wave = base + lax.broadcasted_iota(jnp.int32, shape, axis)
        return wave * wave

    square_x = square((width_x, modes), 0, base_x)
    square_y = square((width_y, modes), 0, base_y)
    square_z = square((8, modes), 1, -(modes // 2))
    cos_x, sin_x = phases(phase_rate * square_x[:, :128].astype(F32))
    cos_y, sin_y = phases(phase_rate * square_y[:, :128].astype(F32))
    cos_z, sin_z = phases(phase_rate * square_z.astype(F32))
    cos_x, sin_x, cos_y, sin_y = (jnp.concatenate([t] * (modes // 128), axis=1) for t in (cos_x, sin_x, cos_y, sin_y))
    column = square((modes, modes), 0, -(modes // 2))
    shells = lax.broadcasted_iota(jnp.int32, (modes, modes), 1).astype(F32)
    near_x = nearest(base_x, width_x)
    for block in range(width_y // 8):
        rows = slice(8 * block, 8 * block + 8)
        near_y = nearest(base_y + 8 * block, 8)
        near = near_x * near_x + near_y * near_y
        lowest = shell_of(near + square_z)
        spot_ref[block] = jnp.where(shell_of(near + column) == shells, 1.0, 0.0).astype(BF16)
        cos_yz = cos_y[rows] * cos_z - sin_y[rows] * sin_z
        sin_yz = sin_y[rows] * cos_z + cos_y[rows] * sin_z
        square_yz = square_y[rows] + square_z
        for at in range(width_x):
            cx, sx = cos_x[at : at + 1], sin_x[at : at + 1]
            turn_ref[0, at, rows] = cos_yz * cx - sin_yz * sx
            turn_ref[1, at, rows] = sin_yz * cx + cos_yz * sx
            shell_ref[at, rows] = shell_of(square_yz + square_x[at : at + 1]) - lowest


def to_slabs(
    field_hbm, table_hbm, ty_hbm, fy_hbm, out_ref, turn_ref, shell_ref, spot_ref, ty_ref, fy_ref, wide_ref, field, table, sems, *, scale
):
    _, width_x, width, modes = field_hbm.shape
    pairs = (table_hbm, table), (field_hbm, field), (ty_hbm, ty_ref), (fy_hbm, fy_ref)
    copies = [pltpu.make_async_copy(source, target, sems.at[k]) for k, (source, target) in enumerate(pairs)]
    for copy in copies:
        copy.start()
    geometry(turn_ref, shell_ref, spot_ref)
    lane = lax.broadcasted_iota(jnp.int32, (width, modes), 1)
    sign = jnp.where(lane % 2 == 0, 1.0, -1.0)
    copies[0].wait()
    copies[1].wait()
    for pair in range(0, width_x, 2):
        rows = []
        for at in (pair, pair + 1):
            real, imag = field[0, at], field[1, at]
            for factor in (None, sign):
                if factor is not None:
                    real, imag = real * factor, imag * factor
                rows.append(jnp.concatenate([real, -imag], axis=1).astype(BF16))
                rows.append(jnp.concatenate([imag, real], axis=1).astype(BF16))
        block = jnp.concatenate(rows, axis=0)
        product = lax.dot_general(
            table[...], block, (((1,), (1,)), ((), ())), preferred_element_type=F32
        ) * scale
        for k in range(2):
            wide_ref[pl.ds(pair + k, modes, stride=width_x), :] = product[:, 128 * k : 128 * (k + 1)]
    out_ref[...] = wide_ref[...].astype(BF16).reshape(out_ref.shape)
    copies[2].wait()
    copies[3].wait()


def dot(left, right):
    return jnp.dot(left, right, preferred_element_type=F32)


def cube(parts, head):
    pr, pi, qr, qi = parts
    if head:
        first = lax.broadcasted_iota(jnp.int32, pr.shape, 0) == 0
        pick = functools.partial(jnp.where, first)
    else:
        pick = lambda special, general: general
    ar, ai = pick(pr, pr - qi), pick(pi, pi + qr)
    br, bi = pick(qr, pr + qi), pick(qi, pi - qr)
    ma = coupling * (ar * ar + ai * ai)
    mb = coupling * (br * br + bi * bi)
    ar, ai, br, bi = ma * ar, ma * ai, mb * br, mb * bi
    folded = pick(ar, ar + br), pick(ai, ai + bi), pick(br, ai - bi), pick(bi, br - ar)
    return [part.astype(BF16) for part in folded]


def planes(in_ref, ty_ref, fx_ref, fy_ref, out_ref, back_ref, *, chunk):
    modes = fx_ref.shape[0]
    grid = 2 * modes
    half = 64
    fx = fx_ref[...]
    tx = fx.T
    spots = [(x1, x0, z) for x1 in range(2) for x0 in range(2) for z in range(2)]
    blocks = [in_ref[:, x1, z, :, x0].reshape(modes, 128) for x1, x0, z in spots]
    lines = jnp.concatenate(
        [jnp.concatenate([b[:, half * plane : half * (plane + 1)] for b in blocks], axis=1) for plane in range(2)], axis=0
    )
    along_y = dot(lines, ty_ref[...]).astype(BF16)
    for plane in range(2):
        mine = slice(plane * modes, (plane + 1) * modes)
        for start in range(0, grid, chunk):
            real, imag = slice(start, start + chunk), slice(grid + start, grid + start + chunk)
            even_odd = dot(tx, jnp.concatenate([along_y[mine, real], along_y[mine, imag]], axis=1))
            even, odd = even_odd[:modes], even_odd[modes:]
            parts = even[:, :chunk], even[:, chunk:], odd[:, :chunk], odd[:, chunk:]
            top, rest = cube([p[:16] for p in parts], True), cube([p[16:] for p in parts], False)
            even_r, even_i, odd_i, odd_r = (jnp.concatenate(pair, axis=0) for pair in zip(top, rest))
            folded = jnp.concatenate(
                [jnp.concatenate([even_r, even_i], axis=1), jnp.concatenate([odd_i, odd_r], axis=1)], axis=0
            )
            back_x = dot(fx, folded).astype(BF16)
            back_ref[mine, real] = back_x[:, :chunk]
            back_ref[mine, imag] = back_x[:, chunk:]
    done = dot(back_ref[...], fy_ref[...]).astype(BF16)
    for k, (x1, x0, z) in enumerate(spots):
        at = slice(half * k, half * (k + 1))
        message = jnp.concatenate([done[:modes, at], done[modes:, at]], axis=1)
        out_ref[:, x1, z, :, x0] = message.reshape(4, 4, 16, 128)


def finish(
    in_ref, field_ref, table_ref, turn_ref, shell_ref, spot_ref, weight_ref, out_hbm, sums_ref, wide_ref, out_ref, energy_ref, sems, *, scale, bins
):
    _, width_x, width_y, modes = field_ref.shape
    lane = lax.broadcasted_iota(jnp.int32, (width_y, modes), 1)
    sign = jnp.where(lane % 2 == 0, 1.0, -1.0)
    wide_ref[...] = in_ref[...].reshape(wide_ref.shape).astype(F32)
    table = table_ref[...]
    copies = [
        pltpu.make_async_copy(out_ref.at[:, pl.ds(at, 1)], out_hbm.at[:, pl.ds(at, 1)], sems.at[at])
        for at in range(width_x)
    ]
    for at in range(width_x):
        slab = wide_ref[pl.ds(at, modes, stride=width_x), :].astype(BF16)
        got = lax.dot_general(slab, table, (((0,), (0,)), ((), ())), preferred_element_type=F32)
        r0, i0, r1, i1 = (got[width_y * k : width_y * (k + 1)] for k in range(4))
        non_r = (r0[:, :modes] + i0[:, modes:] + sign * (r1[:, :modes] + i1[:, modes:])) * scale
        non_i = (i0[:, :modes] - r0[:, modes:] + sign * (i1[:, :modes] - r1[:, modes:])) * scale
        u = field_ref[0, at] - non_i
        v = field_ref[1, at] + non_r
        cos, sin = turn_ref[0, at], turn_ref[1, at]
        new_r = u * cos + v * sin
        new_i = v * cos - u * sin
        out_ref[0, at] = new_r
        out_ref[1, at] = new_i
        copies[at].start()
        energy_ref[at] = new_r * new_r + new_i * new_i
    result = jnp.zeros((1, modes), F32)
    for block in range(width_y // 8):
        rows = slice(8 * block, 8 * block + 8)
        totals = []
        for k in range(bins):
            total = jnp.zeros((8, modes), F32)
            for at in range(width_x):
                total = total + jnp.where(shell_ref[at, rows] == float(k), energy_ref[at, rows], 0.0)
            totals.append(jnp.sum(total, axis=0, keepdims=True))
        totals.extend([jnp.zeros((1, modes), F32)] * (-bins % 16))
        stacked = jnp.concatenate(totals, axis=0)
        high = stacked.astype(BF16)
        left = stacked - high.astype(F32)
        middle = left.astype(BF16)
        low = (left - middle.astype(F32)).astype(BF16)
        placed = dot(jnp.concatenate([high, middle, low], axis=0), spot_ref[block])
        count = stacked.shape[0]
        placed = placed[:count] + placed[count : 2 * count] + placed[2 * count :]
        shifted = pltpu.roll(placed, 0, 1, stride=1, stride_axis=0)
        result = result + jnp.sum(shifted, axis=0, keepdims=True)
    sums_ref[...] = result * weight_ref[...]
    for copy in copies:
        copy.wait()


def add_up(copies_ref, out_ref):
    total = jnp.sum(copies_ref[...].astype(F32), axis=0)
    lanes = out_ref.shape[0]
    out_ref[...] = jnp.sum(total.reshape(-1, lanes, 128), axis=0)


def tables(modes, scale_in, scale_out):
    grid = 2 * modes
    waves = np.arange(modes) - modes // 2
    cos, sin = trig(waves, np.arange(grid), grid)
    low_cos, low_sin = cos[:, :modes].T, sin[:, :modes].T
    z_table = np.concatenate([low_cos, low_sin], axis=1)
    blocks = modes // 32
    c, s = cos.reshape(blocks, 32, grid), sin.reshape(blocks, 32, grid)
    ty = np.stack([np.concatenate([c, s], 2), np.concatenate([-s, c], 2)], 1).reshape(2 * modes, 2 * grid)
    ct, st = c.transpose(2, 0, 1), s.transpose(2, 0, 1)
    fy = np.stack([np.stack([ct, -st], 2), np.stack([st, ct], 2)], 0).reshape(2 * grid, 2 * modes)
    odd = low_sin.copy()
    odd[0] = cos[:, modes]
    tx = np.concatenate([low_cos, odd], axis=0)
    bits = np.arange(modes).reshape(2, 2, 2, 2, 2, modes // 32)
    fx = tx.T[bits.transpose(0, 2, 1, 3, 4, 5).reshape(-1)]
    scaled = (z_table, ty * scale_in, fx * scale_in, fy * (scale_out * scale_out / scale_in))
    return [jnp.asarray(np.ascontiguousarray(t), BF16) for t in scaled]


def shell_counts(modes):
    wave = np.arange(modes) - modes // 2
    square = wave * wave
    total = square[:, None, None] + square[None, :, None] + square[None, None, :]
    shell = np.floor(np.sqrt(total.astype(np.float32)) + np.float32(0.5)).astype(np.int64)
    return np.bincount(shell.reshape(-1), minlength=modes)[:modes].astype(np.float32)


def in_hbm(array):
    return pltpu.with_memory_space_constraint(array, pltpu.HBM)


def params():
    return pltpu.CompilerParams(vmem_limit_bytes=48 * 1024 * 1024)


def body(field):
    _, width_x, width_y, modes = field.shape
    devices = math.prod(lax.axis_size(axis) for axis in RING)
    scale_in = 1.0 / math.sqrt(modes)
    scale_out = math.sqrt(modes) / (2 * modes)
    z_table, ty, fx, fy = tables(modes, scale_in, scale_out)
    messages, turn, shell, spot, near_ty, near_fy = pl.pallas_call(
        functools.partial(to_slabs, scale=scale_in),
        in_specs=[pl.BlockSpec(memory_space=pltpu.HBM)] * 4,
        out_shape=[
            jax.ShapeDtypeStruct((devices, width_x, 128), BF16),
            jax.ShapeDtypeStruct(field.shape, F32),
            jax.ShapeDtypeStruct(field.shape[1:], F32),
            jax.ShapeDtypeStruct((width_y // 8, modes, modes), BF16),
            jax.ShapeDtypeStruct(ty.shape, BF16),
            jax.ShapeDtypeStruct(fy.shape, BF16),
        ],
        scratch_shapes=[
            pltpu.VMEM((devices * width_x, 128), F32),
            pltpu.VMEM(field.shape, F32),
            pltpu.VMEM(z_table.shape, BF16),
            pltpu.SemaphoreType.DMA((4,)),
        ],
        compiler_params=params(),
        name="to_slabs",
    )(in_hbm(field), in_hbm(z_table), in_hbm(ty), in_hbm(fy))
    slabs = lax.all_to_all(messages, RING, 0, 0, tiled=True)
    shape = (4, 2, 2, 4, 2, 2 * width_x, 128)
    back = pl.pallas_call(
        functools.partial(planes, chunk=128),
        out_shape=jax.ShapeDtypeStruct(shape, BF16),
        scratch_shapes=[pltpu.VMEM((2 * modes, 4 * modes), BF16)],
        compiler_params=params(),
        name="planes",
    )(slabs.reshape(shape), near_ty, fx, near_fy)
    home = lax.all_to_all(back.reshape(devices, width_x, 128), RING, 0, 0, tiled=True)
    bins = math.ceil(math.sqrt((width_x - 1) ** 2 + 49)) + 2
    weights = jnp.asarray((1.0 / np.maximum(shell_counts(modes), 1.0)).reshape(1, modes))
    updated, sums = pl.pallas_call(
        functools.partial(finish, scale=scale_out, bins=bins),
        out_shape=[jax.ShapeDtypeStruct(field.shape, F32), jax.ShapeDtypeStruct((1, modes), F32)],
        out_specs=[pl.BlockSpec(memory_space=pltpu.HBM), pl.BlockSpec(memory_space=pltpu.VMEM)],
        scratch_shapes=[
            pltpu.VMEM((devices * width_x, 128), F32),
            pltpu.VMEM(field.shape, F32),
            pltpu.VMEM((width_x, width_y, modes), F32),
            pltpu.SemaphoreType.DMA((width_x,)),
        ],
        compiler_params=params(),
        name="finish",
    )(home, field, z_table, turn, shell, spot, weights)
    lanes = modes // 128
    copies = jnp.broadcast_to(sums.reshape(1, lanes, 128).astype(BF16), (devices, lanes, 128))
    everyone = lax.all_to_all(copies, RING, 0, 0, tiled=True)
    spectrum = pl.pallas_call(
        add_up, out_shape=jax.ShapeDtypeStruct((lanes, 128), F32), compiler_params=params(), name="add_up"
    )(everyone.reshape(-1, 16, 128))
    return updated, spectrum.reshape(modes)


def solution(mesh):
    split = Mesh(mesh.devices.reshape((2,) * 8), ROW + COL)
    placed = (P(None, ROW, COL, None),)
    return jax.shard_map(
        body, mesh=split, in_specs=placed, out_specs=(P(None, ROW, COL, None), P()), check_vma=False
    )
```

```python
import functools
import math

import jax
import jax.numpy as jnp
import numpy as np
from jax import lax
from jax.experimental import pallas as pl
from jax.experimental.pallas import tpu as pltpu
from jax.sharding import Mesh
from jax.sharding import PartitionSpec as P

ROW = ("z_lo1", "z_lo0", "y1", "y0", "core")
COL = ("x1", "x0", "z_hi")
RING = ("z_lo1", "y1", "x1", "z_hi", "z_lo0", "y0", "x0", "core")

phase_rate = 0.0002
coupling = 0.2

F32 = jnp.float32
BF16 = jnp.bfloat16


def trig(waves, points, length):
    turns = np.mod(np.asarray(waves)[:, None] * np.asarray(points)[None, :], length)
    angle = turns.astype(np.float32) * np.float32(2.0 * math.pi / length)
    return np.cos(angle).astype(np.float32), np.sin(angle).astype(np.float32)


def place(width_x, width_y, modes):
    row = functools.reduce(lambda at, axis: 2 * at + lax.axis_index(axis), ROW, 0)
    col = functools.reduce(lambda at, axis: 2 * at + lax.axis_index(axis), COL, 0)
    return row * width_x - modes // 2, col * width_y - modes // 2


def nearest(base, width):
    return jnp.maximum(base, -(base + width - 1))


def shell_of(squared):
    return jnp.floor(jnp.sqrt(squared.astype(F32)) + 0.5)


def phases(angle):
    return jnp.cos(angle), jnp.sin(angle)


def geometry(turn_ref, shell_ref, spot_ref):
    _, width_x, width_y, modes = turn_ref.shape
    base_x, base_y = place(width_x, width_y, modes)

    def square(shape, axis, base):
        wave = base + lax.broadcasted_iota(jnp.int32, shape, axis)
        return wave * wave

    square_x = square((width_x, modes), 0, base_x)
    square_y = square((width_y, modes), 0, base_y)
    square_z = square((8, modes), 1, -(modes // 2))
    cos_x, sin_x = phases(phase_rate * square_x[:, :128].astype(F32))
    cos_y, sin_y = phases(phase_rate * square_y[:, :128].astype(F32))
    cos_z, sin_z = phases(phase_rate * square_z.astype(F32))
    cos_x, sin_x, cos_y, sin_y = (jnp.concatenate([t] * (modes // 128), axis=1) for t in (cos_x, sin_x, cos_y, sin_y))
    column = square((modes, modes), 0, -(modes // 2))
    shells = lax.broadcasted_iota(jnp.int32, (modes, modes), 1).astype(F32)
    near_x = nearest(base_x, width_x)
    for block in range(width_y // 8):
        rows = slice(8 * block, 8 * block + 8)
        near_y = nearest(base_y + 8 * block, 8)
        near = near_x * near_x + near_y * near_y
        lowest = shell_of(near + square_z)
        spot_ref[block] = jnp.where(shell_of(near + column) == shells, 1.0, 0.0).astype(BF16)
        cos_yz = cos_y[rows] * cos_z - sin_y[rows] * sin_z
        sin_yz = sin_y[rows] * cos_z + cos_y[rows] * sin_z
        square_yz = square_y[rows] + square_z
        for at in range(width_x):
            cx, sx = cos_x[at : at + 1], sin_x[at : at + 1]
            turn_ref[0, at, rows] = cos_yz * cx - sin_yz * sx
            turn_ref[1, at, rows] = sin_yz * cx + cos_yz * sx
            shell_ref[at, rows] = shell_of(square_yz + square_x[at : at + 1]) - lowest


def to_slabs(
    field_hbm, table_hbm, ty_hbm, fy_hbm, weight_hbm, out_ref, turn_ref, shell_ref, spot_ref, ty_ref, fy_ref, weight_ref, wide_ref, field, table, sems, *, scale
):
    _, width_x, width, modes = field_hbm.shape
    pairs = (table_hbm, table), (field_hbm, field), (weight_hbm, weight_ref), (ty_hbm, ty_ref), (fy_hbm, fy_ref)
    copies = [pltpu.make_async_copy(source, target, sems.at[k]) for k, (source, target) in enumerate(pairs)]
    for copy in copies:
        copy.start()
    geometry(turn_ref, shell_ref, spot_ref)
    lane = lax.broadcasted_iota(jnp.int32, (width, modes), 1)
    sign = jnp.where(lane % 2 == 0, 1.0, -1.0)
    copies[0].wait()
    copies[1].wait()
    for pair in range(0, width_x, 2):
        rows = []
        for at in (pair, pair + 1):
            real, imag = field[0, at], field[1, at]
            for factor in (None, sign):
                if factor is not None:
                    real, imag = real * factor, imag * factor
                rows.append(jnp.concatenate([real, -imag], axis=1).astype(BF16))
                rows.append(jnp.concatenate([imag, real], axis=1).astype(BF16))
        block = jnp.concatenate(rows, axis=0)
        product = lax.dot_general(
            table[...], block, (((1,), (1,)), ((), ())), preferred_element_type=F32
        ) * scale
        for k in range(2):
            wide_ref[pl.ds(pair + k, modes, stride=width_x), :] = product[:, 128 * k : 128 * (k + 1)]
    out_ref[...] = wide_ref[...].astype(BF16).reshape(out_ref.shape)
    for copy in copies[2:]:
        copy.wait()


def dot(left, right):
    return jnp.dot(left, right, preferred_element_type=F32)


def cube(parts, head):
    pr, pi, qr, qi = parts
    if head:
        first = lax.broadcasted_iota(jnp.int32, pr.shape, 0) == 0
        pick = functools.partial(jnp.where, first)
    else:
        pick = lambda special, general: general
    ar, ai = pick(pr, pr - qi), pick(pi, pi + qr)
    br, bi = pick(qr, pr + qi), pick(qi, pi - qr)
    ma = coupling * (ar * ar + ai * ai)
    mb = coupling * (br * br + bi * bi)
    ar, ai, br, bi = ma * ar, ma * ai, mb * br, mb * bi
    folded = pick(ar, ar + br), pick(ai, ai + bi), pick(br, ai - bi), pick(bi, br - ar)
    return [part.astype(BF16) for part in folded]


def planes(in_ref, ty_ref, fx_ref, fy_ref, out_ref, back_ref, *, chunk):
    modes = fx_ref.shape[0]
    grid = 2 * modes
    half = 64
    fx = fx_ref[...]
    tx = fx.T
    spots = [(x1, x0, z) for x1 in range(2) for x0 in range(2) for z in range(2)]
    blocks = [in_ref[:, x1, z, :, x0].reshape(modes, 128) for x1, x0, z in spots]
    lines = jnp.concatenate(
        [jnp.concatenate([b[:, half * plane : half * (plane + 1)] for b in blocks], axis=1) for plane in range(2)], axis=0
    )
    along_y = dot(lines, ty_ref[...]).astype(BF16)
    for plane in range(2):
        mine = slice(plane * modes, (plane + 1) * modes)
        for start in range(0, grid, chunk):
            real, imag = slice(start, start + chunk), slice(grid + start, grid + start + chunk)
            even_odd = dot(tx, jnp.concatenate([along_y[mine, real], along_y[mine, imag]], axis=1))
            even, odd = even_odd[:modes], even_odd[modes:]
            parts = even[:, :chunk], even[:, chunk:], odd[:, :chunk], odd[:, chunk:]
            top, rest = cube([p[:16] for p in parts], True), cube([p[16:] for p in parts], False)
            even_r, even_i, odd_i, odd_r = (jnp.concatenate(pair, axis=0) for pair in zip(top, rest))
            folded = jnp.concatenate(
                [jnp.concatenate([even_r, even_i], axis=1), jnp.concatenate([odd_i, odd_r], axis=1)], axis=0
            )
            back_x = dot(fx, folded).astype(BF16)
            back_ref[mine, real] = back_x[:, :chunk]
            back_ref[mine, imag] = back_x[:, chunk:]
    done = dot(back_ref[...], fy_ref[...]).astype(BF16)
    for k, (x1, x0, z) in enumerate(spots):
        at = slice(half * k, half * (k + 1))
        message = jnp.concatenate([done[:modes, at], done[modes:, at]], axis=1)
        out_ref[:, x1, z, :, x0] = message.reshape(4, 4, 16, 128)


def finish(
    in_ref, field_ref, table_ref, turn_ref, shell_ref, spot_ref, weight_ref, out_hbm, sums_ref, wide_ref, out_ref, energy_ref, sems, *, scale, bins
):
    _, width_x, width_y, modes = field_ref.shape
    lane = lax.broadcasted_iota(jnp.int32, (width_y, modes), 1)
    sign = jnp.where(lane % 2 == 0, 1.0, -1.0)
    wide_ref[...] = in_ref[...].reshape(wide_ref.shape).astype(F32)
    table = table_ref[...]
    copies = [
        pltpu.make_async_copy(out_ref.at[:, pl.ds(at, 1)], out_hbm.at[:, pl.ds(at, 1)], sems.at[at])
        for at in range(width_x)
    ]
    for at in range(width_x):
        slab = wide_ref[pl.ds(at, modes, stride=width_x), :].astype(BF16)
        got = lax.dot_general(slab, table, (((0,), (0,)), ((), ())), preferred_element_type=F32)
        r0, i0, r1, i1 = (got[width_y * k : width_y * (k + 1)] for k in range(4))
        non_r = (r0[:, :modes] + i0[:, modes:] + sign * (r1[:, :modes] + i1[:, modes:])) * scale
        non_i = (i0[:, :modes] - r0[:, modes:] + sign * (i1[:, :modes] - r1[:, modes:])) * scale
        u = field_ref[0, at] - non_i
        v = field_ref[1, at] + non_r
        cos, sin = turn_ref[0, at], turn_ref[1, at]
        new_r = u * cos + v * sin
        new_i = v * cos - u * sin
        out_ref[0, at] = new_r
        out_ref[1, at] = new_i
        copies[at].start()
        energy_ref[at] = new_r * new_r + new_i * new_i
    result = jnp.zeros((1, modes), F32)
    for block in range(width_y // 8):
        rows = slice(8 * block, 8 * block + 8)
        totals = []
        for k in range(bins):
            total = jnp.zeros((8, modes), F32)
            for at in range(width_x):
                total = total + jnp.where(shell_ref[at, rows] == float(k), energy_ref[at, rows], 0.0)
            totals.append(jnp.sum(total, axis=0, keepdims=True))
        totals.extend([jnp.zeros((1, modes), F32)] * (-bins % 16))
        stacked = jnp.concatenate(totals, axis=0)
        high = stacked.astype(BF16)
        left = stacked - high.astype(F32)
        middle = left.astype(BF16)
        low = (left - middle.astype(F32)).astype(BF16)
        placed = dot(jnp.concatenate([high, middle, low], axis=0), spot_ref[block])
        count = stacked.shape[0]
        placed = placed[:count] + placed[count : 2 * count] + placed[2 * count :]
        shifted = pltpu.roll(placed, 0, 1, stride=1, stride_axis=0)
        result = result + jnp.sum(shifted, axis=0, keepdims=True)
    sums_ref[...] = result * weight_ref[...]
    for copy in copies:
        copy.wait()


def add_up(copies_ref, out_ref):
    total = jnp.sum(copies_ref[...].astype(F32), axis=0)
    lanes = out_ref.shape[0]
    out_ref[...] = jnp.sum(total.reshape(-1, lanes, 128), axis=0)


def tables(modes, scale_in, scale_out):
    grid = 2 * modes
    waves = np.arange(modes) - modes // 2
    cos, sin = trig(waves, np.arange(grid), grid)
    low_cos, low_sin = cos[:, :modes].T, sin[:, :modes].T
    z_table = np.concatenate([low_cos, low_sin], axis=1)
    blocks = modes // 32
    c, s = cos.reshape(blocks, 32, grid), sin.reshape(blocks, 32, grid)
    ty = np.stack([np.concatenate([c, s], 2), np.concatenate([-s, c], 2)], 1).reshape(2 * modes, 2 * grid)
    ct, st = c.transpose(2, 0, 1), s.transpose(2, 0, 1)
    fy = np.stack([np.stack([ct, -st], 2), np.stack([st, ct], 2)], 0).reshape(2 * grid, 2 * modes)
    odd = low_sin.copy()
    odd[0] = cos[:, modes]
    tx = np.concatenate([low_cos, odd], axis=0)
    bits = np.arange(modes).reshape(2, 2, 2, 2, 2, modes // 32)
    fx = tx.T[bits.transpose(0, 2, 1, 3, 4, 5).reshape(-1)]
    scaled = (z_table, ty * scale_in, fx * scale_in, fy * (scale_out * scale_out / scale_in))
    return [jnp.asarray(np.ascontiguousarray(t), BF16) for t in scaled]


def shell_counts(modes):
    wave = np.arange(modes) - modes // 2
    square = wave * wave
    total = square[:, None, None] + square[None, :, None] + square[None, None, :]
    shell = np.floor(np.sqrt(total.astype(np.float32)) + np.float32(0.5)).astype(np.int64)
    return np.bincount(shell.reshape(-1), minlength=modes)[:modes].astype(np.float32)


def in_hbm(array):
    return pltpu.with_memory_space_constraint(array, pltpu.HBM)


def params():
    return pltpu.CompilerParams(vmem_limit_bytes=48 * 1024 * 1024)


def body(field):
    _, width_x, width_y, modes = field.shape
    devices = math.prod(lax.axis_size(axis) for axis in RING)
    scale_in = 1.0 / math.sqrt(modes)
    scale_out = math.sqrt(modes) / (2 * modes)
    z_table, ty, fx, fy = tables(modes, scale_in, scale_out)
    weights = jnp.asarray((1.0 / np.maximum(shell_counts(modes), 1.0)).reshape(1, modes))
    messages, turn, shell, spot, near_ty, near_fy, near_weights = pl.pallas_call(
        functools.partial(to_slabs, scale=scale_in),
        in_specs=[pl.BlockSpec(memory_space=pltpu.HBM)] * 5,
        out_shape=[
            jax.ShapeDtypeStruct((devices, width_x, 128), BF16),
            jax.ShapeDtypeStruct(field.shape, F32),
            jax.ShapeDtypeStruct(field.shape[1:], F32),
            jax.ShapeDtypeStruct((width_y // 8, modes, modes), BF16),
            jax.ShapeDtypeStruct(ty.shape, BF16),
            jax.ShapeDtypeStruct(fy.shape, BF16),
            jax.ShapeDtypeStruct(weights.shape, F32),
        ],
        scratch_shapes=[
            pltpu.VMEM((devices * width_x, 128), F32),
            pltpu.VMEM(field.shape, F32),
            pltpu.VMEM(z_table.shape, BF16),
            pltpu.SemaphoreType.DMA((5,)),
        ],
        compiler_params=params(),
        name="to_slabs",
    )(*(in_hbm(array) for array in (field, z_table, ty, fy, weights)))
    slabs = lax.all_to_all(messages, RING, 0, 0, tiled=True)
    shape = (4, 2, 2, 4, 2, 2 * width_x, 128)
    back = pl.pallas_call(
        functools.partial(planes, chunk=128),
        out_shape=jax.ShapeDtypeStruct(shape, BF16),
        scratch_shapes=[pltpu.VMEM((2 * modes, 4 * modes), BF16)],
        compiler_params=params(),
        name="planes",
    )(slabs.reshape(shape), near_ty, fx, near_fy)
    home = lax.all_to_all(back.reshape(devices, width_x, 128), RING, 0, 0, tiled=True)
    bins = math.ceil(math.sqrt((width_x - 1) ** 2 + 49)) + 2
    updated, sums = pl.pallas_call(
        functools.partial(finish, scale=scale_out, bins=bins),
        out_shape=[jax.ShapeDtypeStruct(field.shape, F32), jax.ShapeDtypeStruct((1, modes), F32)],
        out_specs=[pl.BlockSpec(memory_space=pltpu.HBM), pl.BlockSpec(memory_space=pltpu.VMEM)],
        scratch_shapes=[
            pltpu.VMEM((devices * width_x, 128), F32),
            pltpu.VMEM(field.shape, F32),
            pltpu.VMEM((width_x, width_y, modes), F32),
            pltpu.SemaphoreType.DMA((width_x,)),
        ],
        compiler_params=params(),
        name="finish",
    )(home, field, z_table, turn, shell, spot, near_weights)
    lanes = modes // 128
    copies = jnp.broadcast_to(sums.reshape(1, lanes, 128).astype(BF16), (devices, lanes, 128))
    everyone = lax.all_to_all(copies, RING, 0, 0, tiled=True)
    spectrum = pl.pallas_call(
        add_up, out_shape=jax.ShapeDtypeStruct((lanes, 128), F32), compiler_params=params(), name="add_up"
    )(everyone.reshape(-1, 16, 128))
    return updated, spectrum.reshape(modes)


def solution(mesh):
    split = Mesh(mesh.devices.reshape((2,) * 8), ROW + COL)
    placed = (P(None, ROW, COL, None),)
    return jax.shard_map(
        body, mesh=split, in_specs=placed, out_specs=(P(None, ROW, COL, None), P()), check_vma=False
    )
```

```python
import functools
import math

import jax
import jax.numpy as jnp
import numpy as np
from jax import lax
from jax.experimental import pallas as pl
from jax.experimental.pallas import tpu as pltpu
from jax.sharding import Mesh
from jax.sharding import PartitionSpec as P

ROW = ("z_lo1", "z_lo0", "y1", "y0", "core")
COL = ("x1", "x0", "z_hi")
RING = ("z_lo1", "y1", "x1", "z_hi", "z_lo0", "y0", "x0", "core")

phase_rate = 0.0002
coupling = 0.2

F32 = jnp.float32
BF16 = jnp.bfloat16


def trig(waves, points, length):
    turns = np.mod(np.asarray(waves)[:, None] * np.asarray(points)[None, :], length)
    angle = turns.astype(np.float32) * np.float32(2.0 * math.pi / length)
    return np.cos(angle).astype(np.float32), np.sin(angle).astype(np.float32)


def place(width_x, width_y, modes):
    row = functools.reduce(lambda at, axis: 2 * at + lax.axis_index(axis), ROW, 0)
    col = functools.reduce(lambda at, axis: 2 * at + lax.axis_index(axis), COL, 0)
    return row * width_x - modes // 2, col * width_y - modes // 2


def nearest(base, width):
    return jnp.maximum(base, -(base + width - 1))


def shell_of(squared):
    return jnp.floor(jnp.sqrt(squared.astype(F32)) + 0.5)


def phases(angle):
    return jnp.cos(angle), jnp.sin(angle)


def geometry(turn_ref, shell_ref, spot_ref):
    _, width_x, width_y, modes = turn_ref.shape
    base_x, base_y = place(width_x, width_y, modes)

    def square(shape, axis, base):
        wave = base + lax.broadcasted_iota(jnp.int32, shape, axis)
        return wave * wave

    square_x = square((width_x, modes), 0, base_x)
    square_y = square((width_y, modes), 0, base_y)
    square_z = square((8, modes), 1, -(modes // 2))
    cos_x, sin_x = phases(phase_rate * square_x[:, :128].astype(F32))
    cos_y, sin_y = phases(phase_rate * square_y[:, :128].astype(F32))
    cos_z, sin_z = phases(phase_rate * square_z.astype(F32))
    cos_x, sin_x, cos_y, sin_y = (jnp.concatenate([t] * (modes // 128), axis=1) for t in (cos_x, sin_x, cos_y, sin_y))
    column = square((modes, modes), 0, -(modes // 2))
    shells = lax.broadcasted_iota(jnp.int32, (modes, modes), 1).astype(F32)
    near_x = nearest(base_x, width_x)
    for block in range(width_y // 8):
        rows = slice(8 * block, 8 * block + 8)
        near_y = nearest(base_y + 8 * block, 8)
        near = near_x * near_x + near_y * near_y
        lowest = shell_of(near + square_z)
        spot_ref[block] = jnp.where(shell_of(near + column) == shells, 1.0, 0.0).astype(BF16)
        cos_yz = cos_y[rows] * cos_z - sin_y[rows] * sin_z
        sin_yz = sin_y[rows] * cos_z + cos_y[rows] * sin_z
        square_yz = square_y[rows] + square_z
        for at in range(width_x):
            cx, sx = cos_x[at : at + 1], sin_x[at : at + 1]
            turn_ref[0, at, rows] = cos_yz * cx - sin_yz * sx
            turn_ref[1, at, rows] = sin_yz * cx + cos_yz * sx
            shell_ref[at, rows] = shell_of(square_yz + square_x[at : at + 1]) - lowest


def to_slabs(
    field_hbm, table_hbm, ty_hbm, fy_hbm, weight_hbm, out_ref, turn_ref, shell_ref, spot_ref, ty_ref, fy_ref, weight_ref, wide_ref, field, table, sems, *, scale
):
    _, width_x, width, modes = field_hbm.shape
    pairs = (table_hbm, table), (field_hbm, field), (weight_hbm, weight_ref), (ty_hbm, ty_ref), (fy_hbm, fy_ref)
    copies = [pltpu.make_async_copy(source, target, sems.at[k]) for k, (source, target) in enumerate(pairs)]
    for copy in copies:
        copy.start()
    geometry(turn_ref, shell_ref, spot_ref)
    lane = lax.broadcasted_iota(jnp.int32, (width, modes), 1)
    sign = jnp.where(lane % 2 == 0, 1.0, -1.0)
    copies[0].wait()
    copies[1].wait()
    for pair in range(0, width_x, 2):
        rows = []
        for at in (pair, pair + 1):
            real, imag = field[0, at], field[1, at]
            for factor in (None, sign):
                if factor is not None:
                    real, imag = real * factor, imag * factor
                rows.append(jnp.concatenate([real, -imag], axis=1).astype(BF16))
                rows.append(jnp.concatenate([imag, real], axis=1).astype(BF16))
        block = jnp.concatenate(rows, axis=0)
        product = lax.dot_general(
            table[...], block, (((1,), (1,)), ((), ())), preferred_element_type=F32
        ) * scale
        for k in range(2):
            wide_ref[pl.ds(pair + k, modes, stride=width_x), :] = product[:, 128 * k : 128 * (k + 1)]
    out_ref[...] = wide_ref[...].astype(BF16).reshape(out_ref.shape)
    for copy in copies[2:]:
        copy.wait()


def dot(left, right):
    return jnp.dot(left, right, preferred_element_type=F32)


def cube(parts, head):
    pr, pi, qr, qi = parts
    if head:
        first = lax.broadcasted_iota(jnp.int32, pr.shape, 0) == 0
        pick = functools.partial(jnp.where, first)
    else:
        pick = lambda special, general: general
    ar, ai = pick(pr, pr - qi), pick(pi, pi + qr)
    br, bi = pick(qr, pr + qi), pick(qi, pi - qr)
    ma = coupling * (ar * ar + ai * ai)
    mb = coupling * (br * br + bi * bi)
    ar, ai, br, bi = ma * ar, ma * ai, mb * br, mb * bi
    folded = pick(ar, ar + br), pick(ai, ai + bi), pick(br, ai - bi), pick(bi, br - ar)
    return [part.astype(BF16) for part in folded]


def planes(in_ref, ty_ref, fx_ref, fy_ref, out_ref, back_ref, *, chunk):
    modes = fx_ref.shape[0]
    grid = 2 * modes
    half = 64
    fx = fx_ref[...]
    tx = fx.T
    spots = [(x1, x0, z) for x1 in range(2) for x0 in range(2) for z in range(2)]
    blocks = [in_ref[:, x1, z, :, x0].reshape(modes, 128) for x1, x0, z in spots]
    lines = jnp.concatenate(
        [jnp.concatenate([b[:, half * plane : half * (plane + 1)] for b in blocks], axis=1) for plane in range(2)], axis=0
    )
    along_y = dot(lines, ty_ref[...]).astype(BF16)
    for plane in range(2):
        mine = slice(plane * modes, (plane + 1) * modes)
        for start in range(0, grid, chunk):
            real, imag = slice(start, start + chunk), slice(grid + start, grid + start + chunk)
            even_odd = dot(tx, jnp.concatenate([along_y[mine, real], along_y[mine, imag]], axis=1))
            even, odd = even_odd[:modes], even_odd[modes:]
            parts = even[:, :chunk], even[:, chunk:], odd[:, :chunk], odd[:, chunk:]
            top, rest = cube([p[:16] for p in parts], True), cube([p[16:] for p in parts], False)
            even_r, even_i, odd_i, odd_r = (jnp.concatenate(pair, axis=0) for pair in zip(top, rest))
            folded = jnp.concatenate(
                [jnp.concatenate([even_r, even_i], axis=1), jnp.concatenate([odd_i, odd_r], axis=1)], axis=0
            )
            back_x = dot(fx, folded).astype(BF16)
            back_ref[mine, real] = back_x[:, :chunk]
            back_ref[mine, imag] = back_x[:, chunk:]
    done = dot(back_ref[...], fy_ref[...]).astype(BF16)
    for k, (x1, x0, z) in enumerate(spots):
        at = slice(half * k, half * (k + 1))
        message = jnp.concatenate([done[:modes, at], done[modes:, at]], axis=1)
        out_ref[:, x1, z, :, x0] = message.reshape(4, 4, 16, 128)


def finish(
    in_ref, field_ref, table_ref, turn_ref, shell_ref, spot_ref, weight_ref, out_ref, sums_ref, wide_ref, energy_ref, *, scale, bins
):
    _, width_x, width_y, modes = field_ref.shape
    lane = lax.broadcasted_iota(jnp.int32, (width_y, modes), 1)
    sign = jnp.where(lane % 2 == 0, 1.0, -1.0)
    wide_ref[...] = in_ref[...].reshape(wide_ref.shape).astype(F32)
    table = table_ref[...]
    for at in range(width_x):
        slab = wide_ref[pl.ds(at, modes, stride=width_x), :].astype(BF16)
        got = lax.dot_general(slab, table, (((0,), (0,)), ((), ())), preferred_element_type=F32)
        r0, i0, r1, i1 = (got[width_y * k : width_y * (k + 1)] for k in range(4))
        non_r = (r0[:, :modes] + i0[:, modes:] + sign * (r1[:, :modes] + i1[:, modes:])) * scale
        non_i = (i0[:, :modes] - r0[:, modes:] + sign * (i1[:, :modes] - r1[:, modes:])) * scale
        u = field_ref[0, at] - non_i
        v = field_ref[1, at] + non_r
        cos, sin = turn_ref[0, at], turn_ref[1, at]
        new_r = u * cos + v * sin
        new_i = v * cos - u * sin
        out_ref[0, at] = new_r
        out_ref[1, at] = new_i
        energy_ref[at] = new_r * new_r + new_i * new_i
    result = jnp.zeros((1, modes), F32)
    for block in range(width_y // 8):
        rows = slice(8 * block, 8 * block + 8)
        totals = []
        for k in range(bins):
            total = jnp.zeros((8, modes), F32)
            for at in range(width_x):
                total = total + jnp.where(shell_ref[at, rows] == float(k), energy_ref[at, rows], 0.0)
            totals.append(jnp.sum(total, axis=0, keepdims=True))
        totals.extend([jnp.zeros((1, modes), F32)] * (-bins % 16))
        stacked = jnp.concatenate(totals, axis=0)
        high = stacked.astype(BF16)
        left = stacked - high.astype(F32)
        middle = left.astype(BF16)
        low = (left - middle.astype(F32)).astype(BF16)
        placed = dot(jnp.concatenate([high, middle, low], axis=0), spot_ref[block])
        count = stacked.shape[0]
        placed = placed[:count] + placed[count : 2 * count] + placed[2 * count :]
        shifted = pltpu.roll(placed, 0, 1, stride=1, stride_axis=0)
        result = result + jnp.sum(shifted, axis=0, keepdims=True)
    sums_ref[...] = result * weight_ref[...]


def add_up(copies_ref, out_ref):
    total = jnp.sum(copies_ref[...].astype(F32), axis=0)
    lanes = out_ref.shape[0]
    out_ref[...] = jnp.sum(total.reshape(-1, lanes, 128), axis=0)


def tables(modes, scale_in, scale_out):
    grid = 2 * modes
    waves = np.arange(modes) - modes // 2
    cos, sin = trig(waves, np.arange(grid), grid)
    low_cos, low_sin = cos[:, :modes].T, sin[:, :modes].T
    z_table = np.concatenate([low_cos, low_sin], axis=1)
    blocks = modes // 32
    c, s = cos.reshape(blocks, 32, grid), sin.reshape(blocks, 32, grid)
    ty = np.stack([np.concatenate([c, s], 2), np.concatenate([-s, c], 2)], 1).reshape(2 * modes, 2 * grid)
    ct, st = c.transpose(2, 0, 1), s.transpose(2, 0, 1)
    fy = np.stack([np.stack([ct, -st], 2), np.stack([st, ct], 2)], 0).reshape(2 * grid, 2 * modes)
    odd = low_sin.copy()
    odd[0] = cos[:, modes]
    tx = np.concatenate([low_cos, odd], axis=0)
    bits = np.arange(modes).reshape(2, 2, 2, 2, 2, modes // 32)
    fx = tx.T[bits.transpose(0, 2, 1, 3, 4, 5).reshape(-1)]
    scaled = (z_table, ty * scale_in, fx * scale_in, fy * (scale_out * scale_out / scale_in))
    return [jnp.asarray(np.ascontiguousarray(t), BF16) for t in scaled]


def shell_counts(modes):
    wave = np.arange(modes) - modes // 2
    square = wave * wave
    total = square[:, None, None] + square[None, :, None] + square[None, None, :]
    shell = np.floor(np.sqrt(total.astype(np.float32)) + np.float32(0.5)).astype(np.int64)
    return np.bincount(shell.reshape(-1), minlength=modes)[:modes].astype(np.float32)


def in_hbm(array):
    return pltpu.with_memory_space_constraint(array, pltpu.HBM)


def params():
    return pltpu.CompilerParams(vmem_limit_bytes=48 * 1024 * 1024)


def body(field):
    _, width_x, width_y, modes = field.shape
    devices = math.prod(lax.axis_size(axis) for axis in RING)
    scale_in = 1.0 / math.sqrt(modes)
    scale_out = math.sqrt(modes) / (2 * modes)
    z_table, ty, fx, fy = tables(modes, scale_in, scale_out)
    weights = jnp.asarray((1.0 / np.maximum(shell_counts(modes), 1.0)).reshape(1, modes))
    messages, turn, shell, spot, near_ty, near_fy, near_weights = pl.pallas_call(
        functools.partial(to_slabs, scale=scale_in),
        in_specs=[pl.BlockSpec(memory_space=pltpu.HBM)] * 5,
        out_shape=[
            jax.ShapeDtypeStruct((devices, width_x, 128), BF16),
            jax.ShapeDtypeStruct(field.shape, F32),
            jax.ShapeDtypeStruct(field.shape[1:], F32),
            jax.ShapeDtypeStruct((width_y // 8, modes, modes), BF16),
            jax.ShapeDtypeStruct(ty.shape, BF16),
            jax.ShapeDtypeStruct(fy.shape, BF16),
            jax.ShapeDtypeStruct(weights.shape, F32),
        ],
        scratch_shapes=[
            pltpu.VMEM((devices * width_x, 128), F32),
            pltpu.VMEM(field.shape, F32),
            pltpu.VMEM(z_table.shape, BF16),
            pltpu.SemaphoreType.DMA((5,)),
        ],
        compiler_params=params(),
        name="to_slabs",
    )(*(in_hbm(array) for array in (field, z_table, ty, fy, weights)))
    slabs = lax.all_to_all(messages, RING, 0, 0, tiled=True)
    shape = (4, 2, 2, 4, 2, 2 * width_x, 128)
    back = pl.pallas_call(
        functools.partial(planes, chunk=128),
        out_shape=jax.ShapeDtypeStruct(shape, BF16),
        scratch_shapes=[pltpu.VMEM((2 * modes, 4 * modes), BF16)],
        compiler_params=params(),
        name="planes",
    )(slabs.reshape(shape), near_ty, fx, near_fy)
    home = lax.all_to_all(back.reshape(devices, width_x, 128), RING, 0, 0, tiled=True)
    bins = math.ceil(math.sqrt((width_x - 1) ** 2 + 49)) + 2
    updated, sums = pl.pallas_call(
        functools.partial(finish, scale=scale_out, bins=bins),
        out_shape=[pltpu.VMEM(field.shape, F32), jax.ShapeDtypeStruct((1, modes), F32)],
        scratch_shapes=[pltpu.VMEM((devices * width_x, 128), F32), pltpu.VMEM((width_x, width_y, modes), F32)],
        compiler_params=params(),
        name="finish",
    )(home, field, z_table, turn, shell, spot, near_weights)
    lanes = modes // 128
    copies = jnp.broadcast_to(sums.reshape(1, lanes, 128).astype(BF16), (devices, lanes, 128))
    everyone = lax.all_to_all(copies, RING, 0, 0, tiled=True)
    spectrum = pl.pallas_call(
        add_up, out_shape=jax.ShapeDtypeStruct((lanes, 128), F32), compiler_params=params(), name="add_up"
    )(everyone.reshape(-1, 16, 128))
    return updated, spectrum.reshape(modes)


def solution(mesh):
    split = Mesh(mesh.devices.reshape((2,) * 8), ROW + COL)
    placed = (P(None, ROW, COL, None),)
    return jax.shard_map(
        body, mesh=split, in_specs=placed, out_specs=(P(None, ROW, COL, None), P()), check_vma=False
    )
```

```python
import functools
import math

import jax
import jax.numpy as jnp
import numpy as np
from jax import lax
from jax.experimental import pallas as pl
from jax.experimental.pallas import tpu as pltpu
from jax.sharding import Mesh
from jax.sharding import PartitionSpec as P

ROW = ("z_lo", "y", "core")
COL = ("x", "z_hi")
RING = ("z_hi", "z_lo", "y", "x", "core")

phase_rate = 0.0002
coupling = 0.2

F32 = jnp.float32
BF16 = jnp.bfloat16


def trig(waves, points, length):
    turns = np.mod(np.asarray(waves)[:, None] * np.asarray(points)[None, :], length)
    angle = turns.astype(np.float32) * np.float32(2.0 * math.pi / length)
    return np.cos(angle).astype(np.float32), np.sin(angle).astype(np.float32)


def place(width_x, width_y, modes):
    row = (lax.axis_index("z_lo") * 4 + lax.axis_index("y")) * 2 + lax.axis_index("core")
    col = lax.axis_index("x") * 2 + lax.axis_index("z_hi")
    return row * width_x - modes // 2, col * width_y - modes // 2


def nearest(base, width):
    return jnp.maximum(base, -(base + width - 1))


def shell_of(squared):
    return jnp.floor(jnp.sqrt(squared.astype(F32)) + 0.5)


def phases(angle):
    return jnp.cos(angle), jnp.sin(angle)


def geometry(turn_ref, shell_ref, spot_ref):
    _, width_x, width_y, modes = turn_ref.shape
    base_x, base_y = place(width_x, width_y, modes)

    def square(shape, axis, base):
        wave = base + lax.broadcasted_iota(jnp.int32, shape, axis)
        return wave * wave

    square_x = square((width_x, modes), 0, base_x)
    square_y = square((width_y, modes), 0, base_y)
    square_z = square((8, modes), 1, -(modes // 2))
    cos_x, sin_x = phases(phase_rate * square_x[:, :128].astype(F32))
    cos_y, sin_y = phases(phase_rate * square_y[:, :128].astype(F32))
    cos_z, sin_z = phases(phase_rate * square_z.astype(F32))
    cos_x, sin_x, cos_y, sin_y = (jnp.concatenate([t] * (modes // 128), axis=1) for t in (cos_x, sin_x, cos_y, sin_y))
    column = square((modes, modes), 0, -(modes // 2))
    shells = lax.broadcasted_iota(jnp.int32, (modes, modes), 1).astype(F32)
    near_x = nearest(base_x, width_x)
    for block in range(width_y // 8):
        rows = slice(8 * block, 8 * block + 8)
        near_y = nearest(base_y + 8 * block, 8)
        near = near_x * near_x + near_y * near_y
        lowest = shell_of(near + square_z)
        spot_ref[block] = jnp.where(shell_of(near + column) == shells, 1.0, 0.0).astype(BF16)
        cos_yz = cos_y[rows] * cos_z - sin_y[rows] * sin_z
        sin_yz = sin_y[rows] * cos_z + cos_y[rows] * sin_z
        square_yz = square_y[rows] + square_z
        for at in range(width_x):
            cx, sx = cos_x[at : at + 1], sin_x[at : at + 1]
            turn_ref[0, at, rows] = cos_yz * cx - sin_yz * sx
            turn_ref[1, at, rows] = sin_yz * cx + cos_yz * sx
            shell_ref[at, rows] = shell_of(square_yz + square_x[at : at + 1]) - lowest


def to_slabs(
    field_hbm, table_hbm, ty_hbm, fy_hbm, weight_hbm, out_ref, turn_ref, shell_ref, spot_ref, ty_ref, fy_ref, weight_ref, field, table, wide_ref, sems, *, scale
):
    _, width_x, width, modes = field_hbm.shape
    pairs = (table_hbm, table), (field_hbm, field), (weight_hbm, weight_ref), (ty_hbm, ty_ref), (fy_hbm, fy_ref)
    copies = [pltpu.make_async_copy(source, target, sems.at[k]) for k, (source, target) in enumerate(pairs)]
    for copy in copies:
        copy.start()
    geometry(turn_ref, shell_ref, spot_ref)
    lane = lax.broadcasted_iota(jnp.int32, (width, modes), 1)
    sign = jnp.where(lane % 2 == 0, 1.0, -1.0)
    copies[0].wait()
    copies[1].wait()
    for pair in range(0, width_x, 2):
        rows = []
        for at in (pair, pair + 1):
            real, imag = field[0, at], field[1, at]
            for factor in (None, sign):
                if factor is not None:
                    real, imag = real * factor, imag * factor
                rows.append(jnp.concatenate([real, -imag], axis=1).astype(BF16))
                rows.append(jnp.concatenate([imag, real], axis=1).astype(BF16))
        block = jnp.concatenate(rows, axis=0)
        product = lax.dot_general(
            table[...], block, (((1,), (1,)), ((), ())), preferred_element_type=F32
        ) * scale
        for k in range(2):
            wide_ref[pl.ds(pair + k, modes, stride=width_x), :] = product[:, 128 * k : 128 * (k + 1)]
    out_ref[...] = wide_ref[...].astype(BF16).reshape(out_ref.shape)
    for copy in copies[2:]:
        copy.wait()


def dot(left, right):
    return jnp.dot(left, right, preferred_element_type=F32)


def cube(parts, head):
    pr, pi, qr, qi = parts
    if head:
        first = lax.broadcasted_iota(jnp.int32, pr.shape, 0) == 0
        pick = functools.partial(jnp.where, first)
    else:
        pick = lambda special, general: general
    ar, ai = pick(pr, pr - qi), pick(pi, pi + qr)
    br, bi = pick(qr, pr + qi), pick(qi, pi - qr)
    ma = coupling * (ar * ar + ai * ai)
    mb = coupling * (br * br + bi * bi)
    ar, ai, br, bi = ma * ar, ma * ai, mb * br, mb * bi
    folded = pick(ar, ar + br), pick(ai, ai + bi), pick(br, ai - bi), pick(bi, br - ar)
    return [part.astype(BF16) for part in folded]


def planes(in_ref, ty_ref, fx_ref, fy_ref, out_ref, back_ref, *, chunk):
    modes = fx_ref.shape[0]
    grid = 2 * modes
    half = 64
    fx = fx_ref[...]
    tx = fx.T
    spots = [(x, z) for x in range(4) for z in range(2)]
    blocks = [in_ref[z, :, x].reshape(modes, 128) for x, z in spots]
    lines = jnp.concatenate(
        [jnp.concatenate([b[:, half * plane : half * (plane + 1)] for b in blocks], axis=1) for plane in range(2)], axis=0
    )
    along_y = dot(lines, ty_ref[...]).astype(BF16)
    for plane in range(2):
        mine = slice(plane * modes, (plane + 1) * modes)
        for start in range(0, grid, chunk):
            real, imag = slice(start, start + chunk), slice(grid + start, grid + start + chunk)
            even_odd = dot(tx, jnp.concatenate([along_y[mine, real], along_y[mine, imag]], axis=1))
            even, odd = even_odd[:modes], even_odd[modes:]
            parts = even[:, :chunk], even[:, chunk:], odd[:, :chunk], odd[:, chunk:]
            top, rest = cube([p[:16] for p in parts], True), cube([p[16:] for p in parts], False)
            even_r, even_i, odd_i, odd_r = (jnp.concatenate(pair, axis=0) for pair in zip(top, rest))
            folded = jnp.concatenate(
                [jnp.concatenate([even_r, even_i], axis=1), jnp.concatenate([odd_i, odd_r], axis=1)], axis=0
            )
            back_x = dot(fx, folded).astype(BF16)
            back_ref[mine, real] = back_x[:, :chunk]
            back_ref[mine, imag] = back_x[:, chunk:]
    done = dot(back_ref[...], fy_ref[...]).astype(BF16)
    for k, (x, z) in enumerate(spots):
        at = slice(half * k, half * (k + 1))
        message = jnp.concatenate([done[:modes, at], done[modes:, at]], axis=1)
        out_ref[z, :, x] = message.reshape(16, 16, 128)


def finish(
    in_ref, field_ref, table_ref, turn_ref, shell_ref, spot_ref, weight_ref, out_hbm, sums_ref, wide_ref, out_ref, energy_ref, sems, *, scale, bins
):
    _, width_x, width_y, modes = field_ref.shape
    lane = lax.broadcasted_iota(jnp.int32, (width_y, modes), 1)
    sign = jnp.where(lane % 2 == 0, 1.0, -1.0)
    wide_ref[...] = in_ref[...].reshape(wide_ref.shape).astype(F32)
    table = table_ref[...]
    copies = [
        pltpu.make_async_copy(out_ref.at[:, pl.ds(at, 1)], out_hbm.at[:, pl.ds(at, 1)], sems.at[at])
        for at in range(width_x)
    ]
    for at in range(width_x):
        slab = wide_ref[pl.ds(at, modes, stride=width_x), :].astype(BF16)
        got = lax.dot_general(slab, table, (((0,), (0,)), ((), ())), preferred_element_type=F32)
        r0, i0, r1, i1 = (got[width_y * k : width_y * (k + 1)] for k in range(4))
        non_r = (r0[:, :modes] + i0[:, modes:] + sign * (r1[:, :modes] + i1[:, modes:])) * scale
        non_i = (i0[:, :modes] - r0[:, modes:] + sign * (i1[:, :modes] - r1[:, modes:])) * scale
        u = field_ref[0, at] - non_i
        v = field_ref[1, at] + non_r
        cos, sin = turn_ref[0, at], turn_ref[1, at]
        new_r = u * cos + v * sin
        new_i = v * cos - u * sin
        out_ref[0, at] = new_r
        out_ref[1, at] = new_i
        copies[at].start()
        energy_ref[at] = new_r * new_r + new_i * new_i
    result = jnp.zeros((1, modes), F32)
    for block in range(width_y // 8):
        rows = slice(8 * block, 8 * block + 8)
        totals = []
        for k in range(bins):
            total = jnp.zeros((8, modes), F32)
            for at in range(width_x):
                total = total + jnp.where(shell_ref[at, rows] == float(k), energy_ref[at, rows], 0.0)
            totals.append(jnp.sum(total, axis=0, keepdims=True))
        totals.extend([jnp.zeros((1, modes), F32)] * (-bins % 16))
        stacked = jnp.concatenate(totals, axis=0)
        high = stacked.astype(BF16)
        left = stacked - high.astype(F32)
        middle = left.astype(BF16)
        low = (left - middle.astype(F32)).astype(BF16)
        placed = dot(jnp.concatenate([high, middle, low], axis=0), spot_ref[block])
        count = stacked.shape[0]
        placed = placed[:count] + placed[count : 2 * count] + placed[2 * count :]
        shifted = pltpu.roll(placed, 0, 1, stride=1, stride_axis=0)
        result = result + jnp.sum(shifted, axis=0, keepdims=True)
    sums_ref[...] = result * weight_ref[...]
    for copy in copies:
        copy.wait()


def add_up(copies_ref, out_ref):
    total = jnp.sum(copies_ref[...].astype(F32), axis=0)
    lanes = out_ref.shape[0]
    out_ref[...] = jnp.sum(total.reshape(-1, lanes, 128), axis=0)


def tables(modes, scale_in, scale_out):
    grid = 2 * modes
    waves = np.arange(modes) - modes // 2
    cos, sin = trig(waves, np.arange(grid), grid)
    low_cos, low_sin = cos[:, :modes].T, sin[:, :modes].T
    z_table = np.concatenate([low_cos, low_sin], axis=1)
    blocks = modes // 32
    c, s = cos.reshape(blocks, 32, grid), sin.reshape(blocks, 32, grid)
    ty = np.stack([np.concatenate([c, s], 2), np.concatenate([-s, c], 2)], 1).reshape(2 * modes, 2 * grid)
    ct, st = c.transpose(2, 0, 1), s.transpose(2, 0, 1)
    fy = np.stack([np.stack([ct, -st], 2), np.stack([st, ct], 2)], 0).reshape(2 * grid, 2 * modes)
    odd = low_sin.copy()
    odd[0] = cos[:, modes]
    tx = np.concatenate([low_cos, odd], axis=0)
    fx = tx.T
    scaled = (z_table, ty * scale_in, fx * scale_in, fy * (scale_out * scale_out / scale_in))
    return [jnp.asarray(np.ascontiguousarray(t), BF16) for t in scaled]


def shell_counts(modes):
    wave = np.arange(modes) - modes // 2
    square = wave * wave
    total = square[:, None, None] + square[None, :, None] + square[None, None, :]
    shell = np.floor(np.sqrt(total.astype(np.float32)) + np.float32(0.5)).astype(np.int64)
    return np.bincount(shell.reshape(-1), minlength=modes)[:modes].astype(np.float32)


def in_hbm(array):
    return pltpu.with_memory_space_constraint(array, pltpu.HBM)


def params():
    return pltpu.CompilerParams(vmem_limit_bytes=48 * 1024 * 1024)


def body(field):
    _, width_x, width_y, modes = field.shape
    devices = math.prod(lax.axis_size(axis) for axis in RING)
    scale_in = 1.0 / math.sqrt(modes)
    scale_out = math.sqrt(modes) / (2 * modes)
    z_table, ty, fx, fy = tables(modes, scale_in, scale_out)
    weights = jnp.asarray((1.0 / np.maximum(shell_counts(modes), 1.0)).reshape(1, modes))
    messages, turn, shell, spot, near_ty, near_fy, near_weights, near_field, near_table = pl.pallas_call(
        functools.partial(to_slabs, scale=scale_in),
        in_specs=[pl.BlockSpec(memory_space=pltpu.HBM)] * 5,
        out_shape=[
            jax.ShapeDtypeStruct((devices, width_x, 128), BF16),
            jax.ShapeDtypeStruct(field.shape, F32),
            jax.ShapeDtypeStruct(field.shape[1:], F32),
            jax.ShapeDtypeStruct((width_y // 8, modes, modes), BF16),
            jax.ShapeDtypeStruct(ty.shape, BF16),
            jax.ShapeDtypeStruct(fy.shape, BF16),
            jax.ShapeDtypeStruct(weights.shape, F32),
            jax.ShapeDtypeStruct(field.shape, F32),
            jax.ShapeDtypeStruct(z_table.shape, BF16),
        ],
        scratch_shapes=[
            pltpu.VMEM((devices * width_x, 128), F32),
            pltpu.SemaphoreType.DMA((5,)),
        ],
        compiler_params=params(),
        name="to_slabs",
    )(*(in_hbm(array) for array in (field, z_table, ty, fy, weights)))
    slabs = lax.all_to_all(messages, RING, 0, 0, tiled=True)
    shape = (2, 16, 4, 2 * width_x, 128)
    back = pl.pallas_call(
        functools.partial(planes, chunk=128),
        out_shape=jax.ShapeDtypeStruct(shape, BF16),
        scratch_shapes=[pltpu.VMEM((2 * modes, 4 * modes), BF16)],
        compiler_params=params(),
        name="planes",
    )(slabs.reshape(shape), near_ty, fx, near_fy)
    home = lax.all_to_all(back.reshape(devices, width_x, 128), RING, 0, 0, tiled=True)
    bins = math.ceil(math.sqrt((width_x - 1) ** 2 + 49)) + 2
    updated, sums = pl.pallas_call(
        functools.partial(finish, scale=scale_out, bins=bins),
        out_shape=[jax.ShapeDtypeStruct(field.shape, F32), jax.ShapeDtypeStruct((1, modes), F32)],
        out_specs=[pl.BlockSpec(memory_space=pltpu.HBM), pl.BlockSpec(memory_space=pltpu.VMEM)],
        scratch_shapes=[
            pltpu.VMEM((devices * width_x, 128), F32),
            pltpu.VMEM(field.shape, F32),
            pltpu.VMEM((width_x, width_y, modes), F32),
            pltpu.SemaphoreType.DMA((width_x,)),
        ],
        compiler_params=params(),
        name="finish",
    )(home, near_field, near_table, turn, shell, spot, near_weights)
    lanes = modes // 128
    copies = jnp.broadcast_to(sums.reshape(1, lanes, 128).astype(BF16), (devices, lanes, 128))
    everyone = lax.all_to_all(copies, RING, 0, 0, tiled=True)
    spectrum = pl.pallas_call(
        add_up, out_shape=jax.ShapeDtypeStruct((lanes, 128), F32), compiler_params=params(), name="add_up"
    )(everyone.reshape(-1, 16, 128))
    return updated, spectrum.reshape(modes)


def solution(mesh):
    split = Mesh(mesh.devices.reshape(4, 4, 2, 4, 2), ROW + COL)
    placed = (P(None, ROW, COL, None),)
    return jax.shard_map(
        body, mesh=split, in_specs=placed, out_specs=(P(None, ROW, COL, None), P()), check_vma=False
    )
```

```python
import functools
import math

import jax
import jax.numpy as jnp
import numpy as np
from jax import lax
from jax.experimental import pallas as pl
from jax.experimental.pallas import tpu as pltpu
from jax.sharding import Mesh
from jax.sharding import PartitionSpec as P

ROW = ("z_lo", "y", "core")
COL = ("x", "z_hi")
RING = ("core", "z_hi", "z_lo", "y", "x")

phase_rate = 0.0002
coupling = 0.2

F32 = jnp.float32
BF16 = jnp.bfloat16


def trig(waves, points, length):
    turns = np.mod(np.asarray(waves)[:, None] * np.asarray(points)[None, :], length)
    angle = turns.astype(np.float32) * np.float32(2.0 * math.pi / length)
    return np.cos(angle).astype(np.float32), np.sin(angle).astype(np.float32)


def place(width_x, width_y, modes):
    row = (lax.axis_index("z_lo") * 4 + lax.axis_index("y")) * 2 + lax.axis_index("core")
    col = lax.axis_index("x") * 2 + lax.axis_index("z_hi")
    return row * width_x - modes // 2, col * width_y - modes // 2


def nearest(base, width):
    return jnp.maximum(base, -(base + width - 1))


def shell_of(squared):
    return jnp.floor(jnp.sqrt(squared.astype(F32)) + 0.5)


def phases(angle):
    return jnp.cos(angle), jnp.sin(angle)


def geometry(turn_ref, shell_ref, spot_ref):
    _, width_x, width_y, modes = turn_ref.shape
    base_x, base_y = place(width_x, width_y, modes)

    def square(shape, axis, base):
        wave = base + lax.broadcasted_iota(jnp.int32, shape, axis)
        return wave * wave

    square_x = square((width_x, modes), 0, base_x)
    square_y = square((width_y, modes), 0, base_y)
    square_z = square((8, modes), 1, -(modes // 2))
    cos_x, sin_x = phases(phase_rate * square_x[:, :128].astype(F32))
    cos_y, sin_y = phases(phase_rate * square_y[:, :128].astype(F32))
    cos_z, sin_z = phases(phase_rate * square_z.astype(F32))
    cos_x, sin_x, cos_y, sin_y = (jnp.concatenate([t] * (modes // 128), axis=1) for t in (cos_x, sin_x, cos_y, sin_y))
    column = square((modes, modes), 0, -(modes // 2))
    shells = lax.broadcasted_iota(jnp.int32, (modes, modes), 1).astype(F32)
    near_x = nearest(base_x, width_x)
    for block in range(width_y // 8):
        rows = slice(8 * block, 8 * block + 8)
        near_y = nearest(base_y + 8 * block, 8)
        near = near_x * near_x + near_y * near_y
        lowest = shell_of(near + square_z)
        spot_ref[block] = jnp.where(shell_of(near + column) == shells, 1.0, 0.0).astype(BF16)
        cos_yz = cos_y[rows] * cos_z - sin_y[rows] * sin_z
        sin_yz = sin_y[rows] * cos_z + cos_y[rows] * sin_z
        square_yz = square_y[rows] + square_z
        for at in range(width_x):
            cx, sx = cos_x[at : at + 1], sin_x[at : at + 1]
            turn_ref[0, at, rows] = cos_yz * cx - sin_yz * sx
            turn_ref[1, at, rows] = sin_yz * cx + cos_yz * sx
            shell_ref[at, rows] = shell_of(square_yz + square_x[at : at + 1]) - lowest


def to_slabs(
    field_hbm, table_hbm, ty_hbm, fy_hbm, weight_hbm, out_ref, turn_ref, shell_ref, spot_ref, ty_ref, fy_ref, weight_ref, field, table, wide_ref, sems, *, scale
):
    _, width_x, width, modes = field_hbm.shape
    pairs = (table_hbm, table), (field_hbm, field), (weight_hbm, weight_ref), (ty_hbm, ty_ref), (fy_hbm, fy_ref)
    copies = [pltpu.make_async_copy(source, target, sems.at[k]) for k, (source, target) in enumerate(pairs)]
    for copy in copies:
        copy.start()
    geometry(turn_ref, shell_ref, spot_ref)
    lane = lax.broadcasted_iota(jnp.int32, (width, modes), 1)
    sign = jnp.where(lane % 2 == 0, 1.0, -1.0)
    copies[0].wait()
    copies[1].wait()
    for pair in range(0, width_x, 2):
        rows = []
        for at in (pair, pair + 1):
            real, imag = field[0, at], field[1, at]
            for factor in (None, sign):
                if factor is not None:
                    real, imag = real * factor, imag * factor
                rows.append(jnp.concatenate([real, -imag], axis=1).astype(BF16))
                rows.append(jnp.concatenate([imag, real], axis=1).astype(BF16))
        block = jnp.concatenate(rows, axis=0)
        product = lax.dot_general(
            table[...], block, (((1,), (1,)), ((), ())), preferred_element_type=F32
        ) * scale
        for k in range(2):
            wide_ref[pl.ds(pair + k, modes, stride=width_x), :] = product[:, 128 * k : 128 * (k + 1)]
    out_ref[...] = wide_ref[...].astype(BF16).reshape(out_ref.shape)
    for copy in copies[2:]:
        copy.wait()


def dot(left, right):
    return jnp.dot(left, right, preferred_element_type=F32)


def cube(parts, head):
    pr, pi, qr, qi = parts
    if head:
        first = lax.broadcasted_iota(jnp.int32, pr.shape, 0) == 0
        pick = functools.partial(jnp.where, first)
    else:
        pick = lambda special, general: general
    ar, ai = pick(pr, pr - qi), pick(pi, pi + qr)
    br, bi = pick(qr, pr + qi), pick(qi, pi - qr)
    ma = coupling * (ar * ar + ai * ai)
    mb = coupling * (br * br + bi * bi)
    ar, ai, br, bi = ma * ar, ma * ai, mb * br, mb * bi
    folded = pick(ar, ar + br), pick(ai, ai + bi), pick(br, ai - bi), pick(bi, br - ar)
    return [part.astype(BF16) for part in folded]


def planes(in_ref, ty_ref, fx_ref, fy_ref, out_ref, back_ref, *, chunk):
    modes = fx_ref.shape[0]
    grid = 2 * modes
    half = 64
    fx = fx_ref[...]
    tx = fx.T
    spots = [(x, z) for x in range(4) for z in range(2)]
    blocks = [in_ref[:, z, :, x].reshape(modes, 128) for x, z in spots]
    lines = jnp.concatenate(
        [jnp.concatenate([b[:, half * plane : half * (plane + 1)] for b in blocks], axis=1) for plane in range(2)], axis=0
    )
    along_y = dot(lines, ty_ref[...]).astype(BF16)
    for plane in range(2):
        mine = slice(plane * modes, (plane + 1) * modes)
        for start in range(0, grid, chunk):
            real, imag = slice(start, start + chunk), slice(grid + start, grid + start + chunk)
            even_odd = dot(tx, jnp.concatenate([along_y[mine, real], along_y[mine, imag]], axis=1))
            even, odd = even_odd[:modes], even_odd[modes:]
            parts = even[:, :chunk], even[:, chunk:], odd[:, :chunk], odd[:, chunk:]
            top, rest = cube([p[:16] for p in parts], True), cube([p[16:] for p in parts], False)
            even_r, even_i, odd_i, odd_r = (jnp.concatenate(pair, axis=0) for pair in zip(top, rest))
            folded = jnp.concatenate(
                [jnp.concatenate([even_r, even_i], axis=1), jnp.concatenate([odd_i, odd_r], axis=1)], axis=0
            )
            back_x = dot(fx, folded).astype(BF16)
            back_ref[mine, real] = back_x[:, :chunk]
            back_ref[mine, imag] = back_x[:, chunk:]
    done = dot(back_ref[...], fy_ref[...]).astype(BF16)
    for k, (x, z) in enumerate(spots):
        at = slice(half * k, half * (k + 1))
        message = jnp.concatenate([done[:modes, at], done[modes:, at]], axis=1)
        out_ref[:, z, :, x] = message.reshape(2, 16, -1, 128)


def finish(
    in_ref, field_ref, table_ref, turn_ref, shell_ref, spot_ref, weight_ref, out_hbm, sums_ref, wide_ref, out_ref, energy_ref, sems, *, scale, bins
):
    _, width_x, width_y, modes = field_ref.shape
    lane = lax.broadcasted_iota(jnp.int32, (width_y, modes), 1)
    sign = jnp.where(lane % 2 == 0, 1.0, -1.0)
    wide_ref[...] = in_ref[...].reshape(wide_ref.shape).astype(F32)
    table = table_ref[...]
    copies = [
        pltpu.make_async_copy(out_ref.at[:, pl.ds(at, 1)], out_hbm.at[:, pl.ds(at, 1)], sems.at[at])
        for at in range(width_x)
    ]
    for at in range(width_x):
        slab = wide_ref[pl.ds(at, modes, stride=width_x), :].astype(BF16)
        got = lax.dot_general(slab, table, (((0,), (0,)), ((), ())), preferred_element_type=F32)
        r0, i0, r1, i1 = (got[width_y * k : width_y * (k + 1)] for k in range(4))
        non_r = (r0[:, :modes] + i0[:, modes:] + sign * (r1[:, :modes] + i1[:, modes:])) * scale
        non_i = (i0[:, :modes] - r0[:, modes:] + sign * (i1[:, :modes] - r1[:, modes:])) * scale
        u = field_ref[0, at] - non_i
        v = field_ref[1, at] + non_r
        cos, sin = turn_ref[0, at], turn_ref[1, at]
        new_r = u * cos + v * sin
        new_i = v * cos - u * sin
        out_ref[0, at] = new_r
        out_ref[1, at] = new_i
        copies[at].start()
        energy_ref[at] = new_r * new_r + new_i * new_i
    result = jnp.zeros((1, modes), F32)
    for block in range(width_y // 8):
        rows = slice(8 * block, 8 * block + 8)
        totals = []
        for k in range(bins):
            total = jnp.zeros((8, modes), F32)
            for at in range(width_x):
                total = total + jnp.where(shell_ref[at, rows] == float(k), energy_ref[at, rows], 0.0)
            totals.append(jnp.sum(total, axis=0, keepdims=True))
        totals.extend([jnp.zeros((1, modes), F32)] * (-bins % 16))
        stacked = jnp.concatenate(totals, axis=0)
        high = stacked.astype(BF16)
        left = stacked - high.astype(F32)
        middle = left.astype(BF16)
        low = (left - middle.astype(F32)).astype(BF16)
        placed = dot(jnp.concatenate([high, middle, low], axis=0), spot_ref[block])
        count = stacked.shape[0]
        placed = placed[:count] + placed[count : 2 * count] + placed[2 * count :]
        shifted = pltpu.roll(placed, 0, 1, stride=1, stride_axis=0)
        result = result + jnp.sum(shifted, axis=0, keepdims=True)
    sums_ref[...] = result * weight_ref[...]
    for copy in copies:
        copy.wait()


def add_up(copies_ref, out_ref):
    total = jnp.sum(copies_ref[...].astype(F32), axis=0)
    lanes = out_ref.shape[0]
    out_ref[...] = jnp.sum(total.reshape(-1, lanes, 128), axis=0)


def tables(modes, scale_in, scale_out):
    grid = 2 * modes
    waves = np.arange(modes) - modes // 2
    cos, sin = trig(waves, np.arange(grid), grid)
    low_cos, low_sin = cos[:, :modes].T, sin[:, :modes].T
    z_table = np.concatenate([low_cos, low_sin], axis=1)
    blocks = modes // 32
    c, s = cos.reshape(blocks, 32, grid), sin.reshape(blocks, 32, grid)
    ty = np.stack([np.concatenate([c, s], 2), np.concatenate([-s, c], 2)], 1).reshape(2 * modes, 2 * grid)
    ct, st = c.transpose(2, 0, 1), s.transpose(2, 0, 1)
    fy = np.stack([np.stack([ct, -st], 2), np.stack([st, ct], 2)], 0).reshape(2 * grid, 2 * modes)
    odd = low_sin.copy()
    odd[0] = cos[:, modes]
    tx = np.concatenate([low_cos, odd], axis=0)
    fx = tx.T[np.arange(modes).reshape(16, 2, -1).transpose(1, 0, 2).reshape(-1)]
    scaled = (z_table, ty * scale_in, fx * scale_in, fy * (scale_out * scale_out / scale_in))
    return [jnp.asarray(np.ascontiguousarray(t), BF16) for t in scaled]


def shell_counts(modes):
    wave = np.arange(modes) - modes // 2
    square = wave * wave
    total = square[:, None, None] + square[None, :, None] + square[None, None, :]
    shell = np.floor(np.sqrt(total.astype(np.float32)) + np.float32(0.5)).astype(np.int64)
    return np.bincount(shell.reshape(-1), minlength=modes)[:modes].astype(np.float32)


def in_hbm(array):
    return pltpu.with_memory_space_constraint(array, pltpu.HBM)


def params():
    return pltpu.CompilerParams(vmem_limit_bytes=48 * 1024 * 1024)


def body(field):
    _, width_x, width_y, modes = field.shape
    devices = math.prod(lax.axis_size(axis) for axis in RING)
    scale_in = 1.0 / math.sqrt(modes)
    scale_out = math.sqrt(modes) / (2 * modes)
    z_table, ty, fx, fy = tables(modes, scale_in, scale_out)
    weights = jnp.asarray((1.0 / np.maximum(shell_counts(modes), 1.0)).reshape(1, modes))
    messages, turn, shell, spot, near_ty, near_fy, near_weights, near_field, near_table = pl.pallas_call(
        functools.partial(to_slabs, scale=scale_in),
        in_specs=[pl.BlockSpec(memory_space=pltpu.HBM)] * 5,
        out_shape=[
            jax.ShapeDtypeStruct((devices, width_x, 128), BF16),
            jax.ShapeDtypeStruct(field.shape, F32),
            jax.ShapeDtypeStruct(field.shape[1:], F32),
            jax.ShapeDtypeStruct((width_y // 8, modes, modes), BF16),
            jax.ShapeDtypeStruct(ty.shape, BF16),
            jax.ShapeDtypeStruct(fy.shape, BF16),
            jax.ShapeDtypeStruct(weights.shape, F32),
            jax.ShapeDtypeStruct(field.shape, F32),
            jax.ShapeDtypeStruct(z_table.shape, BF16),
        ],
        scratch_shapes=[
            pltpu.VMEM((devices * width_x, 128), F32),
            pltpu.SemaphoreType.DMA((5,)),
        ],
        compiler_params=params(),
        name="to_slabs",
    )(*(in_hbm(array) for array in (field, z_table, ty, fy, weights)))
    slabs = lax.all_to_all(messages, RING, 0, 0, tiled=True)
    shape = (2, 2, 16, 4, width_x, 128)
    back = pl.pallas_call(
        functools.partial(planes, chunk=128),
        out_shape=jax.ShapeDtypeStruct(shape, BF16),
        scratch_shapes=[pltpu.VMEM((2 * modes, 4 * modes), BF16)],
        compiler_params=params(),
        name="planes",
    )(slabs.reshape(shape), near_ty, fx, near_fy)
    home = lax.all_to_all(back.reshape(devices, width_x, 128), RING, 0, 0, tiled=True)
    bins = math.ceil(math.sqrt((width_x - 1) ** 2 + 49)) + 2
    updated, sums = pl.pallas_call(
        functools.partial(finish, scale=scale_out, bins=bins),
        out_shape=[jax.ShapeDtypeStruct(field.shape, F32), jax.ShapeDtypeStruct((1, modes), F32)],
        out_specs=[pl.BlockSpec(memory_space=pltpu.HBM), pl.BlockSpec(memory_space=pltpu.VMEM)],
        scratch_shapes=[
            pltpu.VMEM((devices * width_x, 128), F32),
            pltpu.VMEM(field.shape, F32),
            pltpu.VMEM((width_x, width_y, modes), F32),
            pltpu.SemaphoreType.DMA((width_x,)),
        ],
        compiler_params=params(),
        name="finish",
    )(home, near_field, near_table, turn, shell, spot, near_weights)
    lanes = modes // 128
    copies = jnp.broadcast_to(sums.reshape(1, lanes, 128).astype(BF16), (devices, lanes, 128))
    everyone = lax.all_to_all(copies, RING, 0, 0, tiled=True)
    spectrum = pl.pallas_call(
        add_up, out_shape=jax.ShapeDtypeStruct((lanes, 128), F32), compiler_params=params(), name="add_up"
    )(everyone.reshape(-1, 16, 128))
    return updated, spectrum.reshape(modes)


def solution(mesh):
    split = Mesh(mesh.devices.reshape(4, 4, 2, 4, 2), ROW + COL)
    placed = (P(None, ROW, COL, None),)
    return jax.shard_map(
        body, mesh=split, in_specs=placed, out_specs=(P(None, ROW, COL, None), P()), check_vma=False
    )
```

```python
import functools
import math

import jax
import jax.numpy as jnp
import numpy as np
from jax import lax
from jax.experimental import pallas as pl
from jax.experimental.pallas import tpu as pltpu
from jax.sharding import Mesh
from jax.sharding import PartitionSpec as P

ROW = ("z_lo", "y", "core")
COL = ("x", "z_hi")
RING = ("z_hi", "z_lo", "y", "x", "core")

phase_rate = 0.0002
coupling = 0.2

F32 = jnp.float32
BF16 = jnp.bfloat16


def trig(waves, points, length):
    turns = np.mod(np.asarray(waves)[:, None] * np.asarray(points)[None, :], length)
    angle = turns.astype(np.float32) * np.float32(2.0 * math.pi / length)
    return np.cos(angle).astype(np.float32), np.sin(angle).astype(np.float32)


def place(width_x, width_y, modes):
    row = (lax.axis_index("z_lo") * 4 + lax.axis_index("y")) * 2 + lax.axis_index("core")
    col = lax.axis_index("x") * 2 + lax.axis_index("z_hi")
    return row * width_x - modes // 2, col * width_y - modes // 2


def nearest(base, width):
    return jnp.maximum(base, -(base + width - 1))


def shell_of(squared):
    return jnp.floor(jnp.sqrt(squared.astype(F32)) + 0.5)


def phases(angle):
    return jnp.cos(angle), jnp.sin(angle)


def geometry(turn_ref, shell_ref, spot_ref):
    _, width_x, width_y, modes = turn_ref.shape
    base_x, base_y = place(width_x, width_y, modes)

    def square(shape, axis, base):
        wave = base + lax.broadcasted_iota(jnp.int32, shape, axis)
        return wave * wave

    square_x = square((width_x, modes), 0, base_x)
    square_y = square((width_y, modes), 0, base_y)
    square_z = square((8, modes), 1, -(modes // 2))
    cos_x, sin_x = phases(phase_rate * square_x[:, :128].astype(F32))
    cos_y, sin_y = phases(phase_rate * square_y[:, :128].astype(F32))
    cos_z, sin_z = phases(phase_rate * square_z.astype(F32))
    cos_x, sin_x, cos_y, sin_y = (jnp.concatenate([t] * (modes // 128), axis=1) for t in (cos_x, sin_x, cos_y, sin_y))
    column = square((modes, modes), 0, -(modes // 2))
    shells = lax.broadcasted_iota(jnp.int32, (modes, modes), 1).astype(F32)
    near_x = nearest(base_x, width_x)
    for block in range(width_y // 8):
        rows = slice(8 * block, 8 * block + 8)
        near_y = nearest(base_y + 8 * block, 8)
        near = near_x * near_x + near_y * near_y
        lowest = shell_of(near + square_z)
        spot_ref[block] = jnp.where(shell_of(near + column) == shells, 1.0, 0.0).astype(BF16)
        cos_yz = cos_y[rows] * cos_z - sin_y[rows] * sin_z
        sin_yz = sin_y[rows] * cos_z + cos_y[rows] * sin_z
        square_yz = square_y[rows] + square_z
        for at in range(width_x):
            cx, sx = cos_x[at : at + 1], sin_x[at : at + 1]
            turn_ref[0, at, rows] = cos_yz * cx - sin_yz * sx
            turn_ref[1, at, rows] = sin_yz * cx + cos_yz * sx
            shell_ref[at, rows] = shell_of(square_yz + square_x[at : at + 1]) - lowest


def to_slabs(
    field_hbm, table_hbm, ty_hbm, fy_hbm, weight_hbm, out_ref, turn_ref, shell_ref, spot_ref, ty_ref, fy_ref, weight_ref, field, table, wide_ref, sems, *, scale
):
    _, width_x, width, modes = field_hbm.shape
    pairs = (table_hbm, table), (field_hbm, field), (weight_hbm, weight_ref), (ty_hbm, ty_ref), (fy_hbm, fy_ref)
    copies = [pltpu.make_async_copy(source, target, sems.at[k]) for k, (source, target) in enumerate(pairs)]
    for copy in copies:
        copy.start()
    geometry(turn_ref, shell_ref, spot_ref)
    lane = lax.broadcasted_iota(jnp.int32, (width, modes), 1)
    sign = jnp.where(lane % 2 == 0, 1.0, -1.0)
    copies[0].wait()
    copies[1].wait()
    for pair in range(0, width_x, 2):
        rows = []
        for at in (pair, pair + 1):
            real, imag = field[0, at], field[1, at]
            for factor in (None, sign):
                if factor is not None:
                    real, imag = real * factor, imag * factor
                rows.append(jnp.concatenate([real, -imag], axis=1).astype(BF16))
                rows.append(jnp.concatenate([imag, real], axis=1).astype(BF16))
        block = jnp.concatenate(rows, axis=0)
        product = lax.dot_general(
            table[...], block, (((1,), (1,)), ((), ())), preferred_element_type=F32
        ) * scale
        for k in range(2):
            wide_ref[pl.ds(pair + k, modes, stride=width_x), :] = product[:, 128 * k : 128 * (k + 1)]
    out_ref[...] = wide_ref[...].astype(BF16).reshape(out_ref.shape)
    for copy in copies[2:]:
        copy.wait()


def dot(left, right):
    return jnp.dot(left, right, preferred_element_type=F32)


def cube(parts, head):
    pr, pi, qr, qi = parts
    if head:
        first = lax.broadcasted_iota(jnp.int32, pr.shape, 0) == 0
        pick = functools.partial(jnp.where, first)
    else:
        pick = lambda special, general: general
    ar, ai = pick(pr, pr - qi), pick(pi, pi + qr)
    br, bi = pick(qr, pr + qi), pick(qi, pi - qr)
    ma = coupling * (ar * ar + ai * ai)
    mb = coupling * (br * br + bi * bi)
    ar, ai, br, bi = ma * ar, ma * ai, mb * br, mb * bi
    folded = pick(ar, ar + br), pick(ai, ai + bi), pick(br, ai - bi), pick(bi, br - ar)
    return [part.astype(BF16) for part in folded]


def planes(in_ref, ty_ref, fx_ref, fy_ref, out_ref, back_ref, *, chunk):
    modes = fx_ref.shape[0]
    grid = 2 * modes
    half = 64
    fx = fx_ref[...]
    tx = fx.T
    spots = [(x, z) for x in range(4) for z in range(2)]
    blocks = [in_ref[z, :, x].reshape(modes, 128) for x, z in spots]
    lines = jnp.concatenate(
        [jnp.concatenate([b[:, half * plane : half * (plane + 1)] for b in blocks], axis=1) for plane in range(2)], axis=0
    )
    along_y = [dot(lines[k * modes : (k + 1) * modes], ty_ref[...]).astype(BF16) for k in range(2)]
    for plane in range(2):
        mine = slice(plane * modes, (plane + 1) * modes)
        for start in range(0, grid, chunk):
            real, imag = slice(start, start + chunk), slice(grid + start, grid + start + chunk)
            even_odd = dot(tx, jnp.concatenate([along_y[plane][:, real], along_y[plane][:, imag]], axis=1))
            even, odd = even_odd[:modes], even_odd[modes:]
            parts = even[:, :chunk], even[:, chunk:], odd[:, :chunk], odd[:, chunk:]
            top, rest = cube([p[:16] for p in parts], True), cube([p[16:] for p in parts], False)
            even_r, even_i, odd_i, odd_r = (jnp.concatenate(pair, axis=0) for pair in zip(top, rest))
            folded = jnp.concatenate(
                [jnp.concatenate([even_r, even_i], axis=1), jnp.concatenate([odd_i, odd_r], axis=1)], axis=0
            )
            back_x = dot(fx, folded).astype(BF16)
            back_ref[mine, real] = back_x[:, :chunk]
            back_ref[mine, imag] = back_x[:, chunk:]
    done = dot(back_ref[...], fy_ref[...]).astype(BF16)
    for k, (x, z) in enumerate(spots):
        at = slice(half * k, half * (k + 1))
        message = jnp.concatenate([done[:modes, at], done[modes:, at]], axis=1)
        out_ref[z, :, x] = message.reshape(16, 16, 128)


def finish(
    in_ref, field_ref, table_ref, turn_ref, shell_ref, spot_ref, weight_ref, out_hbm, sums_ref, wide_ref, out_ref, energy_ref, sems, *, scale, bins
):
    _, width_x, width_y, modes = field_ref.shape
    lane = lax.broadcasted_iota(jnp.int32, (width_y, modes), 1)
    sign = jnp.where(lane % 2 == 0, 1.0, -1.0)
    wide_ref[...] = in_ref[...].reshape(wide_ref.shape).astype(F32)
    table = table_ref[...]
    copies = [
        pltpu.make_async_copy(out_ref.at[:, pl.ds(at, 1)], out_hbm.at[:, pl.ds(at, 1)], sems.at[at])
        for at in range(width_x)
    ]
    for at in range(width_x):
        slab = wide_ref[pl.ds(at, modes, stride=width_x), :].astype(BF16)
        got = lax.dot_general(slab, table, (((0,), (0,)), ((), ())), preferred_element_type=F32)
        r0, i0, r1, i1 = (got[width_y * k : width_y * (k + 1)] for k in range(4))
        non_r = (r0[:, :modes] + i0[:, modes:] + sign * (r1[:, :modes] + i1[:, modes:])) * scale
        non_i = (i0[:, :modes] - r0[:, modes:] + sign * (i1[:, :modes] - r1[:, modes:])) * scale
        u = field_ref[0, at] - non_i
        v = field_ref[1, at] + non_r
        cos, sin = turn_ref[0, at], turn_ref[1, at]
        new_r = u * cos + v * sin
        new_i = v * cos - u * sin
        out_ref[0, at] = new_r
        out_ref[1, at] = new_i
        copies[at].start()
        energy_ref[at] = new_r * new_r + new_i * new_i
    result = jnp.zeros((1, modes), F32)
    for block in range(width_y // 8):
        rows = slice(8 * block, 8 * block + 8)
        totals = []
        for k in range(bins):
            total = jnp.zeros((8, modes), F32)
            for at in range(width_x):
                total = total + jnp.where(shell_ref[at, rows] == float(k), energy_ref[at, rows], 0.0)
            totals.append(jnp.sum(total, axis=0, keepdims=True))
        totals.extend([jnp.zeros((1, modes), F32)] * (-bins % 16))
        stacked = jnp.concatenate(totals, axis=0)
        high = stacked.astype(BF16)
        left = stacked - high.astype(F32)
        middle = left.astype(BF16)
        low = (left - middle.astype(F32)).astype(BF16)
        placed = dot(jnp.concatenate([high, middle, low], axis=0), spot_ref[block])
        count = stacked.shape[0]
        placed = placed[:count] + placed[count : 2 * count] + placed[2 * count :]
        shifted = pltpu.roll(placed, 0, 1, stride=1, stride_axis=0)
        result = result + jnp.sum(shifted, axis=0, keepdims=True)
    share = result * weight_ref[...]
    lines = [share[:, 128 * k : 128 * (k + 1)] for k in range(modes // 128)]
    group = jnp.concatenate(lines * (16 // len(lines)), axis=0).astype(BF16)
    sums_ref[...] = jnp.broadcast_to(group[None], sums_ref.shape)
    for copy in copies:
        copy.wait()


def add_up(copies_ref, out_ref):
    total = jnp.sum(copies_ref[...].astype(F32), axis=0)
    lanes = out_ref.shape[0]
    out_ref[...] = jnp.sum(total.reshape(-1, lanes, 128), axis=0)


def tables(modes, scale_in, scale_out):
    grid = 2 * modes
    waves = np.arange(modes) - modes // 2
    cos, sin = trig(waves, np.arange(grid), grid)
    low_cos, low_sin = cos[:, :modes].T, sin[:, :modes].T
    z_table = np.concatenate([low_cos, low_sin], axis=1)
    blocks = modes // 32
    c, s = cos.reshape(blocks, 32, grid), sin.reshape(blocks, 32, grid)
    ty = np.stack([np.concatenate([c, s], 2), np.concatenate([-s, c], 2)], 1).reshape(2 * modes, 2 * grid)
    ct, st = c.transpose(2, 0, 1), s.transpose(2, 0, 1)
    fy = np.stack([np.stack([ct, -st], 2), np.stack([st, ct], 2)], 0).reshape(2 * grid, 2 * modes)
    odd = low_sin.copy()
    odd[0] = cos[:, modes]
    tx = np.concatenate([low_cos, odd], axis=0)
    fx = tx.T
    scaled = (z_table, ty * scale_in, fx * scale_in, fy * (scale_out * scale_out / scale_in))
    return [jnp.asarray(np.ascontiguousarray(t), BF16) for t in scaled]


def shell_counts(modes):
    wave = np.arange(modes) - modes // 2
    square = wave * wave
    total = square[:, None, None] + square[None, :, None] + square[None, None, :]
    shell = np.floor(np.sqrt(total.astype(np.float32)) + np.float32(0.5)).astype(np.int64)
    return np.bincount(shell.reshape(-1), minlength=modes)[:modes].astype(np.float32)


def in_hbm(array):
    return pltpu.with_memory_space_constraint(array, pltpu.HBM)


def params():
    return pltpu.CompilerParams(vmem_limit_bytes=48 * 1024 * 1024)


def body(field):
    _, width_x, width_y, modes = field.shape
    devices = math.prod(lax.axis_size(axis) for axis in RING)
    scale_in = 1.0 / math.sqrt(modes)
    scale_out = math.sqrt(modes) / (2 * modes)
    z_table, ty, fx, fy = tables(modes, scale_in, scale_out)
    weights = jnp.asarray((1.0 / np.maximum(shell_counts(modes), 1.0)).reshape(1, modes))
    messages, turn, shell, spot, near_ty, near_fy, near_weights, near_field, near_table = pl.pallas_call(
        functools.partial(to_slabs, scale=scale_in),
        in_specs=[pl.BlockSpec(memory_space=pltpu.HBM)] * 5,
        out_shape=[
            jax.ShapeDtypeStruct((devices, width_x, 128), BF16),
            jax.ShapeDtypeStruct(field.shape, F32),
            jax.ShapeDtypeStruct(field.shape[1:], F32),
            jax.ShapeDtypeStruct((width_y // 8, modes, modes), BF16),
            jax.ShapeDtypeStruct(ty.shape, BF16),
            jax.ShapeDtypeStruct(fy.shape, BF16),
            jax.ShapeDtypeStruct(weights.shape, F32),
            jax.ShapeDtypeStruct(field.shape, F32),
            jax.ShapeDtypeStruct(z_table.shape, BF16),
        ],
        scratch_shapes=[
            pltpu.VMEM((devices * width_x, 128), F32),
            pltpu.SemaphoreType.DMA((5,)),
        ],
        compiler_params=params(),
        name="to_slabs",
    )(*(in_hbm(array) for array in (field, z_table, ty, fy, weights)))
    slabs = lax.all_to_all(messages, RING, 0, 0, tiled=True)
    shape = (2, 16, 4, 2 * width_x, 128)
    back = pl.pallas_call(
        functools.partial(planes, chunk=128),
        out_shape=jax.ShapeDtypeStruct(shape, BF16),
        scratch_shapes=[pltpu.VMEM((2 * modes, 4 * modes), BF16)],
        compiler_params=params(),
        name="planes",
    )(slabs.reshape(shape), near_ty, fx, near_fy)
    home = lax.all_to_all(back.reshape(devices, width_x, 128), RING, 0, 0, tiled=True)
    bins = math.ceil(math.sqrt((width_x - 1) ** 2 + 49)) + 2
    lanes = modes // 128
    updated, copies = pl.pallas_call(
        functools.partial(finish, scale=scale_out, bins=bins),
        out_shape=[jax.ShapeDtypeStruct(field.shape, F32), jax.ShapeDtypeStruct((devices * lanes // 16, 16, 128), BF16)],
        out_specs=[pl.BlockSpec(memory_space=pltpu.HBM), pl.BlockSpec(memory_space=pltpu.VMEM)],
        scratch_shapes=[
            pltpu.VMEM((devices * width_x, 128), F32),
            pltpu.VMEM(field.shape, F32),
            pltpu.VMEM((width_x, width_y, modes), F32),
            pltpu.SemaphoreType.DMA((width_x,)),
        ],
        compiler_params=params(),
        name="finish",
    )(home, near_field, near_table, turn, shell, spot, near_weights)
    everyone = lax.all_to_all(copies.reshape(devices, lanes, 128), RING, 0, 0, tiled=True)
    spectrum = pl.pallas_call(
        add_up, out_shape=jax.ShapeDtypeStruct((lanes, 128), F32), compiler_params=params(), name="add_up"
    )(everyone.reshape(-1, 16, 128))
    return updated, spectrum.reshape(modes)


def solution(mesh):
    split = Mesh(mesh.devices.reshape(4, 4, 2, 4, 2), ROW + COL)
    placed = (P(None, ROW, COL, None),)
    return jax.shard_map(
        body, mesh=split, in_specs=placed, out_specs=(P(None, ROW, COL, None), P()), check_vma=False
    )
```

```python
import functools
import math

import jax
import jax.numpy as jnp
import numpy as np
from jax import lax
from jax.experimental import pallas as pl
from jax.experimental.pallas import tpu as pltpu
from jax.sharding import Mesh
from jax.sharding import PartitionSpec as P

ROW = ("z_lo", "y", "core")
COL = ("x", "z_hi")
RING = ("z_hi", "z_lo", "y", "x", "core")

phase_rate = 0.0002
coupling = 0.2

F32 = jnp.float32
BF16 = jnp.bfloat16


def trig(waves, points, length):
    turns = np.mod(np.asarray(waves)[:, None] * np.asarray(points)[None, :], length)
    angle = turns.astype(np.float32) * np.float32(2.0 * math.pi / length)
    return np.cos(angle).astype(np.float32), np.sin(angle).astype(np.float32)


def place(width_x, width_y, modes):
    row = (lax.axis_index("z_lo") * 4 + lax.axis_index("y")) * 2 + lax.axis_index("core")
    col = lax.axis_index("x") * 2 + lax.axis_index("z_hi")
    return row * width_x - modes // 2, col * width_y - modes // 2


def nearest(base, width):
    return jnp.maximum(base, -(base + width - 1))


def shell_of(squared):
    return jnp.floor(jnp.sqrt(squared.astype(F32)) + 0.5)


def phases(angle):
    return jnp.cos(angle), jnp.sin(angle)


def geometry(turn_ref, shell_ref, spot_ref):
    _, width_x, width_y, modes = turn_ref.shape
    base_x, base_y = place(width_x, width_y, modes)

    def square(shape, axis, base):
        wave = base + lax.broadcasted_iota(jnp.int32, shape, axis)
        return wave * wave

    square_x = square((width_x, modes), 0, base_x)
    square_y = square((width_y, modes), 0, base_y)
    square_z = square((8, modes), 1, -(modes // 2))
    cos_x, sin_x = phases(phase_rate * square_x[:, :128].astype(F32))
    cos_y, sin_y = phases(phase_rate * square_y[:, :128].astype(F32))
    cos_z, sin_z = phases(phase_rate * square_z.astype(F32))
    cos_x, sin_x, cos_y, sin_y = (jnp.concatenate([t] * (modes // 128), axis=1) for t in (cos_x, sin_x, cos_y, sin_y))
    column = square((modes, modes), 0, -(modes // 2))
    shells = lax.broadcasted_iota(jnp.int32, (modes, modes), 1).astype(F32)
    near_x = nearest(base_x, width_x)
    for block in range(width_y // 8):
        rows = slice(8 * block, 8 * block + 8)
        near_y = nearest(base_y + 8 * block, 8)
        near = near_x * near_x + near_y * near_y
        lowest = shell_of(near + square_z)
        spot_ref[block] = jnp.where(shell_of(near + column) == shells, 1.0, 0.0).astype(BF16)
        cos_yz = cos_y[rows] * cos_z - sin_y[rows] * sin_z
        sin_yz = sin_y[rows] * cos_z + cos_y[rows] * sin_z
        square_yz = square_y[rows] + square_z
        for at in range(width_x):
            cx, sx = cos_x[at : at + 1], sin_x[at : at + 1]
            turn_ref[0, at, rows] = cos_yz * cx - sin_yz * sx
            turn_ref[1, at, rows] = sin_yz * cx + cos_yz * sx
            shell_ref[at, rows] = shell_of(square_yz + square_x[at : at + 1]) - lowest


def to_slabs(
    field_hbm, table_hbm, ty_hbm, fy_hbm, weight_hbm, out_ref, turn_ref, shell_ref, spot_ref, ty_ref, fy_ref, weight_ref, field, table, wide_ref, sems, *, scale
):
    _, width_x, width, modes = field_hbm.shape
    pairs = (table_hbm, table), (field_hbm, field), (weight_hbm, weight_ref), (ty_hbm, ty_ref), (fy_hbm, fy_ref)
    copies = [pltpu.make_async_copy(source, target, sems.at[k]) for k, (source, target) in enumerate(pairs)]
    for copy in copies:
        copy.start()
    geometry(turn_ref, shell_ref, spot_ref)
    lane = lax.broadcasted_iota(jnp.int32, (width, modes), 1)
    sign = jnp.where(lane % 2 == 0, 1.0, -1.0)
    copies[0].wait()
    copies[1].wait()
    for pair in range(0, width_x, 2):
        rows = []
        for at in (pair, pair + 1):
            real, imag = field[0, at], field[1, at]
            for factor in (None, sign):
                if factor is not None:
                    real, imag = real * factor, imag * factor
                rows.append(jnp.concatenate([real, -imag], axis=1).astype(BF16))
                rows.append(jnp.concatenate([imag, real], axis=1).astype(BF16))
        block = jnp.concatenate(rows, axis=0)
        product = lax.dot_general(
            table[...], block, (((1,), (1,)), ((), ())), preferred_element_type=F32
        ) * scale
        for k in range(2):
            wide_ref[pl.ds(pair + k, modes, stride=width_x), :] = product[:, 128 * k : 128 * (k + 1)]
    out_ref[...] = wide_ref[...].astype(BF16).reshape(out_ref.shape)
    for copy in copies[2:]:
        copy.wait()


def dot(left, right):
    return jnp.dot(left, right, preferred_element_type=F32)


def cube(parts, head):
    pr, pi, qr, qi = parts
    if head:
        first = lax.broadcasted_iota(jnp.int32, pr.shape, 0) == 0
        pick = functools.partial(jnp.where, first)
    else:
        pick = lambda special, general: general
    ar, ai = pick(pr, pr - qi), pick(pi, pi + qr)
    br, bi = pick(qr, pr + qi), pick(qi, pi - qr)
    ma = coupling * (ar * ar + ai * ai)
    mb = coupling * (br * br + bi * bi)
    ar, ai, br, bi = ma * ar, ma * ai, mb * br, mb * bi
    folded = pick(ar, ar + br), pick(ai, ai + bi), pick(br, ai - bi), pick(bi, br - ar)
    return [part.astype(BF16) for part in folded]


def planes(in_ref, ty_ref, fx_ref, fy_ref, out_ref, back_ref, *, chunk):
    modes = fx_ref.shape[0]
    grid = 2 * modes
    half = 64
    fx = fx_ref[...]
    tx = fx.T
    spots = [(x, z) for x in range(4) for z in range(2)]
    blocks = [in_ref[z, :, x].reshape(modes, 128) for x, z in spots]
    lines = jnp.concatenate(
        [jnp.concatenate([b[:, half * plane : half * (plane + 1)] for b in blocks], axis=1) for plane in range(2)], axis=0
    )
    along_y = dot(lines, ty_ref[...]).astype(BF16)
    for plane in range(2):
        mine = slice(plane * modes, (plane + 1) * modes)
        for start in range(0, grid, chunk):
            real, imag = slice(start, start + chunk), slice(grid + start, grid + start + chunk)
            even_odd = dot(tx, jnp.concatenate([along_y[mine, real], along_y[mine, imag]], axis=1))
            even, odd = even_odd[:modes], even_odd[modes:]
            parts = even[:, :chunk], even[:, chunk:], odd[:, :chunk], odd[:, chunk:]
            top, rest = cube([p[:16] for p in parts], True), cube([p[16:] for p in parts], False)
            even_r, even_i, odd_i, odd_r = (jnp.concatenate(pair, axis=0) for pair in zip(top, rest))
            folded = jnp.concatenate(
                [jnp.concatenate([even_r, even_i], axis=1), jnp.concatenate([odd_i, odd_r], axis=1)], axis=0
            )
            back_x = dot(fx, folded).astype(BF16)
            back_ref[mine, real] = back_x[:, :chunk]
            back_ref[mine, imag] = back_x[:, chunk:]
    done = dot(back_ref[...], fy_ref[...]).astype(BF16)
    for k, (x, z) in enumerate(spots):
        at = slice(half * k, half * (k + 1))
        message = jnp.concatenate([done[:modes, at], done[modes:, at]], axis=1)
        out_ref[z, :, x] = message.reshape(16, 16, 128)


def finish(
    in_ref, field_ref, table_ref, turn_ref, shell_ref, spot_ref, weight_ref, out_hbm, sums_ref, wide_ref, out_ref, energy_ref, sems, *, scale, bins
):
    _, width_x, width_y, modes = field_ref.shape
    lane = lax.broadcasted_iota(jnp.int32, (width_y, modes), 1)
    sign = jnp.where(lane % 2 == 0, 1.0, -1.0)
    wide_ref[...] = in_ref[...].reshape(wide_ref.shape).astype(F32)
    table = table_ref[...]
    copies = [
        pltpu.make_async_copy(out_ref.at[:, pl.ds(at, 1)], out_hbm.at[:, pl.ds(at, 1)], sems.at[at])
        for at in range(width_x)
    ]
    for at in range(width_x):
        slab = wide_ref[pl.ds(at, modes, stride=width_x), :].astype(BF16)
        got = lax.dot_general(slab, table, (((0,), (0,)), ((), ())), preferred_element_type=F32)
        r0, i0, r1, i1 = (got[width_y * k : width_y * (k + 1)] for k in range(4))
        non_r = (r0[:, :modes] + i0[:, modes:] + sign * (r1[:, :modes] + i1[:, modes:])) * scale
        non_i = (i0[:, :modes] - r0[:, modes:] + sign * (i1[:, :modes] - r1[:, modes:])) * scale
        u = field_ref[0, at] - non_i
        v = field_ref[1, at] + non_r
        cos, sin = turn_ref[0, at], turn_ref[1, at]
        new_r = u * cos + v * sin
        new_i = v * cos - u * sin
        out_ref[0, at] = new_r
        out_ref[1, at] = new_i
        copies[at].start()
        energy_ref[at] = new_r * new_r + new_i * new_i
    result = jnp.zeros((1, modes), F32)
    for block in range(width_y // 8):
        rows = slice(8 * block, 8 * block + 8)
        totals = []
        for k in range(bins):
            total = jnp.zeros((8, modes), F32)
            for at in range(width_x):
                total = total + jnp.where(shell_ref[at, rows] == float(k), energy_ref[at, rows], 0.0)
            totals.append(jnp.sum(total, axis=0, keepdims=True))
        totals.extend([jnp.zeros((1, modes), F32)] * (-bins % 16))
        stacked = jnp.concatenate(totals, axis=0)
        high = stacked.astype(BF16)
        left = stacked - high.astype(F32)
        middle = left.astype(BF16)
        low = (left - middle.astype(F32)).astype(BF16)
        placed = dot(jnp.concatenate([high, middle, low], axis=0), spot_ref[block])
        count = stacked.shape[0]
        placed = placed[:count] + placed[count : 2 * count] + placed[2 * count :]
        shifted = pltpu.roll(placed, 0, 1, stride=1, stride_axis=0)
        result = result + jnp.sum(shifted, axis=0, keepdims=True)
    sums_ref[...] = result * weight_ref[...]
    for copy in copies:
        copy.wait()


def add_up(copies_ref, out_ref):
    total = jnp.sum(copies_ref[...].astype(F32), axis=0)
    lanes = out_ref.shape[0]
    out_ref[...] = jnp.sum(total.reshape(-1, lanes, 128), axis=0)


def tables(modes, scale_in, scale_out):
    grid = 2 * modes
    waves = np.arange(modes) - modes // 2
    cos, sin = trig(waves, np.arange(grid), grid)
    low_cos, low_sin = cos[:, :modes].T, sin[:, :modes].T
    z_table = np.concatenate([low_cos, low_sin], axis=1)
    blocks = modes // 32
    c, s = cos.reshape(blocks, 32, grid), sin.reshape(blocks, 32, grid)
    ty = np.stack([np.concatenate([c, s], 2), np.concatenate([-s, c], 2)], 1).reshape(2 * modes, 2 * grid)
    ct, st = c.transpose(2, 0, 1), s.transpose(2, 0, 1)
    fy = np.stack([np.stack([ct, -st], 2), np.stack([st, ct], 2)], 0).reshape(2 * grid, 2 * modes)
    odd = low_sin.copy()
    odd[0] = cos[:, modes]
    tx = np.concatenate([low_cos, odd], axis=0)
    fx = tx.T
    scaled = (z_table, ty * scale_in, fx * scale_in, fy * (scale_out * scale_out / scale_in))
    return [jnp.asarray(np.ascontiguousarray(t), BF16) for t in scaled]


def shell_counts(modes):
    wave = np.arange(modes) - modes // 2
    square = wave * wave
    total = square[:, None, None] + square[None, :, None] + square[None, None, :]
    shell = np.floor(np.sqrt(total.astype(np.float32)) + np.float32(0.5)).astype(np.int64)
    return np.bincount(shell.reshape(-1), minlength=modes)[:modes].astype(np.float32)


def in_hbm(array):
    return pltpu.with_memory_space_constraint(array, pltpu.HBM)


def params():
    return pltpu.CompilerParams(vmem_limit_bytes=48 * 1024 * 1024)


def body(field):
    _, width_x, width_y, modes = field.shape
    devices = math.prod(lax.axis_size(axis) for axis in RING)
    scale_in = 1.0 / math.sqrt(modes)
    scale_out = math.sqrt(modes) / (2 * modes)
    z_table, ty, fx, fy = tables(modes, scale_in, scale_out)
    weights = jnp.asarray((1.0 / np.maximum(shell_counts(modes), 1.0)).reshape(1, modes))
    messages, turn, shell, spot, near_ty, near_fy, near_weights, near_field, near_table = pl.pallas_call(
        functools.partial(to_slabs, scale=scale_in),
        in_specs=[pl.BlockSpec(memory_space=pltpu.HBM)] * 5,
        out_shape=[
            jax.ShapeDtypeStruct((devices, width_x, 128), BF16),
            jax.ShapeDtypeStruct(field.shape, F32),
            jax.ShapeDtypeStruct(field.shape[1:], F32),
            jax.ShapeDtypeStruct((width_y // 8, modes, modes), BF16),
            jax.ShapeDtypeStruct(ty.shape, BF16),
            jax.ShapeDtypeStruct(fy.shape, BF16),
            jax.ShapeDtypeStruct(weights.shape, F32),
            jax.ShapeDtypeStruct(field.shape, F32),
            jax.ShapeDtypeStruct(z_table.shape, BF16),
        ],
        scratch_shapes=[
            pltpu.VMEM((devices * width_x, 128), F32),
            pltpu.SemaphoreType.DMA((5,)),
        ],
        compiler_params=params(),
        name="to_slabs",
    )(*(in_hbm(array) for array in (field, z_table, ty, fy, weights)))
    slabs = lax.all_to_all(messages, RING, 0, 0, tiled=True)
    shape = (2, 16, 4, 2 * width_x, 128)
    back = pl.pallas_call(
        functools.partial(planes, chunk=128),
        out_shape=jax.ShapeDtypeStruct(shape, BF16),
        scratch_shapes=[pltpu.VMEM((2 * modes, 4 * modes), BF16)],
        compiler_params=params(),
        name="planes",
    )(slabs.reshape(shape), near_ty, fx, near_fy)
    home = lax.all_to_all(back.reshape(devices, width_x, 128), RING, 0, 0, tiled=True)
    bins = math.ceil(math.sqrt((width_x - 1) ** 2 + 49)) + 2
    updated, sums = pl.pallas_call(
        functools.partial(finish, scale=scale_out, bins=bins),
        out_shape=[jax.ShapeDtypeStruct(field.shape, F32), jax.ShapeDtypeStruct((1, modes), F32)],
        out_specs=[pl.BlockSpec(memory_space=pltpu.HBM), pl.BlockSpec(memory_space=pltpu.VMEM)],
        scratch_shapes=[
            pltpu.VMEM((devices * width_x, 128), F32),
            pltpu.VMEM(field.shape, F32),
            pltpu.VMEM((width_x, width_y, modes), F32),
            pltpu.SemaphoreType.DMA((width_x,)),
        ],
        compiler_params=params(),
        name="finish",
    )(home, near_field, near_table, turn, shell, spot, near_weights)
    lanes = modes // 128
    sums = sums + lax.ppermute(sums, "core", [(0, 1), (1, 0)])
    chips = devices // 2
    copies = jnp.broadcast_to(sums.reshape(1, lanes, 128).astype(BF16), (chips, lanes, 128))
    everyone = lax.all_to_all(copies, RING[:-1], 0, 0, tiled=True)
    spectrum = pl.pallas_call(
        add_up, out_shape=jax.ShapeDtypeStruct((lanes, 128), F32), compiler_params=params(), name="add_up"
    )(everyone.reshape(-1, 16, 128))
    return updated, spectrum.reshape(modes)


def solution(mesh):
    split = Mesh(mesh.devices.reshape(4, 4, 2, 4, 2), ROW + COL)
    placed = (P(None, ROW, COL, None),)
    return jax.shard_map(
        body, mesh=split, in_specs=placed, out_specs=(P(None, ROW, COL, None), P()), check_vma=False
    )
```

```python
import functools
import math

import jax
import jax.numpy as jnp
import numpy as np
from jax import lax
from jax.experimental import pallas as pl
from jax.experimental.pallas import tpu as pltpu
from jax.sharding import Mesh
from jax.sharding import PartitionSpec as P

ROW = ("z_lo", "y", "core")
COL = ("x", "z_hi")
RING = ("z_hi", "z_lo", "y", "x", "core")

phase_rate = 0.0002
coupling = 0.2

F32 = jnp.float32
BF16 = jnp.bfloat16


def trig(waves, points, length):
    turns = np.mod(np.asarray(waves)[:, None] * np.asarray(points)[None, :], length)
    angle = turns.astype(np.float32) * np.float32(2.0 * math.pi / length)
    return np.cos(angle).astype(np.float32), np.sin(angle).astype(np.float32)


def place(width_x, width_y, modes):
    row = (lax.axis_index("z_lo") * 4 + lax.axis_index("y")) * 2 + lax.axis_index("core")
    col = lax.axis_index("x") * 2 + lax.axis_index("z_hi")
    return row * width_x - modes // 2, col * width_y - modes // 2


def nearest(base, width):
    return jnp.maximum(base, -(base + width - 1))


def shell_of(squared):
    return jnp.floor(jnp.sqrt(squared.astype(F32)) + 0.5)


def phases(angle):
    return jnp.cos(angle), jnp.sin(angle)


def geometry(turn_ref, shell_ref, spot_ref):
    _, width_x, width_y, modes = turn_ref.shape
    base_x, base_y = place(width_x, width_y, modes)

    def square(shape, axis, base):
        wave = base + lax.broadcasted_iota(jnp.int32, shape, axis)
        return wave * wave

    square_x = square((width_x, modes), 0, base_x)
    square_y = square((width_y, modes), 0, base_y)
    square_z = square((8, modes), 1, -(modes // 2))
    cos_x, sin_x = phases(phase_rate * square_x[:, :128].astype(F32))
    cos_y, sin_y = phases(phase_rate * square_y[:, :128].astype(F32))
    cos_z, sin_z = phases(phase_rate * square_z.astype(F32))
    cos_x, sin_x, cos_y, sin_y = (jnp.concatenate([t] * (modes // 128), axis=1) for t in (cos_x, sin_x, cos_y, sin_y))
    column = square((modes, modes), 0, -(modes // 2))
    shells = lax.broadcasted_iota(jnp.int32, (modes, modes), 1).astype(F32)
    near_x = nearest(base_x, width_x)
    for block in range(width_y // 8):
        rows = slice(8 * block, 8 * block + 8)
        near_y = nearest(base_y + 8 * block, 8)
        near = near_x * near_x + near_y * near_y
        lowest = shell_of(near + square_z)
        spot_ref[block] = jnp.where(shell_of(near + column) == shells, 1.0, 0.0).astype(BF16)
        cos_yz = cos_y[rows] * cos_z - sin_y[rows] * sin_z
        sin_yz = sin_y[rows] * cos_z + cos_y[rows] * sin_z
        square_yz = square_y[rows] + square_z
        for at in range(width_x):
            cx, sx = cos_x[at : at + 1], sin_x[at : at + 1]
            turn_ref[0, at, rows] = cos_yz * cx - sin_yz * sx
            turn_ref[1, at, rows] = sin_yz * cx + cos_yz * sx
            shell_ref[at, rows] = shell_of(square_yz + square_x[at : at + 1]) - lowest


def to_slabs(
    field_hbm, table_hbm, ty_hbm, fy_hbm, weight_hbm, out_ref, turn_ref, shell_ref, spot_ref, ty_ref, fy_ref, weight_ref, field, table, wide_ref, sems, *, scale
):
    _, width_x, width, modes = field_hbm.shape
    pairs = (table_hbm, table), (field_hbm, field), (weight_hbm, weight_ref), (ty_hbm, ty_ref), (fy_hbm, fy_ref)
    copies = [pltpu.make_async_copy(source, target, sems.at[k]) for k, (source, target) in enumerate(pairs)]
    for copy in copies:
        copy.start()
    geometry(turn_ref, shell_ref, spot_ref)
    lane = lax.broadcasted_iota(jnp.int32, (width, modes), 1)
    sign = jnp.where(lane % 2 == 0, 1.0, -1.0)
    copies[0].wait()
    copies[1].wait()
    for pair in range(0, width_x, 2):
        rows = []
        for at in (pair, pair + 1):
            real, imag = field[0, at], field[1, at]
            for factor in (None, sign):
                if factor is not None:
                    real, imag = real * factor, imag * factor
                rows.append(jnp.concatenate([real, -imag], axis=1).astype(BF16))
                rows.append(jnp.concatenate([imag, real], axis=1).astype(BF16))
        block = jnp.concatenate(rows, axis=0)
        product = lax.dot_general(
            table[...], block, (((1,), (1,)), ((), ())), preferred_element_type=F32
        ) * scale
        for k in range(2):
            wide_ref[pl.ds(pair + k, modes, stride=width_x), :] = product[:, 128 * k : 128 * (k + 1)]
    out_ref[...] = wide_ref[...].astype(BF16).reshape(out_ref.shape)
    for copy in copies[2:]:
        copy.wait()


def dot(left, right):
    return jnp.dot(left, right, preferred_element_type=F32)


def cube(parts, head):
    pr, pi, qr, qi = parts
    if head:
        first = lax.broadcasted_iota(jnp.int32, pr.shape, 0) == 0
        pick = functools.partial(jnp.where, first)
    else:
        pick = lambda special, general: general
    ar, ai = pick(pr, pr - qi), pick(pi, pi + qr)
    br, bi = pick(qr, pr + qi), pick(qi, pi - qr)
    ma = coupling * (ar * ar + ai * ai)
    mb = coupling * (br * br + bi * bi)
    ar, ai, br, bi = ma * ar, ma * ai, mb * br, mb * bi
    folded = pick(ar, ar + br), pick(ai, ai + bi), pick(br, ai - bi), pick(bi, br - ar)
    return [part.astype(BF16) for part in folded]


def planes(in_ref, ty_ref, fx_ref, fy_ref, out_ref, back_ref, *, chunk):
    modes = fx_ref.shape[0]
    grid = 2 * modes
    half = 64
    fx = fx_ref[...]
    tx = fx.T
    spots = [(x, z) for x in range(4) for z in range(2)]
    blocks = [in_ref[z, :, x].reshape(modes, 128) for x, z in spots]
    lines = jnp.concatenate(
        [jnp.concatenate([b[:, half * plane : half * (plane + 1)] for b in blocks], axis=1) for plane in range(2)], axis=0
    )
    along_y = dot(lines, ty_ref[...]).astype(BF16)
    for plane in range(2):
        mine = slice(plane * modes, (plane + 1) * modes)
        for start in range(0, grid, chunk):
            real, imag = slice(start, start + chunk), slice(grid + start, grid + start + chunk)
            even_odd = dot(tx, jnp.concatenate([along_y[mine, real], along_y[mine, imag]], axis=1))
            even, odd = even_odd[:modes], even_odd[modes:]
            parts = even[:, :chunk], even[:, chunk:], odd[:, :chunk], odd[:, chunk:]
            top, rest = cube([p[:16] for p in parts], True), cube([p[16:] for p in parts], False)
            even_r, even_i, odd_i, odd_r = (jnp.concatenate(pair, axis=0) for pair in zip(top, rest))
            folded = jnp.concatenate(
                [jnp.concatenate([even_r, even_i], axis=1), jnp.concatenate([odd_i, odd_r], axis=1)], axis=0
            )
            back_x = dot(fx, folded).astype(BF16)
            back_ref[mine, real] = back_x[:, :chunk]
            back_ref[mine, imag] = back_x[:, chunk:]
    done = dot(back_ref[...], fy_ref[...]).astype(BF16)
    for k, (x, z) in enumerate(spots):
        at = slice(half * k, half * (k + 1))
        message = jnp.concatenate([done[:modes, at], done[modes:, at]], axis=1)
        out_ref[z, :, x] = message.reshape(16, 16, 128)


def finish(
    in_ref, field_ref, table_ref, turn_ref, shell_ref, spot_ref, weight_ref, out_ref, sums_ref, wide_ref, energy_ref, *, scale, bins
):
    _, width_x, width_y, modes = field_ref.shape
    lane = lax.broadcasted_iota(jnp.int32, (width_y, modes), 1)
    sign = jnp.where(lane % 2 == 0, 1.0, -1.0)
    wide_ref[...] = in_ref[...].reshape(wide_ref.shape).astype(F32)
    table = table_ref[...]
    for at in range(width_x):
        slab = wide_ref[pl.ds(at, modes, stride=width_x), :].astype(BF16)
        got = lax.dot_general(slab, table, (((0,), (0,)), ((), ())), preferred_element_type=F32)
        r0, i0, r1, i1 = (got[width_y * k : width_y * (k + 1)] for k in range(4))
        non_r = (r0[:, :modes] + i0[:, modes:] + sign * (r1[:, :modes] + i1[:, modes:])) * scale
        non_i = (i0[:, :modes] - r0[:, modes:] + sign * (i1[:, :modes] - r1[:, modes:])) * scale
        u = field_ref[0, at] - non_i
        v = field_ref[1, at] + non_r
        cos, sin = turn_ref[0, at], turn_ref[1, at]
        new_r = u * cos + v * sin
        new_i = v * cos - u * sin
        out_ref[0, at] = new_r
        out_ref[1, at] = new_i
        energy_ref[at] = new_r * new_r + new_i * new_i
    result = jnp.zeros((1, modes), F32)
    for block in range(width_y // 8):
        rows = slice(8 * block, 8 * block + 8)
        totals = []
        for k in range(bins):
            total = jnp.zeros((8, modes), F32)
            for at in range(width_x):
                total = total + jnp.where(shell_ref[at, rows] == float(k), energy_ref[at, rows], 0.0)
            totals.append(jnp.sum(total, axis=0, keepdims=True))
        totals.extend([jnp.zeros((1, modes), F32)] * (-bins % 16))
        stacked = jnp.concatenate(totals, axis=0)
        high = stacked.astype(BF16)
        left = stacked - high.astype(F32)
        middle = left.astype(BF16)
        low = (left - middle.astype(F32)).astype(BF16)
        placed = dot(jnp.concatenate([high, middle, low], axis=0), spot_ref[block])
        count = stacked.shape[0]
        placed = placed[:count] + placed[count : 2 * count] + placed[2 * count :]
        shifted = pltpu.roll(placed, 0, 1, stride=1, stride_axis=0)
        result = result + jnp.sum(shifted, axis=0, keepdims=True)
    sums_ref[...] = result * weight_ref[...]


def put_out(kept_ref, sums_ref, out_hbm, same_ref, sem):
    copy = pltpu.make_async_copy(kept_ref, out_hbm, sem)
    copy.start()
    same_ref[...] = sums_ref[...]
    copy.wait()


def add_up(copies_ref, out_ref):
    total = jnp.sum(copies_ref[...].astype(F32), axis=0)
    lanes = out_ref.shape[0]
    out_ref[...] = jnp.sum(total.reshape(-1, lanes, 128), axis=0)


def tables(modes, scale_in, scale_out):
    grid = 2 * modes
    waves = np.arange(modes) - modes // 2
    cos, sin = trig(waves, np.arange(grid), grid)
    low_cos, low_sin = cos[:, :modes].T, sin[:, :modes].T
    z_table = np.concatenate([low_cos, low_sin], axis=1)
    blocks = modes // 32
    c, s = cos.reshape(blocks, 32, grid), sin.reshape(blocks, 32, grid)
    ty = np.stack([np.concatenate([c, s], 2), np.concatenate([-s, c], 2)], 1).reshape(2 * modes, 2 * grid)
    ct, st = c.transpose(2, 0, 1), s.transpose(2, 0, 1)
    fy = np.stack([np.stack([ct, -st], 2), np.stack([st, ct], 2)], 0).reshape(2 * grid, 2 * modes)
    odd = low_sin.copy()
    odd[0] = cos[:, modes]
    tx = np.concatenate([low_cos, odd], axis=0)
    fx = tx.T
    scaled = (z_table, ty * scale_in, fx * scale_in, fy * (scale_out * scale_out / scale_in))
    return [jnp.asarray(np.ascontiguousarray(t), BF16) for t in scaled]


def shell_counts(modes):
    wave = np.arange(modes) - modes // 2
    square = wave * wave
    total = square[:, None, None] + square[None, :, None] + square[None, None, :]
    shell = np.floor(np.sqrt(total.astype(np.float32)) + np.float32(0.5)).astype(np.int64)
    return np.bincount(shell.reshape(-1), minlength=modes)[:modes].astype(np.float32)


def in_hbm(array):
    return pltpu.with_memory_space_constraint(array, pltpu.HBM)


def params():
    return pltpu.CompilerParams(vmem_limit_bytes=48 * 1024 * 1024)


def body(field):
    _, width_x, width_y, modes = field.shape
    devices = math.prod(lax.axis_size(axis) for axis in RING)
    scale_in = 1.0 / math.sqrt(modes)
    scale_out = math.sqrt(modes) / (2 * modes)
    z_table, ty, fx, fy = tables(modes, scale_in, scale_out)
    weights = jnp.asarray((1.0 / np.maximum(shell_counts(modes), 1.0)).reshape(1, modes))
    messages, turn, shell, spot, near_ty, near_fy, near_weights, near_field, near_table = pl.pallas_call(
        functools.partial(to_slabs, scale=scale_in),
        in_specs=[pl.BlockSpec(memory_space=pltpu.HBM)] * 5,
        out_shape=[
            jax.ShapeDtypeStruct((devices, width_x, 128), BF16),
            jax.ShapeDtypeStruct(field.shape, F32),
            jax.ShapeDtypeStruct(field.shape[1:], F32),
            jax.ShapeDtypeStruct((width_y // 8, modes, modes), BF16),
            jax.ShapeDtypeStruct(ty.shape, BF16),
            jax.ShapeDtypeStruct(fy.shape, BF16),
            jax.ShapeDtypeStruct(weights.shape, F32),
            jax.ShapeDtypeStruct(field.shape, F32),
            jax.ShapeDtypeStruct(z_table.shape, BF16),
        ],
        scratch_shapes=[
            pltpu.VMEM((devices * width_x, 128), F32),
            pltpu.SemaphoreType.DMA((5,)),
        ],
        compiler_params=params(),
        name="to_slabs",
    )(*(in_hbm(array) for array in (field, z_table, ty, fy, weights)))
    slabs = lax.all_to_all(messages, RING, 0, 0, tiled=True)
    shape = (2, 16, 4, 2 * width_x, 128)
    back = pl.pallas_call(
        functools.partial(planes, chunk=128),
        out_shape=jax.ShapeDtypeStruct(shape, BF16),
        scratch_shapes=[pltpu.VMEM((2 * modes, 4 * modes), BF16)],
        compiler_params=params(),
        name="planes",
    )(slabs.reshape(shape), near_ty, fx, near_fy)
    home = lax.all_to_all(back.reshape(devices, width_x, 128), RING, 0, 0, tiled=True)
    bins = math.ceil(math.sqrt((width_x - 1) ** 2 + 49)) + 2
    kept, sums = pl.pallas_call(
        functools.partial(finish, scale=scale_out, bins=bins),
        out_shape=[pltpu.VMEM(field.shape, F32), jax.ShapeDtypeStruct((1, modes), F32)],
        scratch_shapes=[pltpu.VMEM((devices * width_x, 128), F32), pltpu.VMEM((width_x, width_y, modes), F32)],
        compiler_params=params(),
        name="finish",
    )(home, near_field, near_table, turn, shell, spot, near_weights)
    lanes = modes // 128
    other = lax.ppermute(sums, "core", [(0, 1), (1, 0)])
    updated, same = pl.pallas_call(
        put_out,
        in_specs=[pl.BlockSpec(memory_space=pltpu.VMEM)] * 2,
        out_shape=[jax.ShapeDtypeStruct(field.shape, F32), jax.ShapeDtypeStruct(sums.shape, F32)],
        out_specs=[pl.BlockSpec(memory_space=pltpu.HBM), pl.BlockSpec(memory_space=pltpu.VMEM)],
        scratch_shapes=[pltpu.SemaphoreType.DMA(())],
        compiler_params=params(),
        name="put_out",
    )(kept, sums)
    sums = same + other
    chips = devices // 2
    copies = jnp.broadcast_to(sums.reshape(1, lanes, 128).astype(BF16), (chips, lanes, 128))
    everyone = lax.all_to_all(copies, RING[:-1], 0, 0, tiled=True)
    spectrum = pl.pallas_call(
        add_up, out_shape=jax.ShapeDtypeStruct((lanes, 128), F32), compiler_params=params(), name="add_up"
    )(everyone.reshape(-1, 16, 128))
    return updated, spectrum.reshape(modes)


def solution(mesh):
    split = Mesh(mesh.devices.reshape(4, 4, 2, 4, 2), ROW + COL)
    placed = (P(None, ROW, COL, None),)
    return jax.shard_map(
        body, mesh=split, in_specs=placed, out_specs=(P(None, ROW, COL, None), P()), check_vma=False
    )
```

```python
import functools
import math

import jax
import jax.numpy as jnp
import numpy as np
from jax import lax
from jax.experimental import pallas as pl
from jax.experimental.pallas import tpu as pltpu
from jax.sharding import Mesh
from jax.sharding import PartitionSpec as P

ROW = ("z_lo", "y", "core")
COL = ("x", "z_hi")
RING = ("z_hi", "z_lo", "y", "x", "core")

phase_rate = 0.0002
coupling = 0.2

F32 = jnp.float32
BF16 = jnp.bfloat16


def trig(waves, points, length):
    turns = np.mod(np.asarray(waves)[:, None] * np.asarray(points)[None, :], length)
    angle = turns.astype(np.float32) * np.float32(2.0 * math.pi / length)
    return np.cos(angle).astype(np.float32), np.sin(angle).astype(np.float32)


def place(width_x, width_y, modes):
    row = (lax.axis_index("z_lo") * 4 + lax.axis_index("y")) * 2 + lax.axis_index("core")
    col = lax.axis_index("x") * 2 + lax.axis_index("z_hi")
    return row * width_x - modes // 2, col * width_y - modes // 2


def nearest(base, width):
    return jnp.maximum(base, -(base + width - 1))


def shell_of(squared):
    return jnp.floor(jnp.sqrt(squared.astype(F32)) + 0.5)


def phases(angle):
    return jnp.cos(angle), jnp.sin(angle)


def geometry(turn_ref, shell_ref, spot_ref):
    _, width_x, width_y, modes = turn_ref.shape
    base_x, base_y = place(width_x, width_y, modes)

    def square(shape, axis, base):
        wave = base + lax.broadcasted_iota(jnp.int32, shape, axis)
        return wave * wave

    square_x = square((width_x, modes), 0, base_x)
    square_y = square((width_y, modes), 0, base_y)
    square_z = square((8, modes), 1, -(modes // 2))
    cos_x, sin_x = phases(phase_rate * square_x[:, :128].astype(F32))
    cos_y, sin_y = phases(phase_rate * square_y[:, :128].astype(F32))
    cos_z, sin_z = phases(phase_rate * square_z.astype(F32))
    cos_x, sin_x, cos_y, sin_y = (jnp.concatenate([t] * (modes // 128), axis=1) for t in (cos_x, sin_x, cos_y, sin_y))
    column = square((modes, modes), 0, -(modes // 2))
    shells = lax.broadcasted_iota(jnp.int32, (modes, modes), 1).astype(F32)
    near_x = nearest(base_x, width_x)
    for block in range(width_y // 8):
        rows = slice(8 * block, 8 * block + 8)
        near_y = nearest(base_y + 8 * block, 8)
        near = near_x * near_x + near_y * near_y
        lowest = shell_of(near + square_z)
        spot_ref[block] = jnp.where(shell_of(near + column) == shells, 1.0, 0.0).astype(BF16)
        cos_yz = cos_y[rows] * cos_z - sin_y[rows] * sin_z
        sin_yz = sin_y[rows] * cos_z + cos_y[rows] * sin_z
        square_yz = square_y[rows] + square_z
        for at in range(width_x):
            cx, sx = cos_x[at : at + 1], sin_x[at : at + 1]
            turn_ref[0, at, rows] = cos_yz * cx - sin_yz * sx
            turn_ref[1, at, rows] = sin_yz * cx + cos_yz * sx
            shell_ref[at, rows] = shell_of(square_yz + square_x[at : at + 1]) - lowest


def to_slabs(
    field_hbm, table_hbm, ty_hbm, fy_hbm, weight_hbm, out_ref, turn_ref, shell_ref, spot_ref, ty_ref, fy_ref, weight_ref, field, table, wide_ref, sems, *, scale
):
    _, width_x, width, modes = field_hbm.shape
    pairs = (table_hbm, table), (field_hbm, field), (weight_hbm, weight_ref), (ty_hbm, ty_ref), (fy_hbm, fy_ref)
    copies = [pltpu.make_async_copy(source, target, sems.at[k]) for k, (source, target) in enumerate(pairs)]
    for copy in copies:
        copy.start()
    geometry(turn_ref, shell_ref, spot_ref)
    lane = lax.broadcasted_iota(jnp.int32, (width, modes), 1)
    sign = jnp.where(lane % 2 == 0, 1.0, -1.0)
    copies[0].wait()
    copies[1].wait()
    for pair in range(0, width_x, 2):
        rows = []
        for at in (pair, pair + 1):
            real, imag = field[0, at], field[1, at]
            for factor in (None, sign):
                if factor is not None:
                    real, imag = real * factor, imag * factor
                rows.append(jnp.concatenate([real, -imag], axis=1).astype(BF16))
                rows.append(jnp.concatenate([imag, real], axis=1).astype(BF16))
        block = jnp.concatenate(rows, axis=0)
        product = lax.dot_general(
            table[...], block, (((1,), (1,)), ((), ())), preferred_element_type=F32
        ) * scale
        for k in range(2):
            wide_ref[pl.ds(pair + k, modes, stride=width_x), :] = product[:, 128 * k : 128 * (k + 1)]
    out_ref[...] = wide_ref[...].astype(BF16).reshape(out_ref.shape)
    for copy in copies[2:]:
        copy.wait()


def dot(left, right):
    return jnp.dot(left, right, preferred_element_type=F32)


def cube(parts, head):
    pr, pi, qr, qi = parts
    if head:
        first = lax.broadcasted_iota(jnp.int32, pr.shape, 0) == 0
        pick = functools.partial(jnp.where, first)
    else:
        pick = lambda special, general: general
    ar, ai = pick(pr, pr - qi), pick(pi, pi + qr)
    br, bi = pick(qr, pr + qi), pick(qi, pi - qr)
    ma = coupling * (ar * ar + ai * ai)
    mb = coupling * (br * br + bi * bi)
    ar, ai, br, bi = ma * ar, ma * ai, mb * br, mb * bi
    folded = pick(ar, ar + br), pick(ai, ai + bi), pick(br, ai - bi), pick(bi, br - ar)
    return [part.astype(BF16) for part in folded]


def planes(in_ref, ty_ref, fx_ref, fy_ref, out_ref, back_ref, *, chunk):
    modes = fx_ref.shape[0]
    grid = 2 * modes
    half = 64
    fx = fx_ref[...]
    tx = fx.T
    spots = [(x, z) for x in range(4) for z in range(2)]
    blocks = [in_ref[z, :, x].reshape(modes, 128) for x, z in spots]
    lines = jnp.concatenate(
        [jnp.concatenate([b[:, half * plane : half * (plane + 1)] for b in blocks], axis=1) for plane in range(2)], axis=0
    )
    along_y = [dot(lines[k * modes : (k + 1) * modes], ty_ref[...]).astype(BF16) for k in range(2)]
    for plane in range(2):
        mine = slice(plane * modes, (plane + 1) * modes)
        for start in range(0, grid, chunk):
            real, imag = slice(start, start + chunk), slice(grid + start, grid + start + chunk)
            even_odd = dot(tx, jnp.concatenate([along_y[plane][:, real], along_y[plane][:, imag]], axis=1))
            even, odd = even_odd[:modes], even_odd[modes:]
            parts = even[:, :chunk], even[:, chunk:], odd[:, :chunk], odd[:, chunk:]
            top, rest = cube([p[:16] for p in parts], True), cube([p[16:] for p in parts], False)
            even_r, even_i, odd_i, odd_r = (jnp.concatenate(pair, axis=0) for pair in zip(top, rest))
            folded = jnp.concatenate(
                [jnp.concatenate([even_r, even_i], axis=1), jnp.concatenate([odd_i, odd_r], axis=1)], axis=0
            )
            back_x = dot(fx, folded).astype(BF16)
            back_ref[mine, real] = back_x[:, :chunk]
            back_ref[mine, imag] = back_x[:, chunk:]
    done = dot(back_ref[...], fy_ref[...]).astype(BF16)
    for k, (x, z) in enumerate(spots):
        at = slice(half * k, half * (k + 1))
        message = jnp.concatenate([done[:modes, at], done[modes:, at]], axis=1)
        out_ref[z, :, x] = message.reshape(16, 16, 128)


def finish(
    in_ref, field_ref, table_ref, turn_ref, shell_ref, spot_ref, weight_ref, out_ref, sums_ref, wide_ref, energy_ref, *, scale, bins
):
    _, width_x, width_y, modes = field_ref.shape
    lane = lax.broadcasted_iota(jnp.int32, (width_y, modes), 1)
    sign = jnp.where(lane % 2 == 0, 1.0, -1.0)
    wide_ref[...] = in_ref[...].reshape(wide_ref.shape).astype(F32)
    table = table_ref[...]
    for at in range(width_x):
        slab = wide_ref[pl.ds(at, modes, stride=width_x), :].astype(BF16)
        got = lax.dot_general(slab, table, (((0,), (0,)), ((), ())), preferred_element_type=F32)
        r0, i0, r1, i1 = (got[width_y * k : width_y * (k + 1)] for k in range(4))
        non_r = (r0[:, :modes] + i0[:, modes:] + sign * (r1[:, :modes] + i1[:, modes:])) * scale
        non_i = (i0[:, :modes] - r0[:, modes:] + sign * (i1[:, :modes] - r1[:, modes:])) * scale
        u = field_ref[0, at] - non_i
        v = field_ref[1, at] + non_r
        cos, sin = turn_ref[0, at], turn_ref[1, at]
        new_r = u * cos + v * sin
        new_i = v * cos - u * sin
        out_ref[0, at] = new_r
        out_ref[1, at] = new_i
        energy_ref[at] = new_r * new_r + new_i * new_i
    result = jnp.zeros((1, modes), F32)
    for block in range(width_y // 8):
        rows = slice(8 * block, 8 * block + 8)
        totals = []
        for k in range(bins):
            total = jnp.zeros((8, modes), F32)
            for at in range(width_x):
                total = total + jnp.where(shell_ref[at, rows] == float(k), energy_ref[at, rows], 0.0)
            totals.append(jnp.sum(total, axis=0, keepdims=True))
        totals.extend([jnp.zeros((1, modes), F32)] * (-bins % 16))
        stacked = jnp.concatenate(totals, axis=0)
        high = stacked.astype(BF16)
        left = stacked - high.astype(F32)
        middle = left.astype(BF16)
        low = (left - middle.astype(F32)).astype(BF16)
        placed = dot(jnp.concatenate([high, middle, low], axis=0), spot_ref[block])
        count = stacked.shape[0]
        placed = placed[:count] + placed[count : 2 * count] + placed[2 * count :]
        shifted = pltpu.roll(placed, 0, 1, stride=1, stride_axis=0)
        result = result + jnp.sum(shifted, axis=0, keepdims=True)
    sums_ref[...] = result * weight_ref[...]


def put_out(kept_ref, sums_ref, out_hbm, same_ref, sem):
    copy = pltpu.make_async_copy(kept_ref, out_hbm, sem)
    copy.start()
    same_ref[...] = sums_ref[...]
    copy.wait()


def add_up(copies_ref, out_ref):
    total = jnp.sum(copies_ref[...].astype(F32), axis=0)
    lanes = out_ref.shape[0]
    out_ref[...] = jnp.sum(total.reshape(-1, lanes, 128), axis=0)


def tables(modes, scale_in, scale_out):
    grid = 2 * modes
    waves = np.arange(modes) - modes // 2
    cos, sin = trig(waves, np.arange(grid), grid)
    low_cos, low_sin = cos[:, :modes].T, sin[:, :modes].T
    z_table = np.concatenate([low_cos, low_sin], axis=1)
    blocks = modes // 32
    c, s = cos.reshape(blocks, 32, grid), sin.reshape(blocks, 32, grid)
    ty = np.stack([np.concatenate([c, s], 2), np.concatenate([-s, c], 2)], 1).reshape(2 * modes, 2 * grid)
    ct, st = c.transpose(2, 0, 1), s.transpose(2, 0, 1)
    fy = np.stack([np.stack([ct, -st], 2), np.stack([st, ct], 2)], 0).reshape(2 * grid, 2 * modes)
    odd = low_sin.copy()
    odd[0] = cos[:, modes]
    tx = np.concatenate([low_cos, odd], axis=0)
    fx = tx.T
    scaled = (z_table, ty * scale_in, fx * scale_in, fy * (scale_out * scale_out / scale_in))
    return [jnp.asarray(np.ascontiguousarray(t), BF16) for t in scaled]


def shell_counts(modes):
    wave = np.arange(modes) - modes // 2
    square = wave * wave
    total = square[:, None, None] + square[None, :, None] + square[None, None, :]
    shell = np.floor(np.sqrt(total.astype(np.float32)) + np.float32(0.5)).astype(np.int64)
    return np.bincount(shell.reshape(-1), minlength=modes)[:modes].astype(np.float32)


def in_hbm(array):
    return pltpu.with_memory_space_constraint(array, pltpu.HBM)


def params():
    return pltpu.CompilerParams(vmem_limit_bytes=48 * 1024 * 1024)


def body(field):
    _, width_x, width_y, modes = field.shape
    devices = math.prod(lax.axis_size(axis) for axis in RING)
    scale_in = 1.0 / math.sqrt(modes)
    scale_out = math.sqrt(modes) / (2 * modes)
    z_table, ty, fx, fy = tables(modes, scale_in, scale_out)
    weights = jnp.asarray((1.0 / np.maximum(shell_counts(modes), 1.0)).reshape(1, modes))
    messages, turn, shell, spot, near_ty, near_fy, near_weights, near_field, near_table = pl.pallas_call(
        functools.partial(to_slabs, scale=scale_in),
        in_specs=[pl.BlockSpec(memory_space=pltpu.HBM)] * 5,
        out_shape=[
            jax.ShapeDtypeStruct((devices, width_x, 128), BF16),
            jax.ShapeDtypeStruct(field.shape, F32),
            jax.ShapeDtypeStruct(field.shape[1:], F32),
            jax.ShapeDtypeStruct((width_y // 8, modes, modes), BF16),
            jax.ShapeDtypeStruct(ty.shape, BF16),
            jax.ShapeDtypeStruct(fy.shape, BF16),
            jax.ShapeDtypeStruct(weights.shape, F32),
            jax.ShapeDtypeStruct(field.shape, F32),
            jax.ShapeDtypeStruct(z_table.shape, BF16),
        ],
        scratch_shapes=[
            pltpu.VMEM((devices * width_x, 128), F32),
            pltpu.SemaphoreType.DMA((5,)),
        ],
        compiler_params=params(),
        name="to_slabs",
    )(*(in_hbm(array) for array in (field, z_table, ty, fy, weights)))
    slabs = lax.all_to_all(messages, RING, 0, 0, tiled=True)
    shape = (2, 16, 4, 2 * width_x, 128)
    back = pl.pallas_call(
        functools.partial(planes, chunk=128),
        out_shape=jax.ShapeDtypeStruct(shape, BF16),
        scratch_shapes=[pltpu.VMEM((2 * modes, 4 * modes), BF16)],
        compiler_params=params(),
        name="planes",
    )(slabs.reshape(shape), near_ty, fx, near_fy)
    home = lax.all_to_all(back.reshape(devices, width_x, 128), RING, 0, 0, tiled=True)
    bins = math.ceil(math.sqrt((width_x - 1) ** 2 + 49)) + 2
    kept, sums = pl.pallas_call(
        functools.partial(finish, scale=scale_out, bins=bins),
        out_shape=[pltpu.VMEM(field.shape, F32), jax.ShapeDtypeStruct((1, modes), F32)],
        scratch_shapes=[pltpu.VMEM((devices * width_x, 128), F32), pltpu.VMEM((width_x, width_y, modes), F32)],
        compiler_params=params(),
        name="finish",
    )(home, near_field, near_table, turn, shell, spot, near_weights)
    lanes = modes // 128
    other = lax.ppermute(sums, "core", [(0, 1), (1, 0)])
    updated, same = pl.pallas_call(
        put_out,
        in_specs=[pl.BlockSpec(memory_space=pltpu.VMEM)] * 2,
        out_shape=[jax.ShapeDtypeStruct(field.shape, F32), jax.ShapeDtypeStruct(sums.shape, F32)],
        out_specs=[pl.BlockSpec(memory_space=pltpu.HBM), pl.BlockSpec(memory_space=pltpu.VMEM)],
        scratch_shapes=[pltpu.SemaphoreType.DMA(())],
        compiler_params=params(),
        name="put_out",
    )(kept, sums)
    sums = same + other
    chips = devices // 2
    copies = jnp.broadcast_to(sums.reshape(1, lanes, 128).astype(BF16), (chips, lanes, 128))
    everyone = lax.all_to_all(copies, RING[:-1], 0, 0, tiled=True)
    spectrum = pl.pallas_call(
        add_up, out_shape=jax.ShapeDtypeStruct((lanes, 128), F32), compiler_params=params(), name="add_up"
    )(everyone.reshape(-1, 16, 128))
    return updated, spectrum.reshape(modes)


def solution(mesh):
    split = Mesh(mesh.devices.reshape(4, 4, 2, 4, 2), ROW + COL)
    placed = (P(None, ROW, COL, None),)
    return jax.shard_map(
        body, mesh=split, in_specs=placed, out_specs=(P(None, ROW, COL, None), P()), check_vma=False
    )
```
